32 devices in a mesh: fsdp: 4 (over x, core), ctx: 8 (over z, y).
Axes of the slice: x: 2, y: 2, z: 4, core: 2. Of those that a mesh axis runs over, the one named last changes fastest.
Arguments:
- tokens: bfloat16 [4, 1024, 2048], P('fsdp', 'ctx'), may hold values from -6 to 6
- norm_gain: bfloat16 [2048], P(('fsdp', 'ctx')), may hold values from 0.25 to 1.75
- norm_bias: bfloat16 [2048], P(('fsdp', 'ctx')), may hold values from -3 to 3
- qkv_weight: bfloat16 [2048, 3, 2048], P('ctx', None, 'fsdp'), may hold values from -0.125 to 0.125
- qkv_bias: bfloat16 [3, 2048], P(None, ('fsdp', 'ctx')), may hold values from -7.75 to 7.75
- out_weight: bfloat16 [2048, 2048], P('fsdp', 'ctx'), may hold values from -0.75 to 0.75
- out_bias: bfloat16 [2048], P(('fsdp', 'ctx')), may hold values from -3 to 3
- fc1_weight: bfloat16 [2048, 8192], P('ctx', 'fsdp'), may hold values from -0.125 to 0.125
- fc1_bias: bfloat16 [8192], P(('fsdp', 'ctx')), may hold values from -3 to 3
- fc2_weight: bfloat16 [8192, 2048], P('fsdp', 'ctx'), may hold values from -0.0625 to 0.0625
- fc2_bias: bfloat16 [2048], P(('fsdp', 'ctx')), may hold values from -3 to 3
- cotangent: bfloat16 [4, 1024, 2048], P('fsdp', 'ctx'), may hold values from -6 to 6
Outputs:
- output: bfloat16 [4, 1024, 2048], P('fsdp', 'ctx')
- input_grad: bfloat16 [4, 1024, 2048], P('fsdp', 'ctx')
- grad_norm_gain: float32 [2048], P(('fsdp', 'ctx'))
- grad_norm_bias: float32 [2048], P(('fsdp', 'ctx'))
- grad_qkv_weight: float32 [2048, 3, 2048], P('ctx', None, 'fsdp')
- grad_qkv_bias: float32 [3, 2048], P(None, ('fsdp', 'ctx'))
- grad_out_weight: float32 [2048, 2048], P('fsdp', 'ctx')
- grad_out_bias: float32 [2048], P(('fsdp', 'ctx'))
- grad_fc1_weight: float32 [2048, 8192], P('ctx', 'fsdp')
- grad_fc1_bias: float32 [8192], P(('fsdp', 'ctx'))
- grad_fc2_weight: float32 [8192, 2048], P('fsdp', 'ctx')
- grad_fc2_bias: float32 [2048], P(('fsdp', 'ctx'))
The draws below stay inside these ranges and needn't reach their ends.
All inputs are finite; a program needn't handle non-finite values.
Results may differ from the reference program's by a relative error of at most 0.03.
The reference program's roundings to bfloat16 on the way count: a program that leaves them out, or rounds other values in their place, can miss the bound.
Values may be sent and summed in bfloat16 or wider, within the bound.
A program may use at most 192 MiB of HBM per device.

```python
import math
import jax
import jax.numpy as jnp
from jax import lax

D = 2048
FF = 8192
HEADS = 32
HEAD_DIM = 64
ROT_DIM = 32
SEQ_ALL = 4
LEN = 1024


def draw_qkv_bias(key, part):
    key_base = jax.random.fold_in(key, 11)
    return (0.5 * jax.random.truncated_normal(key_base, -6.0, 6.0, (3, D), jnp.float32)).astype(jnp.bfloat16)


def level_of(own_key, shape, pieces, least, largest):
    def one(axis_at, shards_of):
        draws = jax.random.uniform(jax.random.fold_in(jax.random.fold_in(own_key, 6), axis_at), (shards_of,), jnp.float32, least / len(pieces), largest / len(pieces))
        return jnp.repeat(jnp.exp(draws), shape[axis_at] // shards_of).reshape((-1,) + (1,) * (len(shape) - axis_at - 1))

    loudness = one(*pieces[0])
    for cut in pieces[1:]:
        loudness = loudness * one(*cut)
    return loudness


def bell_draw(rng, shape, deviation, bound, split=(), kind=jnp.bfloat16):
    result = jax.random.normal(rng, shape, jnp.float32) * deviation
    if len(split) > 0:
        result = level_of(rng, shape, split, -0.22, 0.18) * result
    return jnp.clip(result, min=-bound, max=bound).astype(kind)


def setup_inputs(seed: int = 0) -> dict:
    seeds = jax.random.split(jax.random.key(seed), 13)
    tokens = bell_draw(seeds[0], (SEQ_ALL, LEN, D), 1.0, 6.0, ((0, 4), (1, 8)))
    norm_gain = jnp.clip(1.0 + 0.15 * jax.random.normal(seeds[1], (D,), jnp.float32), 0.25, 1.75).astype(jnp.bfloat16)
    norm_bias = bell_draw(seeds[2], (D,), 0.5, 3.0, ((0, 32),))
    qkv_weight = bell_draw(seeds[3], (D, 3, D), D ** -0.5, 0.125, ((0, 8), (2, 4)))
    qkv_bias = draw_qkv_bias(jax.random.fold_in(seeds[12], 71), 0)
    out_weight = bell_draw(seeds[5], (D, D), (D // 32) ** -0.5, 0.75, ((0, 4), (1, 8)))
    out_bias = bell_draw(seeds[6], (D,), 0.5, 3.0, ((0, 32),))
    fc1_weight = bell_draw(seeds[7], (D, FF), D ** -0.5, 0.125, ((0, 8), (1, 4)))
    fc1_bias = bell_draw(seeds[8], (FF,), 0.5, 3.0, ((0, 32),))
    fc2_weight = bell_draw(seeds[9], (FF, D), FF ** -0.5, 0.0625, ((0, 4), (1, 8)))
    fc2_bias = bell_draw(seeds[10], (D,), 0.5, 3.0, ((0, 32),))
    cotangent = bell_draw(seeds[11], (SEQ_ALL, LEN, D), 1.0, 6.0, ((0, 4), (1, 8)))
    return dict(tokens=tokens, norm_gain=norm_gain, norm_bias=norm_bias, qkv_weight=qkv_weight, qkv_bias=qkv_bias, out_weight=out_weight, out_bias=out_bias, fc1_weight=fc1_weight, fc1_bias=fc1_bias, fc2_weight=fc2_weight, fc2_bias=fc2_bias, cotangent=cotangent)


NORM_EPS = 1e-05
GELU_COEF = math.sqrt(2.0 / math.pi)
MASKED = -1e+30

def normalize(rows, gain_vec, bias_vec):
    centred = rows - lax.optimization_barrier(jnp.mean(rows, axis=-1, keepdims=True))
    inv_std = lax.rsqrt(lax.optimization_barrier(jnp.mean(centred * centred, axis=-1, keepdims=True)) + NORM_EPS)
    normed = centred * inv_std
    return (normed * gain_vec.astype(jnp.float32) + bias_vec.astype(jnp.float32), normed, inv_std)

def gelu_tanh(values):
    return 0.5 * values * (1.0 + jnp.tanh(GELU_COEF * (values + 0.044715 * values * values * values)))

def gelu_slope(values):
    tangent = jnp.tanh(GELU_COEF * (values + 0.044715 * values * values * values))
    return 0.5 * (1.0 + tangent) + 0.5 * values * (1.0 - tangent * tangent) * GELU_COEF * (1.0 + 3.0 * 0.044715 * values * values)

def rope_tables(positions, rot_dim):
    half_dim = rot_dim // 2
    inverse = 10000.0 ** (-(jnp.arange(half_dim, dtype=jnp.float32) * 2.0) / rot_dim)
    angles = positions[:, None] * inverse[None, :]
    return (jnp.cos(angles)[:, None, :], jnp.sin(angles)[:, None, :])

def rotate_pairs(values, cosine, sine, rot_dim, sign):
    half_dim = rot_dim // 2
    first_half = values[..., :half_dim]
    second_half = values[..., half_dim:rot_dim]
    return jnp.concatenate([first_half * cosine - sign * second_half * sine, second_half * cosine + sign * first_half * sine, values[..., rot_dim:]], axis=-1)

def widen(values_b):
    return lax.optimization_barrier(values_b).astype(jnp.float32)

def reference(tokens, norm_gain, norm_bias, qkv_weight, qkv_bias, out_weight, out_bias, fc1_weight, fc1_bias, fc2_weight, fc2_bias, cotangent):
    width = D
    head_dim = HEAD_DIM
    scale = head_dim ** (-0.5)
    block = math.gcd(LEN, 512)
    nblocks = LEN // block
    positions = jnp.arange(LEN, dtype=jnp.float32)
    cosine, sine = rope_tables(positions, ROT_DIM)
    key_pos = jnp.arange(LEN, dtype=jnp.int32)
    block_pos = jnp.arange(block, dtype=jnp.int32)
    f32 = jnp.float32
    bf16 = jnp.bfloat16
    qkv_matrix = qkv_weight.reshape(D, 3 * D)
    qkv_vector = qkv_bias.reshape(3 * D)

    def one_sequence(totals, item):
        seq_tokens, seq_cot = item
        x_wide = seq_tokens.astype(f32)
        normed_out, normed, inv_std = normalize(x_wide, norm_gain, norm_bias)
        hidden_in = normed_out.astype(bf16)
        mixed = jnp.dot(hidden_in, qkv_matrix, preferred_element_type=f32) + qkv_vector.astype(f32)
        query = rotate_pairs(mixed[:, :width].reshape(LEN, HEADS, head_dim), cosine, sine, ROT_DIM, 1.0).astype(bf16)
        keys = rotate_pairs(mixed[:, width:2 * width].reshape(LEN, HEADS, head_dim), cosine, sine, ROT_DIM, 1.0).astype(bf16)
        values = mixed[:, 2 * width:].reshape(LEN, HEADS, head_dim).astype(bf16)
        query_wide = widen(query)
        keys_wide = widen(keys)
        values_wide = widen(values)

        def forward_block(block_num):
            first = block_num * block
            query_blk = lax.dynamic_slice_in_dim(query_wide, first, block, 0)
            scores = jnp.einsum('qhd,khd->hqk', query_blk, keys_wide) * scale
            allowed = key_pos[None, :] <= (first + block_pos)[:, None]
            scores = jnp.where(allowed, scores, MASKED)
            row_max = lax.optimization_barrier(jnp.max(scores, axis=-1))
            weights = jnp.where(allowed, jnp.exp(scores - row_max[..., None]), 0.0)
            row_sum = lax.optimization_barrier(jnp.sum(weights, axis=-1))
            context = jnp.einsum('hqk,khd->qhd', widen(weights.astype(bf16)), values_wide) / jnp.transpose(row_sum)[..., None]
            return (context.astype(bf16), row_max + jnp.log(row_sum))
        context_blocks, lse_blocks = lax.map(forward_block, jnp.arange(nblocks, dtype=jnp.int32))
        context_b = context_blocks.reshape(LEN, width)
        attn_out = jnp.dot(context_b, out_weight, preferred_element_type=f32) + out_bias.astype(f32)
        pre = jnp.dot(hidden_in, fc1_weight, preferred_element_type=f32) + fc1_bias.astype(f32)
        act_b = gelu_tanh(pre).astype(bf16)
        mlp_out = jnp.dot(act_b, fc2_weight, preferred_element_type=f32) + fc2_bias.astype(f32)
        seq_out = (x_wide + attn_out + mlp_out).astype(bf16)
        cot_wide = seq_cot.astype(f32)
        grad_fc2_w = jnp.dot(act_b.T, seq_cot, preferred_element_type=f32)
        grad_fc2_b = lax.optimization_barrier(jnp.sum(cot_wide, axis=0))
        pre_grad = jnp.dot(seq_cot, fc2_weight.T, preferred_element_type=f32) * gelu_slope(pre)
        pre_grad_b = pre_grad.astype(bf16)
        grad_fc1_w = jnp.dot(hidden_in.T, pre_grad_b, preferred_element_type=f32)
        grad_fc1_b = lax.optimization_barrier(jnp.sum(pre_grad, axis=0))
        mlp_back = jnp.dot(pre_grad_b, fc1_weight.T, preferred_element_type=f32)
        grad_out_w = jnp.dot(context_b.T, seq_cot, preferred_element_type=f32)
        grad_out_b = lax.optimization_barrier(jnp.sum(cot_wide, axis=0))
        context_grad = jnp.dot(seq_cot, out_weight.T, preferred_element_type=f32).astype(bf16)
        ctx_grad_wide = widen(context_grad).reshape(LEN, HEADS, head_dim)
        delta_rows = jnp.transpose(lax.optimization_barrier(jnp.sum(ctx_grad_wide * widen(context_b).reshape(LEN, HEADS, head_dim), axis=-1)))

        def backward_block(carry, block_num):
            key_grad, value_grad = carry
            first = block_num * block
            query_blk = lax.dynamic_slice_in_dim(query_wide, first, block, 0)
            dctx_blk = lax.dynamic_slice_in_dim(ctx_grad_wide, first, block, 0)
            delta_blk = lax.dynamic_slice_in_dim(delta_rows, first, block, 1)
            lse_blk = lse_blocks[block_num]
            scores = jnp.einsum('qhd,khd->hqk', query_blk, keys_wide) * scale
            allowed = key_pos[None, :] <= (first + block_pos)[:, None]
            probs = jnp.where(allowed, jnp.exp(scores - lse_blk[..., None]), 0.0)
            value_grad = value_grad + jnp.einsum('hqk,qhd->khd', widen(probs.astype(bf16)), dctx_blk)
            prob_grad = jnp.einsum('qhd,khd->hqk', dctx_blk, values_wide)
            score_grad = widen((probs * (prob_grad - delta_blk[..., None])).astype(bf16))
            query_grad = jnp.einsum('hqk,khd->qhd', score_grad, keys_wide) * scale
            key_grad = key_grad + jnp.einsum('hqk,qhd->khd', score_grad, query_blk) * scale
            return ((key_grad, value_grad), query_grad)
        zero_heads = jnp.zeros((LEN, HEADS, head_dim), f32)
        (key_grad, value_grad), query_grads = lax.scan(backward_block, (zero_heads, zero_heads), jnp.arange(nblocks, dtype=jnp.int32))
        query_grad = query_grads.reshape(LEN, HEADS, head_dim)
        mixed_grad = jnp.concatenate([rotate_pairs(query_grad, cosine, sine, ROT_DIM, -1.0).reshape(LEN, width), rotate_pairs(key_grad, cosine, sine, ROT_DIM, -1.0).reshape(LEN, width), value_grad.reshape(LEN, width)], axis=1)
        mixed_grad_b = mixed_grad.astype(bf16)
        grad_qkv_w = jnp.dot(hidden_in.T, mixed_grad_b, preferred_element_type=f32)
        grad_qkv_b = lax.optimization_barrier(jnp.sum(mixed_grad, axis=0))
        normed_grad = jnp.dot(mixed_grad_b, qkv_matrix.T, preferred_element_type=f32) + mlp_back
        grad_gain = lax.optimization_barrier(jnp.sum(normed_grad * normed, axis=0))
        grad_shift = lax.optimization_barrier(jnp.sum(normed_grad, axis=0))
        hat_grad = normed_grad * norm_gain.astype(f32)
        back_rows = inv_std * (hat_grad - lax.optimization_barrier(jnp.mean(hat_grad, axis=-1, keepdims=True)) - normed * lax.optimization_barrier(jnp.mean(hat_grad * normed, axis=-1, keepdims=True)))
        seq_in_grad = (back_rows + cot_wide).astype(bf16)
        updates = (grad_gain, grad_shift, grad_qkv_w, grad_qkv_b, grad_out_w, grad_out_b, grad_fc1_w, grad_fc1_b, grad_fc2_w, grad_fc2_b)
        totals = tuple((total + update for total, update in zip(totals, updates)))
        return (totals, (seq_out, seq_in_grad))
    start_totals = (jnp.zeros((D,), f32), jnp.zeros((D,), f32), jnp.zeros((D, 3 * D), f32), jnp.zeros((3 * D,), f32), jnp.zeros((D, D), f32), jnp.zeros((D,), f32), jnp.zeros((D, FF), f32), jnp.zeros((FF,), f32), jnp.zeros((FF, D), f32), jnp.zeros((D,), f32))
    totals, (outputs, in_grads) = lax.scan(one_sequence, start_totals, (tokens, cotangent))
    return (outputs, in_grads, totals[0], totals[1], totals[2].reshape(D, 3, D), totals[3].reshape(3, D), totals[4], totals[5], totals[6], totals[7], totals[8], totals[9])
```

```python
import functools
import math

import jax
import jax.numpy as jnp
from jax import lax
from jax.experimental import pallas as pl
from jax.experimental.pallas import tpu as pltpu
from jax.sharding import PartitionSpec as P

HEAD_DIM = 64
ROT_DIM = 32
NORM_EPS = 1e-05
GELU_COEF = math.sqrt(2.0 / math.pi)
MASKED = -1e30
LOW = 2
F32 = jnp.float32
BF16 = jnp.bfloat16
ANY = pl.BlockSpec(memory_space=pl.ANY)
VMEM = pl.BlockSpec(memory_space=pltpu.VMEM)


class Axis:
    def __init__(self, name, size):
        self.name = name
        self.size = size
        self.low = LOW
        self.high = size // LOW
        self.me = lax.axis_index(name)
        self.hi = lax.div(self.me, LOW)
        self.lo = lax.rem(self.me, LOW)
        self.partner = self.hi * LOW + (1 - self.lo)

    def at(self, hi, lo):
        return hi * LOW + lo

    def ahead(self, steps):
        return self.at(lax.rem(self.hi + steps, self.high), self.lo)

    def behind(self, steps):
        return self.at(lax.rem(self.hi + self.high - steps, self.high), self.lo)

    def behind_other(self, steps):
        return self.at(lax.rem(self.hi + self.high - steps, self.high), 1 - self.lo)


def remote(src, dst, send_sem, recv_sem, axis, index):
    return pltpu.make_async_remote_copy(
        src_ref=src,
        dst_ref=dst,
        send_sem=send_sem,
        recv_sem=recv_sem,
        device_id={axis.name: index},
        device_id_type=pl.DeviceIdType.MESH,
    )


def arrived(dst, sem):
    pltpu.make_async_copy(dst, dst, sem).wait()


class Spread:
    def __init__(self, axis, slot, source, send_hi, recv_hi, send_lo, recv_lo):
        self.axis, self.slot, self.source = axis, slot, source
        self.send_hi, self.recv_hi, self.send_lo, self.recv_lo = send_hi, recv_hi, send_lo, recv_lo

    def copy_hi(self, step):
        ax = self.axis
        return remote(
            self.source,
            self.slot(ax.me),
            self.send_hi.at[step - 1],
            self.recv_hi.at[step - 1],
            ax,
            ax.ahead(step),
        )

    def copy_lo(self, step):
        ax = self.axis
        held = ax.behind(step)
        src = self.source if step == 0 else self.slot(held)
        return remote(
            src, self.slot(held), self.send_lo.at[step], self.recv_lo.at[step], ax, ax.partner
        )

    def start(self):
        for step in range(1, self.axis.high):
            self.copy_hi(step).start()
        self.copy_lo(0).start()

    def forward(self, step):
        arrived(self.slot(self.axis.behind(step)), self.recv_hi.at[step - 1])
        self.copy_lo(step).start()

    def finish(self):
        for step in range(self.axis.high):
            arrived(self.slot(self.axis.behind_other(step)), self.recv_lo.at[step])
        for step in range(1, self.axis.high):
            self.copy_hi(step).wait_send()
        for step in range(self.axis.high):
            self.copy_lo(step).wait_send()


def spread_sems(axis_size):
    high = axis_size // LOW
    return [
        pltpu.SemaphoreType.DMA((max(high - 1, 1),)),
        pltpu.SemaphoreType.DMA((max(high - 1, 1),)),
        pltpu.SemaphoreType.DMA((high,)),
        pltpu.SemaphoreType.DMA((high,)),
    ]


class Line:
    def __init__(self, axis, slot, source, *sems):
        self.axis, self.slot, self.source = axis, slot, source
        self.send_up, self.recv_up, self.send_down, self.recv_down, self.send_lo, self.recv_lo = (
            sems
        )

    def copy(self, hi, sends, recvs, target):
        ax = self.axis
        block = ax.at(hi, ax.lo)
        src = self.source if hi is ax.hi else self.slot(block)
        return remote(src, self.slot(block), sends.at[hi], recvs.at[hi], ax, target)

    def up(self, hi):
        return self.copy(hi, self.send_up, self.recv_up, self.axis.me + LOW)

    def down(self, hi):
        return self.copy(hi, self.send_down, self.recv_down, self.axis.me - LOW)

    def across(self, hi):
        return self.copy(hi, self.send_lo, self.recv_lo, self.axis.partner)

    def start(self):
        ax = self.axis

        @pl.when(ax.hi < ax.high - 1)
        def _():
            self.up(ax.hi).start()

        @pl.when(ax.hi > 0)
        def _():
            self.down(ax.hi).start()

        self.across(ax.hi).start()

    def forward(self, step):
        ax = self.axis

        @pl.when(ax.hi >= step)
        def _():
            held = ax.hi - step
            arrived(self.slot(ax.at(held, ax.lo)), self.recv_up.at[held])

            @pl.when(ax.hi < ax.high - 1)
            def _():
                self.up(held).start()

            self.across(held).start()

        @pl.when(ax.hi + step < ax.high)
        def _():
            held = ax.hi + step
            arrived(self.slot(ax.at(held, ax.lo)), self.recv_down.at[held])

            @pl.when(ax.hi > 0)
            def _():
                self.down(held).start()

            self.across(held).start()

    def finish(self):
        ax = self.axis
        for hi in range(ax.high):
            arrived(self.slot(ax.at(hi, 1 - ax.lo)), self.recv_lo.at[hi])
        for step in range(ax.high):

            @pl.when(jnp.logical_and(ax.hi >= step, ax.hi < ax.high - 1))
            def _(step=step):
                self.up(ax.hi if step == 0 else ax.hi - step).wait_send()

            @pl.when(jnp.logical_and(ax.hi + step < ax.high, ax.hi > 0))
            def _(step=step):
                self.down(ax.hi if step == 0 else ax.hi + step).wait_send()

            @pl.when(ax.hi >= step)
            def _(step=step):
                self.across(ax.hi if step == 0 else ax.hi - step).wait_send()

            if step > 0:

                @pl.when(ax.hi + step < ax.high)
                def _(step=step):
                    self.across(ax.hi + step).wait_send()


def line_sems(axis_size):
    return [pltpu.SemaphoreType.DMA((axis_size // LOW,))] * 6


def meet_everyone(fs, cx):
    barrier = pltpu.get_barrier_semaphore()
    total = fs.size * cx.size
    me = fs.me * cx.size + cx.me

    def signal(step, carry):
        other = lax.rem(me + step, total)
        pl.semaphore_signal(
            barrier,
            inc=1,
            device_id={fs.name: lax.div(other, cx.size), cx.name: lax.rem(other, cx.size)},
            device_id_type=pl.DeviceIdType.MESH,
        )
        return carry

    lax.fori_loop(1, total, signal, 0)
    pl.semaphore_wait(barrier, total - 1)


def shift_of(f_index, f_size):
    return lax.rem(f_index, LOW) * (f_size // LOW) + lax.div(f_index, LOW)


def unshift(shift, f_size):
    return lax.rem(shift, f_size // LOW) * LOW + lax.div(shift, f_size // LOW)


def low_slot(fs, column, device):
    return lax.rem(device + fs.size - shift_of(column, fs.size), fs.size)


def gather_kernel(n_act, n_w, small, f_size, c_size, *refs):
    fs, cx = Axis("fsdp", f_size), Axis("ctx", c_size)
    ratio = c_size // f_size
    n_ctx = n_act + (1 if small else 0)
    n_in = n_ctx + n_w
    ins, outs, rest = refs[:n_in], refs[n_in : 2 * n_in], list(refs[2 * n_in :])
    acts, w_srcs = ins[:n_ctx], ins[n_ctx:]
    act_outs, w_outs = outs[:n_ctx], outs[n_ctx:]
    own_sem = rest.pop(0)
    lines = []
    for index in range(n_ctx):
        out = act_outs[index]
        if index < n_act:
            slot = lambda c, out=out: out.at[c]
        else:
            slot = lambda c, out=out: out.at[fs.me, c]
        lines.append(Line(cx, slot, acts[index], *rest[:6]))
        rest = rest[6:]
    mids, rest = rest[:n_w], rest[n_w:]
    mid_send, mid_recv, w_send, w_recv = rest[:4]
    rest = rest[4:]
    column = lax.div(cx.me, ratio)
    spreads = []
    for index in range(n_w):
        out = w_outs[index]
        slot = lambda f, out=out: out.at[:, low_slot(fs, column, f)]
        spreads.append(Spread(fs, slot, slot(fs.me), *rest[:4]))
        rest = rest[4:]
    if small:
        out = act_outs[n_act]
        slot = lambda f, out=out: out.at[f]
        small_spread = Spread(fs, slot, slot(fs.me), *rest[:4])

    pass_to = lax.rem(cx.me + shift_of(fs.me, f_size), f_size)
    pass_from = unshift(lax.rem(fs.me + f_size - lax.rem(cx.me, f_size), f_size), f_size)
    stays = pass_to == fs.me
    row_hi, row_lo = lax.div(cx.me, f_size), lax.rem(cx.me, f_size)

    def move(index):
        src, dst = w_srcs[index], mids[index]
        away = lambda: remote(src, dst, mid_send.at[index], mid_recv.at[index], fs, pass_to)
        here = lambda: pltpu.make_async_copy(src, dst, mid_recv.at[index])
        return away, here

    def scatter(index, i):
        to_c = pass_from * ratio + i
        src, dst = mids[index].at[i], w_outs[index].at[row_hi, row_lo]
        sem = w_recv.at[index, row_hi]
        away = lambda: remote(src, dst, w_send.at[index, i], sem, cx, to_c)
        here = lambda: pltpu.make_async_copy(src, dst, sem)
        return to_c == cx.me, away, here

    def either(is_self, away, here):
        @pl.when(is_self)
        def _():
            here().start()

        @pl.when(jnp.logical_not(is_self))
        def _():
            away().start()

    def start_moves():
        for index in range(n_w):
            either(stays, *move(index))

    def start_scatter(index):
        arrived(mids[index], mid_recv.at[index])
        for i in range(ratio):
            either(*scatter(index, i))

    def start_spread(index):
        for hi in range(ratio):
            arrived(w_outs[index].at[hi, low_slot(fs, column, fs.me)], w_recv.at[index, hi])
        spreads[index].start()

    def forward_spread(index):
        for step in range(1, fs.high):
            spreads[index].forward(step)

    meet_everyone(fs, cx)
    own = []
    for index in range(n_ctx):
        copy = pltpu.make_async_copy(acts[index], lines[index].slot(cx.me), own_sem.at[index])
        copy.start()
        own.append(copy)
    if small:
        lines[n_act].start()
    start_moves()
    for index in range(n_act):
        lines[index].start()
    scatters = [functools.partial(start_scatter, index) for index in range(n_w)]
    starts = [functools.partial(start_spread, index) for index in range(n_w)]
    lasts = [functools.partial(forward_spread, index) for index in range(n_w)]
    for work in scatters[:2]:
        work()
    for step in range(1, cx.high):
        if small:
            lines[n_act].forward(step)
        for index in range(n_act):
            lines[index].forward(step)
            if step == 1 and index == n_act - 1:
                for work in scatters[2:]:
                    work()
            if starts and (step > 1 or index == n_act - 1):
                starts.pop(0)()
                if len(lasts) - len(starts) > 1:
                    lasts.pop(0)()
    for work in scatters[2:] if cx.high == 1 else []:
        work()
    while starts:
        starts.pop(0)()
        if len(lasts) - len(starts) > 1:
            lasts.pop(0)()
    for work in lasts:
        work()
    if small:
        lines[n_act].finish()
        own[n_act].wait()
        small_spread.start()
        for step in range(1, fs.high):
            small_spread.forward(step)
    for index in range(n_act):
        own[index].wait()
        lines[index].finish()
    for index in range(n_w):
        spreads[index].finish()

        @pl.when(jnp.logical_not(stays))
        def _(index=index):
            move(index)[0]().wait_send()

        for i in range(ratio):
            is_self, away, here = scatter(index, i)

            @pl.when(jnp.logical_not(is_self))
            def _(away=away):
                away().wait_send()

    if small:
        small_spread.finish()


def gather_call(f_size, c_size, acts, w_srcs, small, collective_id):
    ratio = c_size // f_size
    ins = list(acts) + ([small] if small is not None else []) + list(w_srcs)
    shapes = [jax.ShapeDtypeStruct((c_size, *a.shape), a.dtype) for a in acts]
    if small is not None:
        shapes.append(jax.ShapeDtypeStruct((f_size, c_size, *small.shape), small.dtype))
    for w in w_srcs:
        shapes.append(jax.ShapeDtypeStruct((ratio, f_size, *w.shape[1:]), w.dtype))
    n_ctx = len(acts) + (small is not None)
    scratch = [pltpu.SemaphoreType.DMA((n_ctx,))]
    for _ in range(n_ctx):
        scratch += line_sems(c_size)
    scratch += [pltpu.VMEM(w.shape, w.dtype) for w in w_srcs]
    scratch += [pltpu.SemaphoreType.DMA((len(w_srcs),))] * 2
    scratch += [pltpu.SemaphoreType.DMA((len(w_srcs), ratio))] * 2
    for _ in range(len(w_srcs) + (small is not None)):
        scratch += spread_sems(f_size)
    return pl.pallas_call(
        functools.partial(
            gather_kernel, len(acts), len(w_srcs), small is not None, f_size, c_size
        ),
        out_shape=tuple(shapes),
        in_specs=[VMEM] * len(ins),
        out_specs=tuple([ANY] * len(shapes)),
        scratch_shapes=scratch,
        compiler_params=pltpu.CompilerParams(collective_id=collective_id, has_side_effects=True),
        name=f"gather_{collective_id}",
    )(*ins)


def add_into(dst, terms):
    rows = dst.shape[-2]
    lead = dst.shape[:-2]
    chunk = math.gcd(rows, 32)

    def at(ref, index, start):
        return (*index, pl.ds(start, chunk), slice(None))

    for index in [()] if not lead else [(i,) for i in range(lead[0])]:

        def step(i, carry, index=index):
            start = pl.multiple_of(i * chunk, chunk)
            total = terms[0][at(terms[0], index, start)].astype(F32)
            for term in terms[1:]:
                total = total + term[at(term, index, start)].astype(F32)
            dst[at(dst, index, start)] = total.astype(dst.dtype)
            return carry

        lax.fori_loop(0, rows // chunk, step, 0)


class Fold:
    def __init__(self, axis, block, result, from_lo, staged, from_hi, sems):
        self.axis, self.block, self.result = axis, block, result
        self.from_lo, self.staged, self.from_hi = from_lo, staged, from_hi
        self.send_lo, self.recv_lo, self.send_hi, self.recv_hi = sems

    def copy_lo(self, step):
        ax = self.axis
        hi = lax.rem(ax.hi + step, ax.high)
        return remote(
            self.block(ax.at(hi, 1 - ax.lo)),
            self.from_lo.at[step],
            self.send_lo.at[step],
            self.recv_lo.at[step],
            ax,
            ax.partner,
        )

    def copy_hi(self, step):
        ax = self.axis
        return remote(
            self.staged.at[step - 1],
            self.from_hi.at[step - 1],
            self.send_hi.at[step - 1],
            self.recv_hi.at[step - 1],
            ax,
            ax.ahead(step),
        )

    def start(self):
        for step in list(range(1, self.axis.high)) + [0]:
            self.copy_lo(step).start()

    def forward(self, step):
        arrived(self.from_lo.at[step], self.recv_lo.at[step])
        add_into(
            self.staged.at[step - 1], [self.block(self.axis.ahead(step)), self.from_lo.at[step]]
        )
        self.copy_hi(step).start()

    def finish(self):
        arrived(self.from_lo.at[0], self.recv_lo.at[0])
        terms = [self.block(self.axis.me), self.from_lo.at[0]]
        for step in range(1, self.axis.high):
            arrived(self.from_hi.at[step - 1], self.recv_hi.at[step - 1])
            terms.append(self.from_hi.at[step - 1])
        add_into(self.result, terms)

    def drain(self):
        for step in range(self.axis.high):
            self.copy_lo(step).wait_send()
        for step in range(1, self.axis.high):
            self.copy_hi(step).wait_send()


class LineFold:
    def __init__(self, axis, block, result, from_lo, from_z, from_end, *sems):
        self.axis, self.block, self.result = axis, block, result
        self.from_lo, self.from_z, self.from_end = from_lo, from_z, from_end
        self.send_lo, self.recv_lo, self.send_z, self.recv_z, self.recv_end = sems
        low_end, high_end = jnp.int32(0), jnp.int32(axis.high - 1)
        self.order = []
        for _ in range(axis.high):
            take_low = axis.hi - low_end >= high_end - axis.hi
            self.order.append(jnp.where(take_low, low_end, high_end))
            low_end = jnp.where(take_low, low_end + 1, low_end)
            high_end = jnp.where(take_low, high_end, high_end - 1)

    def across(self, hi):
        ax = self.axis
        return remote(
            self.block(ax.at(hi, 1 - ax.lo)),
            self.from_lo.at[hi],
            self.send_lo.at[hi],
            self.recv_lo.at[hi],
            ax,
            ax.partner,
        )

    def onward(self, hi, up, last):
        ax = self.axis
        side = 0 if up else 1
        dst, sem = (
            (self.from_end.at[side], self.recv_end.at[side])
            if last
            else (self.from_z.at[hi], self.recv_z.at[hi])
        )
        target = ax.me + LOW if up else ax.me - LOW
        return remote(self.from_lo.at[hi], dst, self.send_z.at[hi], sem, ax, target)

    def start(self):
        for hi in self.order:
            self.across(hi).start()

    def pass_on(self, hi, up):
        ax = self.axis
        first = ax.hi == (0 if up else ax.high - 1)
        own = self.block(ax.at(hi, ax.lo))

        @pl.when(first)
        def _():
            add_into(self.from_lo.at[hi], [own, self.from_lo.at[hi]])

        @pl.when(jnp.logical_not(first))
        def _():
            arrived(self.from_z.at[hi], self.recv_z.at[hi])
            add_into(self.from_lo.at[hi], [own, self.from_lo.at[hi], self.from_z.at[hi]])

        near = ax.hi == (hi - 1 if up else hi + 1)

        @pl.when(near)
        def _():
            self.onward(hi, up, True).start()

        @pl.when(jnp.logical_not(near))
        def _():
            self.onward(hi, up, False).start()

    def forward(self, hi):
        ax = self.axis
        arrived(self.from_lo.at[hi], self.recv_lo.at[hi])

        @pl.when(ax.hi < hi)
        def _():
            self.pass_on(hi, True)

        @pl.when(ax.hi > hi)
        def _():
            self.pass_on(hi, False)

    def finish(self):
        ax = self.axis
        own = [self.block(ax.me), self.from_lo.at[ax.hi]]
        if ax.high == 1:
            add_into(self.result, own)
            return
        low_end, high_end = ax.hi == 0, ax.hi == ax.high - 1

        @pl.when(jnp.logical_not(low_end))
        def _():
            arrived(self.from_end.at[0], self.recv_end.at[0])

        @pl.when(jnp.logical_not(high_end))
        def _():
            arrived(self.from_end.at[1], self.recv_end.at[1])

        @pl.when(low_end)
        def _():
            add_into(self.result, own + [self.from_end.at[1]])

        @pl.when(high_end)
        def _():
            add_into(self.result, own + [self.from_end.at[0]])

        @pl.when(jnp.logical_not(jnp.logical_or(low_end, high_end)))
        def _():
            add_into(self.result, own + [self.from_end.at[0], self.from_end.at[1]])

    def drain(self):
        ax = self.axis
        for hi in range(ax.high):
            self.across(hi).wait_send()

            @pl.when(ax.hi != hi)
            def _(hi=hi):
                self.onward(hi, True, False).wait_send()


def line_fold_scratch(axis_size, shape, dtype):
    high = axis_size // LOW
    return [
        pltpu.VMEM((high, *shape), dtype),
        pltpu.VMEM((high, *shape), dtype),
        pltpu.VMEM((2, *shape), dtype),
        pltpu.SemaphoreType.DMA((high,)),
        pltpu.SemaphoreType.DMA((high,)),
        pltpu.SemaphoreType.DMA((high,)),
        pltpu.SemaphoreType.DMA((high,)),
        pltpu.SemaphoreType.DMA((2,)),
    ]


def fold_scratch(axis_size, shape, dtype):
    high = axis_size // LOW
    more = max(high - 1, 1)
    return [
        pltpu.VMEM((high, *shape), dtype),
        pltpu.VMEM((more, *shape), dtype),
        pltpu.VMEM((more, *shape), dtype),
        pltpu.SemaphoreType.DMA((high,)),
        pltpu.SemaphoreType.DMA((high,)),
        pltpu.SemaphoreType.DMA((more,)),
        pltpu.SemaphoreType.DMA((more,)),
    ]


def reduce_kernel(n_part, n_w, f_size, c_size, *refs):
    fs, cx = Axis("fsdp", f_size), Axis("ctx", c_size)
    ratio = c_size // f_size
    parts, refs = refs[:n_part], refs[n_part:]
    grads, refs = refs[:n_w], refs[n_w:]
    rows_outs, refs = refs[:n_part], refs[n_part:]
    grad_outs, scratch = refs[:n_w], list(refs[n_w:])
    row_folds = []
    for index in range(n_part):
        block = lambda c, part=parts[index]: part.at[c]
        row_folds.append(LineFold(cx, block, rows_outs[index], *scratch[:8]))
        scratch = scratch[8:]
    column = lax.div(cx.me, ratio)
    folds, totals = [], []
    for index in range(n_w):
        grad = grads[index]
        block = lambda f, grad=grad: grad.at[:, low_slot(fs, column, f)]
        totals.append(scratch[7])
        folds.append(Fold(fs, block, scratch[7], *scratch[:3], scratch[3:7]))
        scratch = scratch[8:]
    g_send, g_recv = scratch

    meet_everyone(fs, cx)
    for fold in row_folds:
        fold.start()
    for fold in folds:
        fold.start()

    slot = lax.rem(cx.me, ratio)
    row_lo = low_slot(fs, column, fs.me)

    def deliver(index, hi):
        to_c = hi * f_size + row_lo
        is_self = jnp.logical_and(column == fs.me, to_c == cx.me)
        src = totals[index].at[hi]
        dst = grad_outs[index].at[slot]
        away = lambda: pltpu.make_async_remote_copy(
            src_ref=src,
            dst_ref=dst,
            send_sem=g_send.at[index, hi],
            recv_sem=g_recv.at[index, slot],
            device_id={fs.name: column, cx.name: to_c},
            device_id_type=pl.DeviceIdType.MESH,
        )
        here = lambda: pltpu.make_async_copy(src, dst, g_recv.at[index, slot])
        return is_self, away, here

    def deliver_all(index):
        folds[index].finish()
        for hi in range(ratio):
            is_self, away, here = deliver(index, hi)

            @pl.when(is_self)
            def _(here=here):
                here().start()

            @pl.when(jnp.logical_not(is_self))
            def _(away=away):
                away().start()

    def pass_halves(index):
        for step in range(1, fs.high):
            folds[index].forward(step)

    row_work = [
        functools.partial(fold.forward, hi) for fold in row_folds for hi in fold.order
    ]
    halves = [functools.partial(pass_halves, index) for index in range(n_w)]
    delivers = [functools.partial(deliver_all, index) for index in range(n_w)]
    for count, work in enumerate(row_work):
        for more in halves[:2]:
            more()
        halves = halves[2:]
        work()
        if count >= 1 and delivers and not halves:
            delivers.pop(0)()
    for work in halves + delivers:
        work()
    for fold in row_folds:
        fold.finish()
    for index in range(n_w):
        for i in range(ratio):
            arrived(grad_outs[index].at[i], g_recv.at[index, i])
    for fold in row_folds:
        fold.drain()
    for index in range(n_w):
        folds[index].drain()
        for hi in range(ratio):
            is_self, away, here = deliver(index, hi)

            @pl.when(jnp.logical_not(is_self))
            def _(away=away):
                away().wait_send()


def reduce_call(f_size, c_size, parts, grads, collective_id):
    ratio = c_size // f_size
    shapes, scratch = [], []
    for part in parts:
        shapes.append(jax.ShapeDtypeStruct(part.shape[1:], F32))
        scratch += line_fold_scratch(c_size, part.shape[1:], part.dtype)
    for g in grads:
        piece = (ratio, *g.shape[2:])
        shapes.append(jax.ShapeDtypeStruct(piece, g.dtype))
        scratch += fold_scratch(f_size, piece, g.dtype) + [pltpu.VMEM(piece, g.dtype)]
    scratch += [pltpu.SemaphoreType.DMA((len(grads), ratio))] * 2
    outs = pl.pallas_call(
        functools.partial(reduce_kernel, len(parts), len(grads), f_size, c_size),
        out_shape=tuple(shapes),
        in_specs=[VMEM] * (len(parts) + len(grads)),
        out_specs=tuple([VMEM] * len(shapes)),
        scratch_shapes=scratch,
        compiler_params=pltpu.CompilerParams(collective_id=collective_id, has_side_effects=True),
        name=f"reduce_{collective_id}",
    )(*parts, *grads)
    return outs[: len(parts)], outs[len(parts) :]


def reduce_all(f_size, c_size, parts, grads):
    size = sum(2.25 * part.size * part.dtype.itemsize for part in parts)
    size += sum(2.5 * grad.size * grad.dtype.itemsize for grad in grads)
    if size <= 56 * 2**20:
        return reduce_call(f_size, c_size, parts, grads, 2)
    half = len(grads) // 2
    (first,), early = reduce_call(f_size, c_size, parts[:1], grads[:half], 2)
    (second,), late = reduce_call(f_size, c_size, parts[1:], grads[half:], 3)
    return (first, second), (*early, *late)


def small_kernel(f_size, c_size, tiles, out, held, send_sem, recv_sem):
    fs, cx = Axis("fsdp", f_size), Axis("ctx", c_size)
    total = f_size * c_size
    me = fs.me * c_size + cx.me
    meet_everyone(fs, cx)

    def copy(step):
        other = lax.rem(me + step, total)
        return pltpu.make_async_remote_copy(
            src_ref=tiles.at[other],
            dst_ref=held.at[step - 1],
            send_sem=send_sem.at[step - 1],
            recv_sem=recv_sem.at[step - 1],
            device_id={fs.name: lax.div(other, c_size), cx.name: lax.rem(other, c_size)},
            device_id_type=pl.DeviceIdType.MESH,
        )

    def start(step, carry):
        copy(step).start()
        return carry

    lax.fori_loop(1, total, start, 0)

    def collect(step, acc):
        arrived(held.at[step - 1], recv_sem.at[step - 1])
        return acc + held[step - 1]

    out[...] = lax.fori_loop(1, total, collect, tiles[me])

    def drain(step, carry):
        copy(step).wait_send()
        return carry

    lax.fori_loop(1, total, drain, 0)


def small_call(f_size, c_size, tiles, collective_id):
    total = f_size * c_size
    return pl.pallas_call(
        functools.partial(small_kernel, f_size, c_size),
        out_shape=jax.ShapeDtypeStruct(tiles.shape[1:], F32),
        in_specs=[VMEM],
        out_specs=VMEM,
        scratch_shapes=[
            pltpu.VMEM((total - 1, *tiles.shape[1:]), F32),
            pltpu.SemaphoreType.DMA((total - 1,)),
            pltpu.SemaphoreType.DMA((total - 1,)),
        ],
        compiler_params=pltpu.CompilerParams(collective_id=collective_id, has_side_effects=True),
        name=f"small_{collective_id}",
    )(tiles)


def normed_of(rows):
    centred = rows - jnp.mean(rows, axis=-1, keepdims=True)
    inv_std = lax.rsqrt(jnp.mean(centred * centred, axis=-1, keepdims=True) + NORM_EPS)
    return centred * inv_std, inv_std


def gelu_both(values):
    tangent = jnp.tanh(GELU_COEF * (values + 0.044715 * values * values * values))
    act = 0.5 * values * (1.0 + tangent)
    slope = 0.5 * (1.0 + tangent) + 0.5 * values * (1.0 - tangent * tangent) * GELU_COEF * (
        1.0 + 3.0 * 0.044715 * values * values
    )
    return act, slope


def rope_tables(count, rot_dim):
    positions = jnp.arange(count, dtype=F32)
    half_dim = rot_dim // 2
    inverse = 10000.0 ** (-(jnp.arange(half_dim, dtype=F32) * 2.0) / rot_dim)
    angles = positions[:, None] * inverse[None, :]
    return (jnp.cos(angles)[:, None, :], jnp.sin(angles)[:, None, :])


def rotate_pairs(values, cosine, sine, rot_dim, sign):
    half_dim = rot_dim // 2
    first_half = values[..., :half_dim]
    second_half = values[..., half_dim:rot_dim]
    return jnp.concatenate(
        [
            first_half * cosine - sign * second_half * sine,
            second_half * cosine + sign * first_half * sine,
            values[..., rot_dim:],
        ],
        axis=-1,
    )


def attention_forward(query, key, value, scale):
    length = query.shape[0]
    block = math.gcd(length, 256)
    contexts, lses = [], []
    for first in range(0, length, block):
        last = first + block
        scores = (
            jnp.einsum("qhd,khd->hqk", query[first:last], key[:last], preferred_element_type=F32)
            * scale
        )
        allowed = jnp.arange(last)[None, :] <= (first + jnp.arange(block))[:, None]
        scores = jnp.where(allowed, scores, MASKED)
        top = jnp.max(scores, axis=-1)
        weights = jnp.where(allowed, jnp.exp(scores - top[..., None]), 0.0)
        total = jnp.sum(weights, axis=-1)
        context = jnp.einsum(
            "hqk,khd->qhd", weights.astype(BF16), value[:last], preferred_element_type=F32
        )
        contexts.append(context / jnp.transpose(total)[..., None])
        lses.append(top + jnp.log(total))
    return jnp.concatenate(contexts, axis=0), jnp.concatenate(lses, axis=1)


def attention_backward(query, key, value, context_grad, delta, lse, scale):
    length, heads, dim = query.shape
    block = math.gcd(length, 256)
    query_grads = []
    key_grad = jnp.zeros((length, heads, dim), F32)
    value_grad = jnp.zeros((length, heads, dim), F32)
    for first in range(0, length, block):
        last = first + block
        q, g = query[first:last], context_grad[first:last]
        scores = jnp.einsum("qhd,khd->hqk", q, key[:last], preferred_element_type=F32) * scale
        allowed = jnp.arange(last)[None, :] <= (first + jnp.arange(block))[:, None]
        probs = jnp.where(allowed, jnp.exp(scores - lse[:, first:last, None]), 0.0)
        value_grad = value_grad.at[:last].add(
            jnp.einsum("hqk,qhd->khd", probs.astype(BF16), g, preferred_element_type=F32)
        )
        prob_grad = jnp.einsum("qhd,khd->hqk", g, value[:last], preferred_element_type=F32)
        score_grad = (probs * (prob_grad - delta[:, first:last, None])).astype(BF16)
        query_grads.append(
            jnp.einsum("hqk,khd->qhd", score_grad, key[:last], preferred_element_type=F32) * scale
        )
        key_grad = key_grad.at[:last].add(
            jnp.einsum("hqk,qhd->khd", score_grad, q, preferred_element_type=F32) * scale
        )
    return jnp.concatenate(query_grads, axis=0), key_grad, value_grad


def body(
    tokens,
    norm_gain,
    norm_bias,
    qkv_weight,
    qkv_bias,
    out_weight,
    out_bias,
    fc1_weight,
    fc1_bias,
    fc2_weight,
    fc2_bias,
    cotangent,
):
    f_size, c_size = lax.axis_size("fsdp"), lax.axis_size("ctx")
    ratio = c_size // f_size
    devices = f_size * c_size
    own_seqs, tok_count, width = tokens.shape
    own_rows = own_seqs * tok_count
    length = tok_count * c_size
    rows = own_seqs * length
    head_dim = HEAD_DIM
    scale = head_dim ** (-0.5)
    row_block = qkv_weight.shape[0]
    cols = qkv_weight.shape[2] // ratio
    hidden_cols = fc1_weight.shape[1] // ratio
    heads = cols // head_dim
    c_index = lax.axis_index("ctx")

    vec = norm_gain.shape[0]
    vec1 = fc1_bias.shape[0]
    def lanes(array):
        array = array.reshape(-1, min(array.shape[-1], 128))
        return jnp.pad(array, ((0, 0), (0, 128 - array.shape[1])))

    small = jnp.concatenate(
        [
            lanes(v)
            for v in (norm_gain, norm_bias, out_bias, fc2_bias, qkv_bias, fc1_bias)
        ]
    )
    small = jnp.pad(small, ((0, -small.shape[0] % 16), (0, 0)))

    qkv_src = (
        jnp.transpose(qkv_weight.reshape(row_block, 3, ratio, cols), (2, 0, 1, 3))
        .reshape(ratio, row_block, 3 * cols)
    )
    fc1_src = jnp.transpose(fc1_weight.reshape(row_block, ratio, hidden_cols), (1, 0, 2))
    out_src = jnp.transpose(out_weight.reshape(ratio, cols, row_block), (0, 2, 1))
    fc2_src = jnp.transpose(fc2_weight.reshape(ratio, hidden_cols, row_block), (0, 2, 1))

    tok_all, cot_all, small_all, qkv_all, fc1_all, fc2_all, out_all = gather_call(
        f_size,
        c_size,
        [tokens.reshape(own_rows, width), cotangent.reshape(own_rows, width)],
        [qkv_src, fc1_src, fc2_src, out_src],
        small,
        0,
    )

    def rows_of(gathered):
        return jnp.swapaxes(gathered.reshape(c_size, own_seqs, tok_count, width), 0, 1).reshape(
            rows, width
        )

    def blocks_of(array):
        return jnp.swapaxes(array.reshape(own_seqs, c_size, tok_count, width), 0, 1).reshape(
            c_size, own_rows, width
        )

    x_rows = rows_of(tok_all)
    grad_rows = rows_of(cot_all)
    qkv_w = qkv_all.reshape(width, 3 * cols)
    fc1_w = fc1_all.reshape(width, hidden_cols)
    out_t = out_all.reshape(width, cols)
    fc2_t = fc2_all.reshape(width, hidden_cols)

    vectors = small_all.reshape(devices, -1, 128)
    gain_full = vectors[:, 0, :vec].reshape(-1).astype(F32)
    shift_full = vectors[:, 1, :vec].reshape(-1).astype(F32)
    out_bias_full = vectors[:, 2, :vec].reshape(-1).astype(F32)
    fc2_bias_full = vectors[:, 3, :vec].reshape(-1).astype(F32)
    qkv_bias_full = jnp.swapaxes(vectors[:, 4:7, :vec], 0, 1).reshape(3, -1)
    lane = min(vec1, 128)
    fc1_bias_full = vectors[:, 7 : 7 + vec1 // lane, :lane].reshape(-1)
    qkv_b = (
        lax.dynamic_slice_in_dim(qkv_bias_full, c_index * cols, cols, 1).reshape(-1).astype(F32)
    )
    fc1_b = lax.dynamic_slice_in_dim(fc1_bias_full, c_index * hidden_cols, hidden_cols, 0).astype(
        F32
    )

    normed, _ = normed_of(x_rows.astype(F32))
    hidden_in = (normed * gain_full + shift_full).astype(BF16)
    mixed = jnp.dot(hidden_in, qkv_w, preferred_element_type=F32) + qkv_b
    cosine, sine = rope_tables(length, ROT_DIM)

    def heads_of(array):
        return array.reshape(own_seqs, length, heads, head_dim)

    query = rotate_pairs(heads_of(mixed[:, :cols]), cosine, sine, ROT_DIM, 1.0).astype(BF16)
    key = rotate_pairs(heads_of(mixed[:, cols : 2 * cols]), cosine, sine, ROT_DIM, 1.0).astype(
        BF16
    )
    value = heads_of(mixed[:, 2 * cols :].astype(BF16))
    forward = [attention_forward(query[s], key[s], value[s], scale) for s in range(own_seqs)]
    context_b = jnp.stack([pair[0] for pair in forward]).astype(BF16)
    context_rows = context_b.reshape(rows, cols)
    pre = jnp.dot(hidden_in, fc1_w, preferred_element_type=F32) + fc1_b
    act, slope = gelu_both(pre)
    act_b = act.astype(BF16)
    contract_last = (((1,), (1,)), ((), ()))
    partial_out = lax.dot_general(
        context_rows, out_t, contract_last, preferred_element_type=F32
    ) + lax.dot_general(act_b, fc2_t, contract_last, preferred_element_type=F32)

    pre_grad = jnp.dot(grad_rows, fc2_t, preferred_element_type=F32) * slope
    pre_grad_b = pre_grad.astype(BF16)
    contract_first = (((0,), (0,)), ((), ()))

    def weight_grad(left, right):
        product = lax.dot_general(left, right, contract_first, preferred_element_type=F32)
        return product.astype(BF16).reshape(ratio, f_size, row_block, right.shape[1])

    fc2_grad = weight_grad(grad_rows, act_b)
    fc1_grad = weight_grad(hidden_in, pre_grad_b)
    out_grad = weight_grad(grad_rows, context_rows)
    fc1_b_grad = jnp.sum(pre_grad, axis=0)
    mlp_back = lax.dot_general(pre_grad_b, fc1_w, contract_last, preferred_element_type=F32)
    context_grad = heads_of(jnp.dot(grad_rows, out_t, preferred_element_type=F32).astype(BF16))
    delta = jnp.swapaxes(
        jnp.sum(context_grad.astype(F32) * context_b.astype(F32), axis=-1), 1, 2
    )
    grads = [
        attention_backward(
            query[s], key[s], value[s], context_grad[s], delta[s], forward[s][1], scale
        )
        for s in range(own_seqs)
    ]
    query_grad, key_grad, value_grad = [jnp.stack(parts) for parts in zip(*grads)]
    mixed_grad = jnp.concatenate(
        [
            rotate_pairs(query_grad, cosine, sine, ROT_DIM, -1.0).reshape(rows, cols),
            rotate_pairs(key_grad, cosine, sine, ROT_DIM, -1.0).reshape(rows, cols),
            value_grad.reshape(rows, cols),
        ],
        axis=1,
    )
    mixed_grad_b = mixed_grad.astype(BF16)
    qkv_grad = weight_grad(hidden_in, mixed_grad_b)
    qkv_b_grad = jnp.sum(mixed_grad, axis=0).reshape(3, cols)
    normed_part = (
        lax.dot_general(mixed_grad_b, qkv_w, contract_last, preferred_element_type=F32) + mlp_back
    )
    (branch, normed_grad), (fc2_shard, fc1_shard, out_shard, qkv_shard) = reduce_all(
        f_size,
        c_size,
        [blocks_of(partial_out.astype(BF16)), blocks_of(normed_part.astype(BF16))],
        [fc2_grad, fc1_grad, out_grad, qkv_grad],
    )

    x_own = tokens.reshape(own_rows, width).astype(F32)
    cot_own = cotangent.reshape(own_rows, width).astype(F32)
    output = (x_own + branch + out_bias_full + fc2_bias_full).astype(BF16)
    normed_own, inv_std_own = normed_of(x_own)
    hat_grad = normed_grad * gain_full
    back_rows = inv_std_own * (
        hat_grad
        - jnp.mean(hat_grad, axis=-1, keepdims=True)
        - normed_own * jnp.mean(hat_grad * normed_own, axis=-1, keepdims=True)
    )
    input_grad = (back_rows + cot_own).astype(BF16)

    def whole(block, full, axis):
        return lax.dynamic_update_slice_in_dim(
            jnp.zeros(full, F32), block, c_index * block.shape[axis], axis
        )

    grad_gain = jnp.sum(normed_grad * normed_own, axis=0).reshape(devices, vec)
    grad_shift = jnp.sum(normed_grad, axis=0).reshape(devices, vec)
    grad_cot = jnp.sum(cot_own, axis=0).reshape(devices, vec)
    q_parts = jnp.swapaxes(whole(qkv_b_grad, (3, width), 1).reshape(3, devices, vec), 0, 1)
    f_parts = whole(fc1_b_grad, (vec1 * devices,), 0).reshape(devices, vec1)
    tiles = jnp.concatenate(
        [grad_gain, grad_shift, grad_cot, q_parts.reshape(devices, 3 * vec), f_parts], axis=1
    )
    used = tiles.shape[1]
    tiles = jnp.pad(tiles, ((0, 0), (0, -used % 1024))).reshape(devices, -1, 128)
    sums = small_call(f_size, c_size, tiles, 4).reshape(-1)

    qkv_out = jnp.transpose(
        qkv_shard.reshape(ratio, row_block, 3, cols), (1, 2, 0, 3)
    ).reshape(row_block, 3, ratio * cols)
    fc1_out = jnp.swapaxes(fc1_shard, 0, 1).reshape(row_block, ratio * hidden_cols)
    out_out = jnp.swapaxes(out_shard, 1, 2).reshape(ratio * cols, row_block)
    fc2_out = jnp.swapaxes(fc2_shard, 1, 2).reshape(ratio * hidden_cols, row_block)
    return (
        output.reshape(own_seqs, tok_count, width),
        input_grad.reshape(own_seqs, tok_count, width),
        sums[:vec],
        sums[vec : 2 * vec],
        qkv_out.astype(F32),
        sums[3 * vec : 6 * vec].reshape(3, vec),
        out_out.astype(F32),
        sums[2 * vec : 3 * vec],
        fc1_out.astype(F32),
        sums[6 * vec : 6 * vec + vec1],
        fc2_out.astype(F32),
        sums[2 * vec : 3 * vec],
    )


def solution(mesh):
    row = P("fsdp", "ctx", None)
    vector = P(("fsdp", "ctx"))
    return jax.shard_map(
        body,
        mesh=mesh,
        in_specs=(
            row,
            vector,
            vector,
            P("ctx", None, "fsdp"),
            P(None, ("fsdp", "ctx")),
            P("fsdp", "ctx"),
            vector,
            P("ctx", "fsdp"),
            vector,
            P("fsdp", "ctx"),
            vector,
            row,
        ),
        out_specs=(
            row,
            row,
            vector,
            vector,
            P("ctx", None, "fsdp"),
            P(None, ("fsdp", "ctx")),
            P("fsdp", "ctx"),
            vector,
            P("ctx", "fsdp"),
            vector,
            P("fsdp", "ctx"),
            vector,
        ),
        check_vma=False,
    )
```

```python
import functools
import math

import jax
import jax.numpy as jnp
from jax import lax
from jax.experimental import pallas as pl
from jax.experimental.pallas import tpu as pltpu
from jax.sharding import PartitionSpec as P

HEAD_DIM = 64
ROT_DIM = 32
NORM_EPS = 1e-05
GELU_COEF = math.sqrt(2.0 / math.pi)
MASKED = -1e30
LOW = 2
F32 = jnp.float32
BF16 = jnp.bfloat16
ANY = pl.BlockSpec(memory_space=pl.ANY)
VMEM = pl.BlockSpec(memory_space=pltpu.VMEM)


class Axis:
    def __init__(self, name, size):
        self.name = name
        self.size = size
        self.low = LOW
        self.high = size // LOW
        self.me = lax.axis_index(name)
        self.hi = lax.div(self.me, LOW)
        self.lo = lax.rem(self.me, LOW)
        self.partner = self.hi * LOW + (1 - self.lo)

    def at(self, hi, lo):
        return hi * LOW + lo

    def ahead(self, steps):
        return self.at(lax.rem(self.hi + steps, self.high), self.lo)

    def behind(self, steps):
        return self.at(lax.rem(self.hi + self.high - steps, self.high), self.lo)

    def behind_other(self, steps):
        return self.at(lax.rem(self.hi + self.high - steps, self.high), 1 - self.lo)


def remote(src, dst, send_sem, recv_sem, axis, index):
    return pltpu.make_async_remote_copy(
        src_ref=src,
        dst_ref=dst,
        send_sem=send_sem,
        recv_sem=recv_sem,
        device_id={axis.name: index},
        device_id_type=pl.DeviceIdType.MESH,
    )


def arrived(dst, sem):
    pltpu.make_async_copy(dst, dst, sem).wait()


class Spread:
    def __init__(self, axis, slot, source, send_hi, recv_hi, send_lo, recv_lo):
        self.axis, self.slot, self.source = axis, slot, source
        self.send_hi, self.recv_hi, self.send_lo, self.recv_lo = send_hi, recv_hi, send_lo, recv_lo

    def copy_hi(self, step):
        ax = self.axis
        return remote(
            self.source,
            self.slot(ax.me),
            self.send_hi.at[step - 1],
            self.recv_hi.at[step - 1],
            ax,
            ax.ahead(step),
        )

    def copy_lo(self, step):
        ax = self.axis
        held = ax.behind(step)
        src = self.source if step == 0 else self.slot(held)
        return remote(
            src, self.slot(held), self.send_lo.at[step], self.recv_lo.at[step], ax, ax.partner
        )

    def start(self):
        for step in range(1, self.axis.high):
            self.copy_hi(step).start()
        self.copy_lo(0).start()

    def forward(self, step):
        arrived(self.slot(self.axis.behind(step)), self.recv_hi.at[step - 1])
        self.copy_lo(step).start()

    def finish(self):
        for step in range(self.axis.high):
            arrived(self.slot(self.axis.behind_other(step)), self.recv_lo.at[step])
        for step in range(1, self.axis.high):
            self.copy_hi(step).wait_send()
        for step in range(self.axis.high):
            self.copy_lo(step).wait_send()


def spread_sems(axis_size):
    high = axis_size // LOW
    return [
        pltpu.SemaphoreType.DMA((max(high - 1, 1),)),
        pltpu.SemaphoreType.DMA((max(high - 1, 1),)),
        pltpu.SemaphoreType.DMA((high,)),
        pltpu.SemaphoreType.DMA((high,)),
    ]


class Line:
    def __init__(self, axis, slot, source, *sems):
        self.axis, self.slot, self.source = axis, slot, source
        self.send_up, self.recv_up, self.send_down, self.recv_down, self.send_lo, self.recv_lo = (
            sems
        )

    def copy(self, hi, sends, recvs, target):
        ax = self.axis
        block = ax.at(hi, ax.lo)
        src = self.source if hi is ax.hi else self.slot(block)
        return remote(src, self.slot(block), sends.at[hi], recvs.at[hi], ax, target)

    def up(self, hi):
        return self.copy(hi, self.send_up, self.recv_up, self.axis.me + LOW)

    def down(self, hi):
        return self.copy(hi, self.send_down, self.recv_down, self.axis.me - LOW)

    def across(self, hi):
        return self.copy(hi, self.send_lo, self.recv_lo, self.axis.partner)

    def start(self):
        ax = self.axis

        @pl.when(ax.hi < ax.high - 1)
        def _():
            self.up(ax.hi).start()

        @pl.when(ax.hi > 0)
        def _():
            self.down(ax.hi).start()

        self.across(ax.hi).start()

    def forward(self, step):
        ax = self.axis

        @pl.when(ax.hi >= step)
        def _():
            held = ax.hi - step
            arrived(self.slot(ax.at(held, ax.lo)), self.recv_up.at[held])

            @pl.when(ax.hi < ax.high - 1)
            def _():
                self.up(held).start()

            self.across(held).start()

        @pl.when(ax.hi + step < ax.high)
        def _():
            held = ax.hi + step
            arrived(self.slot(ax.at(held, ax.lo)), self.recv_down.at[held])

            @pl.when(ax.hi > 0)
            def _():
                self.down(held).start()

            self.across(held).start()

    def finish(self):
        ax = self.axis
        for hi in range(ax.high):
            arrived(self.slot(ax.at(hi, 1 - ax.lo)), self.recv_lo.at[hi])
        for step in range(ax.high):

            @pl.when(jnp.logical_and(ax.hi >= step, ax.hi < ax.high - 1))
            def _(step=step):
                self.up(ax.hi if step == 0 else ax.hi - step).wait_send()

            @pl.when(jnp.logical_and(ax.hi + step < ax.high, ax.hi > 0))
            def _(step=step):
                self.down(ax.hi if step == 0 else ax.hi + step).wait_send()

            @pl.when(ax.hi >= step)
            def _(step=step):
                self.across(ax.hi if step == 0 else ax.hi - step).wait_send()

            if step > 0:

                @pl.when(ax.hi + step < ax.high)
                def _(step=step):
                    self.across(ax.hi + step).wait_send()


def line_sems(axis_size):
    return [pltpu.SemaphoreType.DMA((axis_size // LOW,))] * 6


def meet_everyone(fs, cx):
    barrier = pltpu.get_barrier_semaphore()
    total = fs.size * cx.size
    me = fs.me * cx.size + cx.me

    def signal(step, carry):
        other = lax.rem(me + step, total)
        pl.semaphore_signal(
            barrier,
            inc=1,
            device_id={fs.name: lax.div(other, cx.size), cx.name: lax.rem(other, cx.size)},
            device_id_type=pl.DeviceIdType.MESH,
        )
        return carry

    lax.fori_loop(1, total, signal, 0)
    pl.semaphore_wait(barrier, total - 1)


def shift_of(f_index, f_size):
    return lax.rem(f_index, LOW) * (f_size // LOW) + lax.div(f_index, LOW)


def unshift(shift, f_size):
    return lax.rem(shift, f_size // LOW) * LOW + lax.div(shift, f_size // LOW)


def low_slot(fs, column, device):
    return lax.rem(device + fs.size - shift_of(column, fs.size), fs.size)


def gather_kernel(n_act, n_w, small, f_size, c_size, *refs):
    fs, cx = Axis("fsdp", f_size), Axis("ctx", c_size)
    ratio = c_size // f_size
    n_ctx = n_act + (1 if small else 0)
    n_in = n_ctx + n_w
    ins, outs, rest = refs[:n_in], refs[n_in : 2 * n_in], list(refs[2 * n_in :])
    acts, w_srcs = ins[:n_ctx], ins[n_ctx:]
    act_outs, w_outs = outs[:n_ctx], outs[n_ctx:]
    own_sem = rest.pop(0)
    lines = []
    for index in range(n_ctx):
        out = act_outs[index]
        if index < n_act:
            slot = lambda c, out=out: out.at[c]
        else:
            slot = lambda c, out=out: out.at[fs.me, c]
        lines.append(Line(cx, slot, acts[index], *rest[:6]))
        rest = rest[6:]
    mids, rest = rest[:n_w], rest[n_w:]
    mid_send, mid_recv, w_send, w_recv = rest[:4]
    rest = rest[4:]
    column = lax.div(cx.me, ratio)
    spreads = []
    for index in range(n_w):
        out = w_outs[index]
        slot = lambda f, out=out: out.at[:, low_slot(fs, column, f)]
        spreads.append(Spread(fs, slot, slot(fs.me), *rest[:4]))
        rest = rest[4:]
    if small:
        out = act_outs[n_act]
        slot = lambda f, out=out: out.at[f]
        small_spread = Spread(fs, slot, slot(fs.me), *rest[:4])

    pass_to = lax.rem(cx.me + shift_of(fs.me, f_size), f_size)
    pass_from = unshift(lax.rem(fs.me + f_size - lax.rem(cx.me, f_size), f_size), f_size)
    stays = pass_to == fs.me
    row_hi, row_lo = lax.div(cx.me, f_size), lax.rem(cx.me, f_size)

    def move(index):
        src, dst = w_srcs[index], mids[index]
        away = lambda: remote(src, dst, mid_send.at[index], mid_recv.at[index], fs, pass_to)
        here = lambda: pltpu.make_async_copy(src, dst, mid_recv.at[index])
        return away, here

    def scatter(index, i):
        to_c = pass_from * ratio + i
        src, dst = mids[index].at[i], w_outs[index].at[row_hi, row_lo]
        sem = w_recv.at[index, row_hi]
        away = lambda: remote(src, dst, w_send.at[index, i], sem, cx, to_c)
        here = lambda: pltpu.make_async_copy(src, dst, sem)
        return to_c == cx.me, away, here

    def either(is_self, away, here):
        @pl.when(is_self)
        def _():
            here().start()

        @pl.when(jnp.logical_not(is_self))
        def _():
            away().start()

    def start_moves():
        for index in range(n_w):
            either(stays, *move(index))

    def start_scatter(index):
        arrived(mids[index], mid_recv.at[index])
        for i in range(ratio):
            either(*scatter(index, i))

    def start_spread(index):
        for hi in range(ratio):
            arrived(w_outs[index].at[hi, low_slot(fs, column, fs.me)], w_recv.at[index, hi])
        spreads[index].start()

    def forward_spread(index):
        for step in range(1, fs.high):
            spreads[index].forward(step)

    meet_everyone(fs, cx)
    own = []
    for index in range(n_ctx):
        copy = pltpu.make_async_copy(acts[index], lines[index].slot(cx.me), own_sem.at[index])
        copy.start()
        own.append(copy)
    if small:
        lines[n_act].start()
    start_moves()
    for index in range(n_act):
        lines[index].start()
    scatters = [functools.partial(start_scatter, index) for index in range(n_w)]
    starts = [functools.partial(start_spread, index) for index in range(n_w)]
    lasts = [functools.partial(forward_spread, index) for index in range(n_w)]
    for work in scatters[:2]:
        work()
    for step in range(1, cx.high):
        if small:
            lines[n_act].forward(step)
        for index in range(n_act):
            lines[index].forward(step)
            if step == 1 and index == n_act - 1:
                for work in scatters[2:]:
                    work()
            if starts and (step > 1 or index == n_act - 1):
                starts.pop(0)()
                if len(lasts) - len(starts) > 1:
                    lasts.pop(0)()
    for work in scatters[2:] if cx.high == 1 else []:
        work()
    while starts:
        starts.pop(0)()
        if len(lasts) - len(starts) > 1:
            lasts.pop(0)()
    for work in lasts:
        work()
    if small:
        lines[n_act].finish()
        own[n_act].wait()
        small_spread.start()
        for step in range(1, fs.high):
            small_spread.forward(step)
    for index in range(n_act):
        own[index].wait()
        lines[index].finish()
    for index in range(n_w):
        spreads[index].finish()

        @pl.when(jnp.logical_not(stays))
        def _(index=index):
            move(index)[0]().wait_send()

        for i in range(ratio):
            is_self, away, here = scatter(index, i)

            @pl.when(jnp.logical_not(is_self))
            def _(away=away):
                away().wait_send()

    if small:
        small_spread.finish()


def gather_call(f_size, c_size, acts, w_srcs, small, collective_id):
    ratio = c_size // f_size
    ins = list(acts) + ([small] if small is not None else []) + list(w_srcs)
    shapes = [jax.ShapeDtypeStruct((c_size, *a.shape), a.dtype) for a in acts]
    if small is not None:
        shapes.append(jax.ShapeDtypeStruct((f_size, c_size, *small.shape), small.dtype))
    for w in w_srcs:
        shapes.append(jax.ShapeDtypeStruct((ratio, f_size, *w.shape[1:]), w.dtype))
    n_ctx = len(acts) + (small is not None)
    scratch = [pltpu.SemaphoreType.DMA((n_ctx,))]
    for _ in range(n_ctx):
        scratch += line_sems(c_size)
    scratch += [pltpu.VMEM(w.shape, w.dtype) for w in w_srcs]
    scratch += [pltpu.SemaphoreType.DMA((len(w_srcs),))] * 2
    scratch += [pltpu.SemaphoreType.DMA((len(w_srcs), ratio))] * 2
    for _ in range(len(w_srcs) + (small is not None)):
        scratch += spread_sems(f_size)
    return pl.pallas_call(
        functools.partial(
            gather_kernel, len(acts), len(w_srcs), small is not None, f_size, c_size
        ),
        out_shape=tuple(shapes),
        in_specs=[VMEM] * len(ins),
        out_specs=tuple([ANY] * len(shapes)),
        scratch_shapes=scratch,
        compiler_params=pltpu.CompilerParams(collective_id=collective_id, has_side_effects=True),
        name=f"gather_{collective_id}",
    )(*ins)


def add_into(dst, terms):
    rows = dst.shape[-2]
    lead = dst.shape[:-2]
    chunk = math.gcd(rows, 32)

    def at(ref, index, start):
        return (*index, pl.ds(start, chunk), slice(None))

    for index in [()] if not lead else [(i,) for i in range(lead[0])]:

        def step(i, carry, index=index):
            start = pl.multiple_of(i * chunk, chunk)
            total = terms[0][at(terms[0], index, start)].astype(F32)
            for term in terms[1:]:
                total = total + term[at(term, index, start)].astype(F32)
            dst[at(dst, index, start)] = total.astype(dst.dtype)
            return carry

        lax.fori_loop(0, rows // chunk, step, 0)


class Fold:
    def __init__(self, axis, block, result, from_lo, staged, from_hi, sems):
        self.axis, self.block, self.result = axis, block, result
        self.from_lo, self.staged, self.from_hi = from_lo, staged, from_hi
        self.send_lo, self.recv_lo, self.send_hi, self.recv_hi = sems

    def copy_lo(self, step):
        ax = self.axis
        hi = lax.rem(ax.hi + step, ax.high)
        return remote(
            self.block(ax.at(hi, 1 - ax.lo)),
            self.from_lo.at[step],
            self.send_lo.at[step],
            self.recv_lo.at[step],
            ax,
            ax.partner,
        )

    def copy_hi(self, step):
        ax = self.axis
        return remote(
            self.staged.at[step - 1],
            self.from_hi.at[step - 1],
            self.send_hi.at[step - 1],
            self.recv_hi.at[step - 1],
            ax,
            ax.ahead(step),
        )

    def start(self):
        for step in list(range(1, self.axis.high)) + [0]:
            self.copy_lo(step).start()

    def forward(self, step):
        arrived(self.from_lo.at[step], self.recv_lo.at[step])
        add_into(
            self.staged.at[step - 1], [self.block(self.axis.ahead(step)), self.from_lo.at[step]]
        )
        self.copy_hi(step).start()

    def finish(self):
        arrived(self.from_lo.at[0], self.recv_lo.at[0])
        terms = [self.block(self.axis.me), self.from_lo.at[0]]
        for step in range(1, self.axis.high):
            arrived(self.from_hi.at[step - 1], self.recv_hi.at[step - 1])
            terms.append(self.from_hi.at[step - 1])
        add_into(self.result, terms)

    def drain(self):
        for step in range(self.axis.high):
            self.copy_lo(step).wait_send()
        for step in range(1, self.axis.high):
            self.copy_hi(step).wait_send()


class LineFold:
    def __init__(self, axis, block, result, from_lo, from_z, from_end, *sems):
        self.axis, self.block, self.result = axis, block, result
        self.from_lo, self.from_z, self.from_end = from_lo, from_z, from_end
        self.send_lo, self.recv_lo, self.send_z, self.recv_z, self.recv_end = sems
        low_end, high_end = jnp.int32(0), jnp.int32(axis.high - 1)
        self.order = []
        for _ in range(axis.high):
            take_low = axis.hi - low_end >= high_end - axis.hi
            self.order.append(jnp.where(take_low, low_end, high_end))
            low_end = jnp.where(take_low, low_end + 1, low_end)
            high_end = jnp.where(take_low, high_end, high_end - 1)

    def across(self, hi):
        ax = self.axis
        return remote(
            self.block(ax.at(hi, 1 - ax.lo)),
            self.from_lo.at[hi],
            self.send_lo.at[hi],
            self.recv_lo.at[hi],
            ax,
            ax.partner,
        )

    def onward(self, hi, up, last):
        ax = self.axis
        side = 0 if up else 1
        dst, sem = (
            (self.from_end.at[side], self.recv_end.at[side])
            if last
            else (self.from_z.at[hi], self.recv_z.at[hi])
        )
        target = ax.me + LOW if up else ax.me - LOW
        return remote(self.from_lo.at[hi], dst, self.send_z.at[hi], sem, ax, target)

    def start(self):
        for hi in self.order:
            self.across(hi).start()

    def pass_on(self, hi, up):
        ax = self.axis
        first = ax.hi == (0 if up else ax.high - 1)
        own = self.block(ax.at(hi, ax.lo))

        @pl.when(first)
        def _():
            add_into(self.from_lo.at[hi], [own, self.from_lo.at[hi]])

        @pl.when(jnp.logical_not(first))
        def _():
            arrived(self.from_z.at[hi], self.recv_z.at[hi])
            add_into(self.from_lo.at[hi], [own, self.from_lo.at[hi], self.from_z.at[hi]])

        near = ax.hi == (hi - 1 if up else hi + 1)

        @pl.when(near)
        def _():
            self.onward(hi, up, True).start()

        @pl.when(jnp.logical_not(near))
        def _():
            self.onward(hi, up, False).start()

    def forward(self, hi):
        ax = self.axis
        arrived(self.from_lo.at[hi], self.recv_lo.at[hi])

        @pl.when(ax.hi < hi)
        def _():
            self.pass_on(hi, True)

        @pl.when(ax.hi > hi)
        def _():
            self.pass_on(hi, False)

    def finish(self):
        ax = self.axis
        own = [self.block(ax.me), self.from_lo.at[ax.hi]]
        if ax.high == 1:
            add_into(self.result, own)
            return
        low_end, high_end = ax.hi == 0, ax.hi == ax.high - 1

        @pl.when(jnp.logical_not(low_end))
        def _():
            arrived(self.from_end.at[0], self.recv_end.at[0])

        @pl.when(jnp.logical_not(high_end))
        def _():
            arrived(self.from_end.at[1], self.recv_end.at[1])

        @pl.when(low_end)
        def _():
            add_into(self.result, own + [self.from_end.at[1]])

        @pl.when(high_end)
        def _():
            add_into(self.result, own + [self.from_end.at[0]])

        @pl.when(jnp.logical_not(jnp.logical_or(low_end, high_end)))
        def _():
            add_into(self.result, own + [self.from_end.at[0], self.from_end.at[1]])

    def drain(self):
        ax = self.axis
        for hi in range(ax.high):
            self.across(hi).wait_send()

            @pl.when(ax.hi != hi)
            def _(hi=hi):
                self.onward(hi, True, False).wait_send()


def line_fold_scratch(axis_size, shape, dtype):
    high = axis_size // LOW
    return [
        pltpu.VMEM((high, *shape), dtype),
        pltpu.VMEM((high, *shape), dtype),
        pltpu.VMEM((2, *shape), dtype),
        pltpu.SemaphoreType.DMA((high,)),
        pltpu.SemaphoreType.DMA((high,)),
        pltpu.SemaphoreType.DMA((high,)),
        pltpu.SemaphoreType.DMA((high,)),
        pltpu.SemaphoreType.DMA((2,)),
    ]


def fold_scratch(axis_size, shape, dtype):
    high = axis_size // LOW
    more = max(high - 1, 1)
    return [
        pltpu.VMEM((high, *shape), dtype),
        pltpu.VMEM((more, *shape), dtype),
        pltpu.VMEM((more, *shape), dtype),
        pltpu.SemaphoreType.DMA((high,)),
        pltpu.SemaphoreType.DMA((high,)),
        pltpu.SemaphoreType.DMA((more,)),
        pltpu.SemaphoreType.DMA((more,)),
    ]


def reduce_kernel(n_part, n_w, f_size, c_size, *refs):
    fs, cx = Axis("fsdp", f_size), Axis("ctx", c_size)
    ratio = c_size // f_size
    parts, refs = refs[:n_part], refs[n_part:]
    grads, refs = refs[:n_w], refs[n_w:]
    rows_outs, refs = refs[:n_part], refs[n_part:]
    grad_outs, scratch = refs[:n_w], list(refs[n_w:])
    row_folds = []
    for index in range(n_part):
        block = lambda c, part=parts[index]: part.at[c]
        row_folds.append(LineFold(cx, block, rows_outs[index], *scratch[:8]))
        scratch = scratch[8:]
    column = lax.div(cx.me, ratio)
    folds, totals = [], []
    for index in range(n_w):
        grad = grads[index]
        block = lambda f, grad=grad: grad.at[:, low_slot(fs, column, f)]
        totals.append(scratch[7])
        folds.append(Fold(fs, block, scratch[7], *scratch[:3], scratch[3:7]))
        scratch = scratch[8:]
    g_send, g_recv = scratch

    meet_everyone(fs, cx)
    for fold in row_folds:
        fold.start()
    for fold in folds:
        fold.start()

    slot = lax.rem(cx.me, ratio)
    row_lo = low_slot(fs, column, fs.me)

    def deliver(index, hi):
        to_c = hi * f_size + row_lo
        is_self = jnp.logical_and(column == fs.me, to_c == cx.me)
        src = totals[index].at[hi]
        dst = grad_outs[index].at[slot]
        away = lambda: pltpu.make_async_remote_copy(
            src_ref=src,
            dst_ref=dst,
            send_sem=g_send.at[index, hi],
            recv_sem=g_recv.at[index, slot],
            device_id={fs.name: column, cx.name: to_c},
            device_id_type=pl.DeviceIdType.MESH,
        )
        here = lambda: pltpu.make_async_copy(src, dst, g_recv.at[index, slot])
        return is_self, away, here

    def deliver_all(index):
        folds[index].finish()
        for hi in range(ratio):
            is_self, away, here = deliver(index, hi)

            @pl.when(is_self)
            def _(here=here):
                here().start()

            @pl.when(jnp.logical_not(is_self))
            def _(away=away):
                away().start()

    def pass_halves(index):
        for step in range(1, fs.high):
            folds[index].forward(step)

    row_work = [
        functools.partial(fold.forward, hi) for fold in row_folds for hi in fold.order
    ]
    halves = [functools.partial(pass_halves, index) for index in range(n_w)]
    delivers = [functools.partial(deliver_all, index) for index in range(n_w)]
    for count, work in enumerate(row_work):
        for more in halves[:2]:
            more()
        halves = halves[2:]
        work()
        if count >= 1 and delivers and not halves:
            delivers.pop(0)()
    for work in halves + delivers:
        work()
    for fold in row_folds:
        fold.finish()
    for index in range(n_w):
        for i in range(ratio):
            arrived(grad_outs[index].at[i], g_recv.at[index, i])
    for fold in row_folds:
        fold.drain()
    for index in range(n_w):
        folds[index].drain()
        for hi in range(ratio):
            is_self, away, here = deliver(index, hi)

            @pl.when(jnp.logical_not(is_self))
            def _(away=away):
                away().wait_send()


def reduce_call(f_size, c_size, parts, grads, collective_id):
    ratio = c_size // f_size
    shapes, scratch = [], []
    for part in parts:
        shapes.append(jax.ShapeDtypeStruct(part.shape[1:], F32))
        scratch += line_fold_scratch(c_size, part.shape[1:], part.dtype)
    for g in grads:
        piece = (ratio, *g.shape[2:])
        shapes.append(jax.ShapeDtypeStruct(piece, g.dtype))
        scratch += fold_scratch(f_size, piece, g.dtype) + [pltpu.VMEM(piece, g.dtype)]
    scratch += [pltpu.SemaphoreType.DMA((len(grads), ratio))] * 2
    outs = pl.pallas_call(
        functools.partial(reduce_kernel, len(parts), len(grads), f_size, c_size),
        out_shape=tuple(shapes),
        in_specs=[VMEM] * (len(parts) + len(grads)),
        out_specs=tuple([VMEM] * len(shapes)),
        scratch_shapes=scratch,
        compiler_params=pltpu.CompilerParams(collective_id=collective_id, has_side_effects=True),
        name=f"reduce_{collective_id}",
    )(*parts, *grads)
    return outs[: len(parts)], outs[len(parts) :]


def small_kernel(f_size, c_size, tiles, out, held, send_sem, recv_sem):
    fs, cx = Axis("fsdp", f_size), Axis("ctx", c_size)
    total = f_size * c_size
    me = fs.me * c_size + cx.me
    meet_everyone(fs, cx)

    def copy(step):
        other = lax.rem(me + step, total)
        return pltpu.make_async_remote_copy(
            src_ref=tiles.at[other],
            dst_ref=held.at[step - 1],
            send_sem=send_sem.at[step - 1],
            recv_sem=recv_sem.at[step - 1],
            device_id={fs.name: lax.div(other, c_size), cx.name: lax.rem(other, c_size)},
            device_id_type=pl.DeviceIdType.MESH,
        )

    def start(step, carry):
        copy(step).start()
        return carry

    lax.fori_loop(1, total, start, 0)

    def collect(step, acc):
        arrived(held.at[step - 1], recv_sem.at[step - 1])
        return acc + held[step - 1]

    out[...] = lax.fori_loop(1, total, collect, tiles[me])

    def drain(step, carry):
        copy(step).wait_send()
        return carry

    lax.fori_loop(1, total, drain, 0)


def small_call(f_size, c_size, tiles, collective_id):
    total = f_size * c_size
    return pl.pallas_call(
        functools.partial(small_kernel, f_size, c_size),
        out_shape=jax.ShapeDtypeStruct(tiles.shape[1:], F32),
        in_specs=[VMEM],
        out_specs=VMEM,
        scratch_shapes=[
            pltpu.VMEM((total - 1, *tiles.shape[1:]), F32),
            pltpu.SemaphoreType.DMA((total - 1,)),
            pltpu.SemaphoreType.DMA((total - 1,)),
        ],
        compiler_params=pltpu.CompilerParams(collective_id=collective_id, has_side_effects=True),
        name=f"small_{collective_id}",
    )(tiles)


def normed_of(rows):
    centred = rows - jnp.mean(rows, axis=-1, keepdims=True)
    inv_std = lax.rsqrt(jnp.mean(centred * centred, axis=-1, keepdims=True) + NORM_EPS)
    return centred * inv_std, inv_std


def gelu_both(values):
    tangent = jnp.tanh(GELU_COEF * (values + 0.044715 * values * values * values))
    act = 0.5 * values * (1.0 + tangent)
    slope = 0.5 * (1.0 + tangent) + 0.5 * values * (1.0 - tangent * tangent) * GELU_COEF * (
        1.0 + 3.0 * 0.044715 * values * values
    )
    return act, slope


def rope_tables(count, rot_dim):
    positions = jnp.arange(count, dtype=F32)
    half_dim = rot_dim // 2
    inverse = 10000.0 ** (-(jnp.arange(half_dim, dtype=F32) * 2.0) / rot_dim)
    angles = positions[:, None] * inverse[None, :]
    return (jnp.cos(angles)[:, None, :], jnp.sin(angles)[:, None, :])


def rotate_pairs(values, cosine, sine, rot_dim, sign):
    half_dim = rot_dim // 2
    first_half = values[..., :half_dim]
    second_half = values[..., half_dim:rot_dim]
    return jnp.concatenate(
        [
            first_half * cosine - sign * second_half * sine,
            second_half * cosine + sign * first_half * sine,
            values[..., rot_dim:],
        ],
        axis=-1,
    )


def attention_forward(query, key, value, scale):
    length = query.shape[0]
    block = math.gcd(length, 256)
    contexts, lses = [], []
    for first in range(0, length, block):
        last = first + block
        scores = (
            jnp.einsum("qhd,khd->hqk", query[first:last], key[:last], preferred_element_type=F32)
            * scale
        )
        allowed = jnp.arange(last)[None, :] <= (first + jnp.arange(block))[:, None]
        scores = jnp.where(allowed, scores, MASKED)
        top = jnp.max(scores, axis=-1)
        weights = jnp.where(allowed, jnp.exp(scores - top[..., None]), 0.0)
        total = jnp.sum(weights, axis=-1)
        context = jnp.einsum(
            "hqk,khd->qhd", weights.astype(BF16), value[:last], preferred_element_type=F32
        )
        contexts.append(context / jnp.transpose(total)[..., None])
        lses.append(top + jnp.log(total))
    return jnp.concatenate(contexts, axis=0), jnp.concatenate(lses, axis=1)


def attention_backward(query, key, value, context_grad, delta, lse, scale):
    length, heads, dim = query.shape
    block = math.gcd(length, 256)
    query_grads = []
    key_grad = jnp.zeros((length, heads, dim), F32)
    value_grad = jnp.zeros((length, heads, dim), F32)
    for first in range(0, length, block):
        last = first + block
        q, g = query[first:last], context_grad[first:last]
        scores = jnp.einsum("qhd,khd->hqk", q, key[:last], preferred_element_type=F32) * scale
        allowed = jnp.arange(last)[None, :] <= (first + jnp.arange(block))[:, None]
        probs = jnp.where(allowed, jnp.exp(scores - lse[:, first:last, None]), 0.0)
        value_grad = value_grad.at[:last].add(
            jnp.einsum("hqk,qhd->khd", probs.astype(BF16), g, preferred_element_type=F32)
        )
        prob_grad = jnp.einsum("qhd,khd->hqk", g, value[:last], preferred_element_type=F32)
        score_grad = (probs * (prob_grad - delta[:, first:last, None])).astype(BF16)
        query_grads.append(
            jnp.einsum("hqk,khd->qhd", score_grad, key[:last], preferred_element_type=F32) * scale
        )
        key_grad = key_grad.at[:last].add(
            jnp.einsum("hqk,qhd->khd", score_grad, q, preferred_element_type=F32) * scale
        )
    return jnp.concatenate(query_grads, axis=0), key_grad, value_grad


def body(
    tokens,
    norm_gain,
    norm_bias,
    qkv_weight,
    qkv_bias,
    out_weight,
    out_bias,
    fc1_weight,
    fc1_bias,
    fc2_weight,
    fc2_bias,
    cotangent,
):
    f_size, c_size = lax.axis_size("fsdp"), lax.axis_size("ctx")
    ratio = c_size // f_size
    devices = f_size * c_size
    own_seqs, tok_count, width = tokens.shape
    own_rows = own_seqs * tok_count
    length = tok_count * c_size
    rows = own_seqs * length
    head_dim = HEAD_DIM
    scale = head_dim ** (-0.5)
    row_block = qkv_weight.shape[0]
    cols = qkv_weight.shape[2] // ratio
    hidden_cols = fc1_weight.shape[1] // ratio
    heads = cols // head_dim
    c_index = lax.axis_index("ctx")

    vec = norm_gain.shape[0]
    vec1 = fc1_bias.shape[0]
    def lanes(array):
        array = array.reshape(-1, min(array.shape[-1], 128))
        return jnp.pad(array, ((0, 0), (0, 128 - array.shape[1])))

    small = jnp.concatenate(
        [
            lanes(v)
            for v in (norm_gain, norm_bias, out_bias, fc2_bias, qkv_bias, fc1_bias)
        ]
    )
    small = jnp.pad(small, ((0, -small.shape[0] % 16), (0, 0)))

    qkv_src = (
        jnp.transpose(qkv_weight.reshape(row_block, 3, ratio, cols), (2, 0, 1, 3))
        .reshape(ratio, row_block, 3 * cols)
    )
    fc1_src = jnp.transpose(fc1_weight.reshape(row_block, ratio, hidden_cols), (1, 0, 2))
    out_src = jnp.transpose(out_weight.reshape(ratio, cols, row_block), (0, 2, 1))
    fc2_src = jnp.transpose(fc2_weight.reshape(ratio, hidden_cols, row_block), (0, 2, 1))

    grad_rows = lax.all_gather(cotangent, "ctx", axis=1, tiled=True).reshape(rows, width)
    tok_all, small_all, qkv_all, fc1_all, fc2_all, out_all = gather_call(
        f_size,
        c_size,
        [tokens.reshape(own_rows, width)],
        [qkv_src, fc1_src, fc2_src, out_src],
        small,
        0,
    )

    def rows_of(gathered):
        return jnp.swapaxes(gathered.reshape(c_size, own_seqs, tok_count, width), 0, 1).reshape(
            rows, width
        )

    def blocks_of(array):
        return jnp.swapaxes(array.reshape(own_seqs, c_size, tok_count, width), 0, 1).reshape(
            c_size, own_rows, width
        )

    x_rows = rows_of(tok_all)
    qkv_w = qkv_all.reshape(width, 3 * cols)
    fc1_w = fc1_all.reshape(width, hidden_cols)
    out_t = out_all.reshape(width, cols)
    fc2_t = fc2_all.reshape(width, hidden_cols)

    vectors = small_all.reshape(devices, -1, 128)
    gain_full = vectors[:, 0, :vec].reshape(-1).astype(F32)
    shift_full = vectors[:, 1, :vec].reshape(-1).astype(F32)
    out_bias_full = vectors[:, 2, :vec].reshape(-1).astype(F32)
    fc2_bias_full = vectors[:, 3, :vec].reshape(-1).astype(F32)
    qkv_bias_full = jnp.swapaxes(vectors[:, 4:7, :vec], 0, 1).reshape(3, -1)
    lane = min(vec1, 128)
    fc1_bias_full = vectors[:, 7 : 7 + vec1 // lane, :lane].reshape(-1)
    qkv_b = (
        lax.dynamic_slice_in_dim(qkv_bias_full, c_index * cols, cols, 1).reshape(-1).astype(F32)
    )
    fc1_b = lax.dynamic_slice_in_dim(fc1_bias_full, c_index * hidden_cols, hidden_cols, 0).astype(
        F32
    )

    normed, _ = normed_of(x_rows.astype(F32))
    hidden_in = (normed * gain_full + shift_full).astype(BF16)
    mixed = jnp.dot(hidden_in, qkv_w, preferred_element_type=F32) + qkv_b
    cosine, sine = rope_tables(length, ROT_DIM)

    def heads_of(array):
        return array.reshape(own_seqs, length, heads, head_dim)

    query = rotate_pairs(heads_of(mixed[:, :cols]), cosine, sine, ROT_DIM, 1.0).astype(BF16)
    key = rotate_pairs(heads_of(mixed[:, cols : 2 * cols]), cosine, sine, ROT_DIM, 1.0).astype(
        BF16
    )
    value = heads_of(mixed[:, 2 * cols :].astype(BF16))
    forward = [attention_forward(query[s], key[s], value[s], scale) for s in range(own_seqs)]
    context_b = jnp.stack([pair[0] for pair in forward]).astype(BF16)
    context_rows = context_b.reshape(rows, cols)
    pre = jnp.dot(hidden_in, fc1_w, preferred_element_type=F32) + fc1_b
    act, slope = gelu_both(pre)
    act_b = act.astype(BF16)
    contract_last = (((1,), (1,)), ((), ()))
    partial_out = lax.dot_general(
        context_rows, out_t, contract_last, preferred_element_type=F32
    ) + lax.dot_general(act_b, fc2_t, contract_last, preferred_element_type=F32)

    pre_grad = jnp.dot(grad_rows, fc2_t, preferred_element_type=F32) * slope
    pre_grad_b = pre_grad.astype(BF16)
    contract_first = (((0,), (0,)), ((), ()))

    def weight_grad(left, right):
        product = lax.dot_general(left, right, contract_first, preferred_element_type=F32)
        return product.astype(BF16).reshape(ratio, f_size, row_block, right.shape[1])

    fc2_grad = weight_grad(grad_rows, act_b)
    fc1_grad = weight_grad(hidden_in, pre_grad_b)
    out_grad = weight_grad(grad_rows, context_rows)
    fc1_b_grad = jnp.sum(pre_grad, axis=0)
    mlp_back = lax.dot_general(pre_grad_b, fc1_w, contract_last, preferred_element_type=F32)
    context_grad = heads_of(jnp.dot(grad_rows, out_t, preferred_element_type=F32).astype(BF16))
    delta = jnp.swapaxes(
        jnp.sum(context_grad.astype(F32) * context_b.astype(F32), axis=-1), 1, 2
    )
    grads = [
        attention_backward(
            query[s], key[s], value[s], context_grad[s], delta[s], forward[s][1], scale
        )
        for s in range(own_seqs)
    ]
    query_grad, key_grad, value_grad = [jnp.stack(parts) for parts in zip(*grads)]
    mixed_grad = jnp.concatenate(
        [
            rotate_pairs(query_grad, cosine, sine, ROT_DIM, -1.0).reshape(rows, cols),
            rotate_pairs(key_grad, cosine, sine, ROT_DIM, -1.0).reshape(rows, cols),
            value_grad.reshape(rows, cols),
        ],
        axis=1,
    )
    mixed_grad_b = mixed_grad.astype(BF16)
    qkv_grad = weight_grad(hidden_in, mixed_grad_b)
    qkv_b_grad = jnp.sum(mixed_grad, axis=0).reshape(3, cols)
    normed_part = (
        lax.dot_general(mixed_grad_b, qkv_w, contract_last, preferred_element_type=F32) + mlp_back
    )
    branch = (
        lax.psum_scatter(
            partial_out.astype(BF16).reshape(own_seqs, length, width),
            "ctx",
            scatter_dimension=1,
            tiled=True,
        )
        .reshape(own_rows, width)
        .astype(F32)
    )
    (normed_grad,), (fc2_shard, fc1_shard, out_shard, qkv_shard) = reduce_call(
        f_size,
        c_size,
        [blocks_of(normed_part.astype(BF16))],
        [fc2_grad, fc1_grad, out_grad, qkv_grad],
        2,
    )

    x_own = tokens.reshape(own_rows, width).astype(F32)
    cot_own = cotangent.reshape(own_rows, width).astype(F32)
    output = (x_own + branch + out_bias_full + fc2_bias_full).astype(BF16)
    normed_own, inv_std_own = normed_of(x_own)
    hat_grad = normed_grad * gain_full
    back_rows = inv_std_own * (
        hat_grad
        - jnp.mean(hat_grad, axis=-1, keepdims=True)
        - normed_own * jnp.mean(hat_grad * normed_own, axis=-1, keepdims=True)
    )
    input_grad = (back_rows + cot_own).astype(BF16)

    def whole(block, full, axis):
        return lax.dynamic_update_slice_in_dim(
            jnp.zeros(full, F32), block, c_index * block.shape[axis], axis
        )

    grad_gain = jnp.sum(normed_grad * normed_own, axis=0).reshape(devices, vec)
    grad_shift = jnp.sum(normed_grad, axis=0).reshape(devices, vec)
    grad_cot = jnp.sum(cot_own, axis=0).reshape(devices, vec)
    q_parts = jnp.swapaxes(whole(qkv_b_grad, (3, width), 1).reshape(3, devices, vec), 0, 1)
    f_parts = whole(fc1_b_grad, (vec1 * devices,), 0).reshape(devices, vec1)
    tiles = jnp.concatenate(
        [grad_gain, grad_shift, grad_cot, q_parts.reshape(devices, 3 * vec), f_parts], axis=1
    )
    used = tiles.shape[1]
    tiles = jnp.pad(tiles, ((0, 0), (0, -used % 1024))).reshape(devices, -1, 128)
    sums = small_call(f_size, c_size, tiles, 4).reshape(-1)

    qkv_out = jnp.transpose(
        qkv_shard.reshape(ratio, row_block, 3, cols), (1, 2, 0, 3)
    ).reshape(row_block, 3, ratio * cols)
    fc1_out = jnp.swapaxes(fc1_shard, 0, 1).reshape(row_block, ratio * hidden_cols)
    out_out = jnp.swapaxes(out_shard, 1, 2).reshape(ratio * cols, row_block)
    fc2_out = jnp.swapaxes(fc2_shard, 1, 2).reshape(ratio * hidden_cols, row_block)
    return (
        output.reshape(own_seqs, tok_count, width),
        input_grad.reshape(own_seqs, tok_count, width),
        sums[:vec],
        sums[vec : 2 * vec],
        qkv_out.astype(F32),
        sums[3 * vec : 6 * vec].reshape(3, vec),
        out_out.astype(F32),
        sums[2 * vec : 3 * vec],
        fc1_out.astype(F32),
        sums[6 * vec : 6 * vec + vec1],
        fc2_out.astype(F32),
        sums[2 * vec : 3 * vec],
    )


def solution(mesh):
    row = P("fsdp", "ctx", None)
    vector = P(("fsdp", "ctx"))
    return jax.shard_map(
        body,
        mesh=mesh,
        in_specs=(
            row,
            vector,
            vector,
            P("ctx", None, "fsdp"),
            P(None, ("fsdp", "ctx")),
            P("fsdp", "ctx"),
            vector,
            P("ctx", "fsdp"),
            vector,
            P("fsdp", "ctx"),
            vector,
            row,
        ),
        out_specs=(
            row,
            row,
            vector,
            vector,
            P("ctx", None, "fsdp"),
            P(None, ("fsdp", "ctx")),
            P("fsdp", "ctx"),
            vector,
            P("ctx", "fsdp"),
            vector,
            P("fsdp", "ctx"),
            vector,
        ),
        check_vma=False,
    )
```

```python
import functools
import math

import jax
import jax.numpy as jnp
import numpy as np
from jax import lax
from jax.experimental import pallas as pl
from jax.experimental.pallas import tpu as pltpu
from jax.sharding import PartitionSpec as P

HEAD_DIM = 64
ROT_DIM = 32
NORM_EPS = 1e-05
GELU_COEF = math.sqrt(2.0 / math.pi)
MASKED = -1e30
LOW = 2
F32 = jnp.float32
BF16 = jnp.bfloat16
ANY = pl.BlockSpec(memory_space=pl.ANY)
VMEM = pl.BlockSpec(memory_space=pltpu.VMEM)


class Axis:
    def __init__(self, name, size):
        self.name = name
        self.size = size
        self.low = LOW
        self.high = size // LOW
        self.me = lax.axis_index(name)
        self.hi = lax.div(self.me, LOW)
        self.lo = lax.rem(self.me, LOW)
        self.partner = self.hi * LOW + (1 - self.lo)

    def at(self, hi, lo):
        return hi * LOW + lo

    def ahead(self, steps):
        return self.at(lax.rem(self.hi + steps, self.high), self.lo)

    def behind(self, steps):
        return self.at(lax.rem(self.hi + self.high - steps, self.high), self.lo)

    def behind_other(self, steps):
        return self.at(lax.rem(self.hi + self.high - steps, self.high), 1 - self.lo)


def remote(src, dst, send_sem, recv_sem, axis, index):
    return pltpu.make_async_remote_copy(
        src_ref=src,
        dst_ref=dst,
        send_sem=send_sem,
        recv_sem=recv_sem,
        device_id={axis.name: index},
        device_id_type=pl.DeviceIdType.MESH,
    )


def arrived(dst, sem):
    pltpu.make_async_copy(dst, dst, sem).wait()


class Spread:
    def __init__(self, axis, slot, source, send_hi, recv_hi, send_lo, recv_lo):
        self.axis, self.slot, self.source = axis, slot, source
        self.send_hi, self.recv_hi, self.send_lo, self.recv_lo = send_hi, recv_hi, send_lo, recv_lo

    def copy_hi(self, step):
        ax = self.axis
        return remote(
            self.source,
            self.slot(ax.me),
            self.send_hi.at[step - 1],
            self.recv_hi.at[step - 1],
            ax,
            ax.ahead(step),
        )

    def copy_lo(self, step):
        ax = self.axis
        held = ax.behind(step)
        src = self.source if step == 0 else self.slot(held)
        return remote(
            src, self.slot(held), self.send_lo.at[step], self.recv_lo.at[step], ax, ax.partner
        )

    def start(self):
        for step in range(1, self.axis.high):
            self.copy_hi(step).start()
        self.copy_lo(0).start()

    def forward(self, step):
        arrived(self.slot(self.axis.behind(step)), self.recv_hi.at[step - 1])
        self.copy_lo(step).start()

    def finish(self):
        for step in range(self.axis.high):
            arrived(self.slot(self.axis.behind_other(step)), self.recv_lo.at[step])
        for step in range(1, self.axis.high):
            self.copy_hi(step).wait_send()
        for step in range(self.axis.high):
            self.copy_lo(step).wait_send()


def spread_sems(axis_size):
    high = axis_size // LOW
    return [
        pltpu.SemaphoreType.DMA((max(high - 1, 1),)),
        pltpu.SemaphoreType.DMA((max(high - 1, 1),)),
        pltpu.SemaphoreType.DMA((high,)),
        pltpu.SemaphoreType.DMA((high,)),
    ]


class Line:
    def __init__(self, axis, slot, source, *sems):
        self.axis, self.slot, self.source = axis, slot, source
        self.send_up, self.recv_up, self.send_down, self.recv_down, self.send_lo, self.recv_lo = (
            sems
        )

    def copy(self, hi, sends, recvs, target):
        ax = self.axis
        block = ax.at(hi, ax.lo)
        src = self.source if hi is ax.hi else self.slot(block)
        return remote(src, self.slot(block), sends.at[hi], recvs.at[hi], ax, target)

    def up(self, hi):
        return self.copy(hi, self.send_up, self.recv_up, self.axis.me + LOW)

    def down(self, hi):
        return self.copy(hi, self.send_down, self.recv_down, self.axis.me - LOW)

    def across(self, hi):
        return self.copy(hi, self.send_lo, self.recv_lo, self.axis.partner)

    def start(self):
        ax = self.axis

        @pl.when(ax.hi < ax.high - 1)
        def _():
            self.up(ax.hi).start()

        @pl.when(ax.hi > 0)
        def _():
            self.down(ax.hi).start()

        self.across(ax.hi).start()

    def forward(self, step):
        ax = self.axis

        @pl.when(ax.hi >= step)
        def _():
            held = ax.hi - step
            arrived(self.slot(ax.at(held, ax.lo)), self.recv_up.at[held])

            @pl.when(ax.hi < ax.high - 1)
            def _():
                self.up(held).start()

            self.across(held).start()

        @pl.when(ax.hi + step < ax.high)
        def _():
            held = ax.hi + step
            arrived(self.slot(ax.at(held, ax.lo)), self.recv_down.at[held])

            @pl.when(ax.hi > 0)
            def _():
                self.down(held).start()

            self.across(held).start()

    def finish(self):
        ax = self.axis
        for hi in range(ax.high):
            arrived(self.slot(ax.at(hi, 1 - ax.lo)), self.recv_lo.at[hi])
        for step in range(ax.high):

            @pl.when(jnp.logical_and(ax.hi >= step, ax.hi < ax.high - 1))
            def _(step=step):
                self.up(ax.hi if step == 0 else ax.hi - step).wait_send()

            @pl.when(jnp.logical_and(ax.hi + step < ax.high, ax.hi > 0))
            def _(step=step):
                self.down(ax.hi if step == 0 else ax.hi + step).wait_send()

            @pl.when(ax.hi >= step)
            def _(step=step):
                self.across(ax.hi if step == 0 else ax.hi - step).wait_send()

            if step > 0:

                @pl.when(ax.hi + step < ax.high)
                def _(step=step):
                    self.across(ax.hi + step).wait_send()


def line_sems(axis_size):
    return [pltpu.SemaphoreType.DMA((axis_size // LOW,))] * 6


def meet_everyone(fs, cx):
    barrier = pltpu.get_barrier_semaphore()
    total = fs.size * cx.size
    me = fs.me * cx.size + cx.me

    def signal(step, carry):
        other = lax.rem(me + step, total)
        pl.semaphore_signal(
            barrier,
            inc=1,
            device_id={fs.name: lax.div(other, cx.size), cx.name: lax.rem(other, cx.size)},
            device_id_type=pl.DeviceIdType.MESH,
        )
        return carry

    lax.fori_loop(1, total, signal, 0)
    pl.semaphore_wait(barrier, total - 1)


def shift_of(f_index, f_size):
    return lax.rem(f_index, LOW) * (f_size // LOW) + lax.div(f_index, LOW)


def unshift(shift, f_size):
    return lax.rem(shift, f_size // LOW) * LOW + lax.div(shift, f_size // LOW)


def low_slot(fs, column, device):
    return lax.rem(device + fs.size - shift_of(column, fs.size), fs.size)


def gather_kernel(n_act, n_w, fused, f_size, c_size, *refs):
    fs, cx = Axis("fsdp", f_size), Axis("ctx", c_size)
    ratio = c_size // f_size
    total = f_size * c_size
    me = fs.me * c_size + cx.me
    n_extra = 2 if fused else 0
    n_in = n_act + 1 + n_w + n_extra
    ins, refs = refs[:n_in], refs[n_in:]
    acts, small_own, w_srcs = ins[:n_act], ins[n_act], ins[n_act + 1 : n_act + 1 + n_w]
    n_out = n_act + 1 + n_w + (5 if fused else 0)
    outs, rest = refs[:n_out], list(refs[n_out:])
    act_outs, small_out, w_outs = outs[:n_act], outs[n_act], outs[n_act + 1 : n_act + 1 + n_w]
    if fused:
        tables = ins[n_act + 1 + n_w :]
        query, key, value, context, lse = outs[n_act + 1 + n_w :]
    small_send, small_recv = rest[:2]
    rest = rest[2:]
    own_sem = rest.pop(0)
    lines = []
    for index in range(n_act):
        out = act_outs[index]
        slot = lambda c, out=out: out.at[c]
        source = slot(cx.me) if fused and index == 0 else acts[index]
        lines.append(Line(cx, slot, source, *rest[:6]))
        rest = rest[6:]
    mids, rest = rest[:n_w], rest[n_w:]
    mid_send, mid_recv, w_send, w_recv = rest[:4]
    rest = rest[4:]
    column = lax.div(cx.me, ratio)
    spreads = []
    for index in range(n_w):
        out = w_outs[index]
        slot = lambda f, out=out: out.at[:, low_slot(fs, column, f)]
        spreads.append(Spread(fs, slot, slot(fs.me), *rest[:4]))
        rest = rest[4:]
    pass_to = lax.rem(cx.me + shift_of(fs.me, f_size), f_size)
    pass_from = unshift(lax.rem(fs.me + f_size - lax.rem(cx.me, f_size), f_size), f_size)
    stays = pass_to == fs.me
    row_hi, row_lo = lax.div(cx.me, f_size), lax.rem(cx.me, f_size)

    def move(index):
        src, dst = w_srcs[index], mids[index]
        away = lambda: remote(src, dst, mid_send.at[index], mid_recv.at[index], fs, pass_to)
        here = lambda: pltpu.make_async_copy(src, dst, mid_recv.at[index])
        return away, here

    def scatter(index, i):
        to_c = pass_from * ratio + i
        src, dst = mids[index].at[i], w_outs[index].at[row_hi, row_lo]
        sem = w_recv.at[index, row_hi]
        away = lambda: remote(src, dst, w_send.at[index, i], sem, cx, to_c)
        here = lambda: pltpu.make_async_copy(src, dst, sem)
        return to_c == cx.me, away, here

    def either(is_self, away, here):
        @pl.when(is_self)
        def _():
            here().start()

        @pl.when(jnp.logical_not(is_self))
        def _():
            away().start()

    def start_moves():
        for index in range(n_w):
            either(stays, *move(index))

    def start_scatter(index):
        arrived(mids[index], mid_recv.at[index])
        for i in range(ratio):
            either(*scatter(index, i))

    def start_spread(index):
        for hi in range(ratio):
            arrived(w_outs[index].at[hi, low_slot(fs, column, fs.me)], w_recv.at[index, hi])
        spreads[index].start()

    def forward_spread(index):
        for step in range(1, fs.high):
            spreads[index].forward(step)

    def small_copy(step):
        other = lax.rem(me + step, total)
        return pltpu.make_async_remote_copy(
            src_ref=small_own,
            dst_ref=small_out.at[me],
            send_sem=small_send.at[step - 1],
            recv_sem=small_recv.at[me],
            device_id={fs.name: lax.div(other, c_size), cx.name: lax.rem(other, c_size)},
            device_id_type=pl.DeviceIdType.MESH,
        )

    def small_start(step, carry):
        small_copy(step).start()
        return carry

    def small_wait(step, carry):
        other = lax.rem(me + step, total)
        arrived(small_out.at[other], small_recv.at[other])
        return carry

    def small_drain(step, carry):
        small_copy(step).wait_send()
        return carry

    def vector(row, first, chunks, per):
        parts = []
        for chunk in range(chunks):
            part = small_out[first + chunk * per, row : row + 1, :].astype(F32)
            for more in range(1, per):
                part = part + small_out[first + chunk * per + more, row : row + 1, :].astype(F32)
            parts.append(part)
        return jnp.concatenate(parts, axis=1)

    def normalise():
        width = acts[0].shape[1]
        chunks = width // 128
        gain = vector(0, 0, chunks, total // chunks)
        shift = vector(1, 0, chunks, total // chunks)

        def step(i, carry):
            rows = pl.ds(pl.multiple_of(i * 32, 32), 32)
            x = acts[0][rows, :].astype(F32)
            centred = x - jnp.mean(x, axis=-1, keepdims=True)
            inv_std = lax.rsqrt(jnp.mean(centred * centred, axis=-1, keepdims=True) + NORM_EPS)
            act_outs[0][cx.me, rows, :] = (centred * inv_std * gain + shift).astype(BF16)
            return carry

        lax.fori_loop(0, acts[0].shape[0] // 32, step, 0)

    def project():
        rows, width = acts[0].shape
        cols = query.shape[1]
        per = total * cols // width
        first = cx.me * per
        bias = [vector(4 + part, first, cols // 128, per * 128 // cols) for part in range(3)]

        def step(i, carry):
            x = act_outs[0][pl.ds(2 * i, 2)].reshape(2 * rows, width)
            span = pl.ds(pl.multiple_of(i * 2 * rows, 2 * rows), 2 * rows)
            straight, swing = [table[span, :] for table in tables]
            for part, out in enumerate((query, key, value)):
                w = w_outs[0][:, :, :, part * cols : (part + 1) * cols].reshape(width, cols)
                y = jnp.dot(x, w, preferred_element_type=F32) + bias[part]
                for lane in range(0, cols, 128):
                    half = y[:, lane : lane + 128]
                    if part < 2:
                        half = turn(half, straight, swing, 1.0)
                    out[span, lane : lane + 128] = half.astype(BF16)
            return carry

        lax.fori_loop(0, c_size // 2, step, 0)

    def attend(head):
        length = query.shape[0]
        block = math.gcd(length, 256)
        lanes = slice(head * HEAD_DIM, (head + 1) * HEAD_DIM)
        last_two = (((1,), (1,)), ((), ()))
        for first in range(0, length, block):
            last = first + block
            scores = (
                lax.dot_general(
                    query[first:last, lanes],
                    key[:last, lanes],
                    last_two,
                    preferred_element_type=F32,
                )
                * HEAD_DIM ** (-0.5)
            )
            row = lax.broadcasted_iota(jnp.int32, (block, last), 0) + first
            col = lax.broadcasted_iota(jnp.int32, (block, last), 1)
            scores = jnp.where(col <= row, scores, MASKED)
            top = jnp.max(scores, axis=-1, keepdims=True)
            weights = jnp.exp(scores - top)
            summed = jnp.sum(weights, axis=-1, keepdims=True)
            mixed = jnp.dot(weights.astype(BF16), value[:last, lanes], preferred_element_type=F32)
            context[first:last, lanes] = (mixed / summed).astype(BF16)
            lse[first:last, head : head + 1] = top + jnp.log(summed)

    meet_everyone(fs, cx)
    lax.fori_loop(1, total, small_start, 0)
    start_moves()
    own = {}
    small_own_copy = pltpu.make_async_copy(small_own, small_out.at[me], own_sem.at[n_act])
    small_own_copy.start()
    for index in range(n_act):
        if not (fused and index == 0):
            own[index] = pltpu.make_async_copy(
                acts[index], lines[index].slot(cx.me), own_sem.at[index]
            )
            own[index].start()
            lines[index].start()
    small_own_copy.wait()
    lax.fori_loop(1, total, small_wait, 0)
    if fused:
        normalise()
        lines[0].start()

    scatters = [functools.partial(start_scatter, index) for index in range(n_w)]
    starts = [functools.partial(start_spread, index) for index in range(n_w)]
    lasts = [functools.partial(forward_spread, index) for index in range(n_w)]
    rows = [
        [functools.partial(lines[index].forward, step) for step in range(1, cx.high)]
        for index in range(n_act)
    ]
    comm = [scatters.pop(0)] + [more[0] for more in rows[1:]] + [scatters.pop(0), rows[0][0]]
    comm += scatters
    comm += rows[0][1:2] + [starts[0]] + [more[1] for more in rows[1:] if len(more) > 1]
    comm += [starts[1], lasts[0]] + rows[0][2:]
    for work in comm:
        work()
    comm = []
    for index in range(2, n_w):
        comm += [starts[index], lasts[index - 1]]
    comm += [work for more in rows[1:] for work in more[2:]] + [lasts[-1]]
    lines[0].finish()
    spreads[0].finish()
    if fused:
        compute = [project]
        compute += [functools.partial(attend, head) for head in range(lse.shape[1])]
        for work in compute:
            if comm:
                comm.pop(0)()
            if comm and work is project:
                comm.pop(0)()
            work()
    for work in comm:
        work()
    for index in own:
        own[index].wait()
    for index in range(1, n_act):
        lines[index].finish()
    for index in range(n_w):
        if index > 0:
            spreads[index].finish()

        @pl.when(jnp.logical_not(stays))
        def _(index=index):
            move(index)[0]().wait_send()

        for i in range(ratio):
            is_self, away, here = scatter(index, i)

            @pl.when(jnp.logical_not(is_self))
            def _(away=away):
                away().wait_send()

    lax.fori_loop(1, total, small_drain, 0)


def gather_call(f_size, c_size, acts, small, w_srcs, tables, collective_id):
    ratio = c_size // f_size
    total = f_size * c_size
    fused = tables is not None
    ins = [*acts, small, *w_srcs] + (list(tables) if fused else [])
    shapes = [jax.ShapeDtypeStruct((c_size, *a.shape), a.dtype) for a in acts]
    shapes.append(jax.ShapeDtypeStruct((total, *small.shape), small.dtype))
    for w in w_srcs:
        shapes.append(jax.ShapeDtypeStruct((ratio, f_size, *w.shape[1:]), w.dtype))
    specs = [ANY] * len(shapes)
    specs[len(acts)] = VMEM
    if fused:
        specs[0] = specs[len(acts) + 1] = VMEM
        length, cols = c_size * acts[0].shape[0], w_srcs[0].shape[2] // 3
        shapes += [jax.ShapeDtypeStruct((length, cols), BF16)] * 4
        shapes.append(jax.ShapeDtypeStruct((length, cols // HEAD_DIM), F32))
        specs += [VMEM] * 5
    scratch = [pltpu.SemaphoreType.DMA((total - 1,)), pltpu.SemaphoreType.DMA((total,))]
    scratch.append(pltpu.SemaphoreType.DMA((len(acts) + 1,)))
    for _ in acts:
        scratch += line_sems(c_size)
    scratch += [pltpu.VMEM(w.shape, w.dtype) for w in w_srcs]
    scratch += [pltpu.SemaphoreType.DMA((len(w_srcs),))] * 2
    scratch += [pltpu.SemaphoreType.DMA((len(w_srcs), ratio))] * 2
    for _ in w_srcs:
        scratch += spread_sems(f_size)
    return pl.pallas_call(
        functools.partial(gather_kernel, len(acts), len(w_srcs), fused, f_size, c_size),
        out_shape=tuple(shapes),
        in_specs=[VMEM] * len(ins),
        out_specs=tuple(specs),
        scratch_shapes=scratch,
        compiler_params=pltpu.CompilerParams(collective_id=collective_id, has_side_effects=True),
        name=f"gather_{collective_id}",
    )(*ins)


def add_into(dst, terms):
    rows = dst.shape[-2]
    lead = dst.shape[:-2]
    chunk = math.gcd(rows, 32)

    def at(ref, index, start):
        return (*index, pl.ds(start, chunk), slice(None))

    for index in [()] if not lead else [(i,) for i in range(lead[0])]:

        def step(i, carry, index=index):
            start = pl.multiple_of(i * chunk, chunk)
            total = terms[0][at(terms[0], index, start)].astype(F32)
            for term in terms[1:]:
                total = total + term[at(term, index, start)].astype(F32)
            dst[at(dst, index, start)] = total.astype(dst.dtype)
            return carry

        lax.fori_loop(0, rows // chunk, step, 0)


class Fold:
    def __init__(self, axis, block, from_lo, from_hi, *sems):
        self.axis, self.block, self.result = axis, block, from_lo.at[0]
        self.from_lo, self.from_hi = from_lo, from_hi
        self.send_lo, self.recv_lo, self.send_hi, self.recv_hi = sems

    def copy_lo(self, step):
        ax = self.axis
        hi = lax.rem(ax.hi + step, ax.high)
        return remote(
            self.block(ax.at(hi, 1 - ax.lo)),
            self.from_lo.at[step],
            self.send_lo.at[step],
            self.recv_lo.at[step],
            ax,
            ax.partner,
        )

    def copy_hi(self, step):
        ax = self.axis
        return remote(
            self.from_lo.at[step],
            self.from_hi.at[step - 1],
            self.send_hi.at[step - 1],
            self.recv_hi.at[step - 1],
            ax,
            ax.ahead(step),
        )

    def start(self):
        for step in list(range(1, self.axis.high)) + [0]:
            self.copy_lo(step).start()

    def forward(self, step):
        arrived(self.from_lo.at[step], self.recv_lo.at[step])
        add_into(
            self.from_lo.at[step], [self.block(self.axis.ahead(step)), self.from_lo.at[step]]
        )
        self.copy_hi(step).start()

    def finish(self):
        arrived(self.from_lo.at[0], self.recv_lo.at[0])
        terms = [self.block(self.axis.me), self.from_lo.at[0]]
        for step in range(1, self.axis.high):
            arrived(self.from_hi.at[step - 1], self.recv_hi.at[step - 1])
            terms.append(self.from_hi.at[step - 1])
        add_into(self.result, terms)

    def drain(self):
        for step in range(self.axis.high):
            self.copy_lo(step).wait_send()
        for step in range(1, self.axis.high):
            self.copy_hi(step).wait_send()


class LineFold:
    def __init__(self, axis, block, own, result, from_lo, from_z, from_end, *sems):
        self.axis, self.block, self.own, self.result = axis, block, own, result
        self.from_lo, self.from_z, self.from_end = from_lo, from_z, from_end
        self.send_lo, self.recv_lo, self.send_z, self.recv_z, self.recv_end = sems
        low_end, high_end = jnp.int32(0), jnp.int32(axis.high - 1)
        self.order = []
        for _ in range(axis.high):
            take_low = axis.hi - low_end >= high_end - axis.hi
            self.order.append(jnp.where(take_low, low_end, high_end))
            low_end = jnp.where(take_low, low_end + 1, low_end)
            high_end = jnp.where(take_low, high_end, high_end - 1)

    def across(self, hi):
        ax = self.axis
        return remote(
            self.block(ax.at(hi, 1 - ax.lo)),
            self.from_lo.at[hi],
            self.send_lo.at[hi],
            self.recv_lo.at[hi],
            ax,
            ax.partner,
        )

    def onward(self, hi, up, last):
        ax = self.axis
        side = 0 if up else 1
        dst, sem = (
            (self.from_end.at[side], self.recv_end.at[side])
            if last
            else (self.from_z.at[hi], self.recv_z.at[hi])
        )
        target = ax.me + LOW if up else ax.me - LOW
        return remote(self.from_lo.at[hi], dst, self.send_z.at[hi], sem, ax, target)

    def start(self):
        for hi in self.order:
            self.across(hi).start()

    def pass_on(self, hi, up):
        ax = self.axis
        first = ax.hi == (0 if up else ax.high - 1)
        own = self.own(hi)

        @pl.when(first)
        def _():
            add_into(self.from_lo.at[hi], [own, self.from_lo.at[hi]])

        @pl.when(jnp.logical_not(first))
        def _():
            arrived(self.from_z.at[hi], self.recv_z.at[hi])
            add_into(self.from_lo.at[hi], [own, self.from_lo.at[hi], self.from_z.at[hi]])

        near = ax.hi == (hi - 1 if up else hi + 1)

        @pl.when(near)
        def _():
            self.onward(hi, up, True).start()

        @pl.when(jnp.logical_not(near))
        def _():
            self.onward(hi, up, False).start()

    def forward(self, hi):
        ax = self.axis
        arrived(self.from_lo.at[hi], self.recv_lo.at[hi])

        @pl.when(ax.hi < hi)
        def _():
            self.pass_on(hi, True)

        @pl.when(ax.hi > hi)
        def _():
            self.pass_on(hi, False)

    def finish(self):
        ax = self.axis
        own = [self.own(ax.hi), self.from_lo.at[ax.hi]]
        if ax.high == 1:
            add_into(self.result, own)
            return
        low_end, high_end = ax.hi == 0, ax.hi == ax.high - 1

        @pl.when(jnp.logical_not(low_end))
        def _():
            arrived(self.from_end.at[0], self.recv_end.at[0])

        @pl.when(jnp.logical_not(high_end))
        def _():
            arrived(self.from_end.at[1], self.recv_end.at[1])

        @pl.when(low_end)
        def _():
            add_into(self.result, own + [self.from_end.at[1]])

        @pl.when(high_end)
        def _():
            add_into(self.result, own + [self.from_end.at[0]])

        @pl.when(jnp.logical_not(jnp.logical_or(low_end, high_end)))
        def _():
            add_into(self.result, own + [self.from_end.at[0], self.from_end.at[1]])

    def drain(self):
        ax = self.axis
        for hi in range(ax.high):
            self.across(hi).wait_send()

            @pl.when(ax.hi != hi)
            def _(hi=hi):
                self.onward(hi, True, False).wait_send()


def line_fold_scratch(axis_size, shape, dtype):
    high = axis_size // LOW
    return [
        pltpu.VMEM((high, *shape), dtype),
        pltpu.VMEM((high, *shape), dtype),
        pltpu.VMEM((2, *shape), dtype),
        pltpu.SemaphoreType.DMA((high,)),
        pltpu.SemaphoreType.DMA((high,)),
        pltpu.SemaphoreType.DMA((high,)),
        pltpu.SemaphoreType.DMA((high,)),
        pltpu.SemaphoreType.DMA((2,)),
    ]


def fold_scratch(axis_size, shape, dtype):
    high = axis_size // LOW
    more = max(high - 1, 1)
    return [
        pltpu.VMEM((high, *shape), dtype),
        pltpu.VMEM((more, *shape), dtype),
        pltpu.SemaphoreType.DMA((high,)),
        pltpu.SemaphoreType.DMA((high,)),
        pltpu.SemaphoreType.DMA((more,)),
        pltpu.SemaphoreType.DMA((more,)),
    ]


def reduce_kernel(n_part, n_w, fused, f_size, c_size, *refs):
    fs, cx = Axis("fsdp", f_size), Axis("ctx", c_size)
    ratio = c_size // f_size
    n_late = 1 if fused else 0
    parts, refs = refs[: n_part - n_late], refs[n_part - n_late :]
    grads, refs = refs[: n_w - n_late], refs[n_w - n_late :]
    if fused:
        heads_in, refs = refs[:6], refs[6:]
        straight, swing, qkv_w, hidden, mlp_back = refs[:5]
        refs = refs[5:]
    rows_outs, refs = refs[:n_part], refs[n_part:]
    grad_outs, scratch = refs[:n_w], list(refs[n_w:])
    if fused:
        sums = scratch.pop(0)
        late_part, late_grad, own_rows, own_sem = scratch[:4]
        dq, dk, dv, mixed_grad, tall, tall_sem, wide, wide_sem = scratch[4:12]
        scratch = scratch[12:]
        parts, grads = (*parts, late_part), (*grads, late_grad)
    row_folds = []
    for index in range(n_part):
        block = lambda c, part=parts[index]: part.at[c]
        own = lambda hi, block=block: block(cx.at(hi, cx.lo))
        if fused and index == 0:
            own = lambda hi: own_rows.at[hi]
        row_folds.append(LineFold(cx, block, own, rows_outs[index], *scratch[:8]))
        scratch = scratch[8:]
    column = lax.div(cx.me, ratio)
    folds, totals = [], []
    for index in range(n_w):
        block = lambda f, grad=grads[index]: grad.at[:, low_slot(fs, column, f)]
        totals.append(scratch[0].at[0])
        folds.append(Fold(fs, block, *scratch[:6]))
        scratch = scratch[6:]
    g_send, g_recv = scratch

    meet_everyone(fs, cx)
    for fold in row_folds[: n_part - n_late]:
        fold.start()
    for fold in folds[: n_w - n_late]:
        fold.start()
    own_copies = []
    if fused:
        for hi in range(cx.high):
            own_copies.append(
                pltpu.make_async_copy(
                    parts[0].at[cx.at(hi, cx.lo)], own_rows.at[hi], own_sem.at[hi]
                )
            )
            own_copies[-1].start()

    slot = lax.rem(cx.me, ratio)
    row_lo = low_slot(fs, column, fs.me)

    def deliver(index, hi):
        to_c = hi * f_size + row_lo
        is_self = jnp.logical_and(column == fs.me, to_c == cx.me)
        src = totals[index].at[hi]
        dst = grad_outs[index].at[slot]
        away = lambda: pltpu.make_async_remote_copy(
            src_ref=src,
            dst_ref=dst,
            send_sem=g_send.at[index, hi],
            recv_sem=g_recv.at[index, slot],
            device_id={fs.name: column, cx.name: to_c},
            device_id_type=pl.DeviceIdType.MESH,
        )
        here = lambda: pltpu.make_async_copy(src, dst, g_recv.at[index, slot])
        return is_self, away, here

    def deliver_all(index):
        folds[index].finish()
        for hi in range(ratio):
            is_self, away, here = deliver(index, hi)

            @pl.when(is_self)
            def _(here=here):
                here().start()

            @pl.when(jnp.logical_not(is_self))
            def _(away=away):
                away().start()

    def pass_halves(index):
        for step in range(1, fs.high):
            folds[index].forward(step)

    def row_work(fold):
        return [functools.partial(fold.forward, hi) for hi in fold.order]

    halves = [functools.partial(pass_halves, index) for index in range(n_w)]
    delivers = [functools.partial(deliver_all, index) for index in range(n_w)]

    def column_grads():
        wide_rows = late_grad.shape[2]

        def copy(i):
            at = pl.ds(pl.multiple_of(i * wide_rows, wide_rows), wide_rows)
            slot = lax.rem(i, 2)
            return pltpu.make_async_copy(hidden.at[:, at], tall.at[slot], tall_sem.at[slot])

        copy(0).start()

        def step(i, carry):
            @pl.when(i + 1 < c_size)
            def _():
                copy(i + 1).start()

            copy(i).wait()
            late_grad[lax.div(i, f_size), lax.rem(i, f_size)] = lax.dot_general(
                tall[lax.rem(i, 2)],
                mixed_grad[...],
                (((0,), (0,)), ((), ())),
                preferred_element_type=F32,
            ).astype(BF16)
            return carry

        lax.fori_loop(0, c_size, step, 0)

    def row_grads():
        rows = late_part.shape[1]

        def copy(i):
            slot = lax.rem(i, 2)
            return pltpu.make_async_copy(
                mlp_back.at[pl.ds(2 * i, 2)], wide.at[slot], wide_sem.at[slot]
            )

        copy(0).start()

        def step(i, carry):
            @pl.when(i + 1 < c_size // 2)
            def _():
                copy(i + 1).start()

            copy(i).wait()
            span = pl.ds(pl.multiple_of(2 * i * rows, 2 * rows), 2 * rows)
            total = lax.dot_general(
                mixed_grad[span, :],
                qkv_w[...],
                (((1,), (1,)), ((), ())),
                preferred_element_type=F32,
            )
            total = total.reshape(2, rows, total.shape[1]) + wide[lax.rem(i, 2)]
            late_part[pl.ds(2 * i, 2)] = total.astype(BF16)
            return carry

        lax.fori_loop(0, c_size // 2, step, 0)

    if fused:
        heads = dq.shape[1] // HEAD_DIM
        early = row_work(row_folds[0])
        comm = [early.pop(0), early.pop(0), delivers.pop(0)]
        for work in early:
            comm.append(work)
            if len(delivers) > 1:
                comm.append(delivers.pop(0))
        for work in halves[:-1]:
            work()
        for copy in own_copies:
            copy.wait()
        for head in range(heads):
            backward_head(head, *heads_in, dq, dk, dv)
            if comm:
                comm.pop(0)()
        backward_turn(straight, swing, dq, dk, dv, mixed_grad, sums)
        row_grads()
        row_folds[1].start()
        if comm:
            comm.pop(0)()
        column_grads()
        folds[-1].start()
        for work in comm:
            work()
        halves[-1]()
        for count, work in enumerate(row_work(row_folds[1])):
            work()
            if count >= 1 and delivers:
                delivers.pop(0)()
    else:
        for count, work in enumerate([work for fold in row_folds for work in row_work(fold)]):
            for more in halves[:2]:
                more()
            halves = halves[2:]
            work()
            if count >= 1 and delivers and not halves:
                delivers.pop(0)()
        for work in halves:
            work()
    for work in delivers:
        work()
    for fold in row_folds:
        fold.finish()
    for index in range(n_w):
        for i in range(ratio):
            arrived(grad_outs[index].at[i], g_recv.at[index, i])
    for fold in row_folds:
        fold.drain()
    for index in range(n_w):
        folds[index].drain()
        for hi in range(ratio):
            is_self, away, here = deliver(index, hi)

            @pl.when(jnp.logical_not(is_self))
            def _(away=away):
                away().wait_send()


def reduce_call(f_size, c_size, parts, grads, collective_id, late=None):
    ratio = c_size // f_size
    fused = late is not None
    ins, in_specs = [*parts, *grads], [VMEM] * (len(parts) + len(grads))
    part_shapes = [(part.shape, part.dtype) for part in parts]
    grad_shapes = [(grad.shape, grad.dtype) for grad in grads]
    own = []
    if fused:
        in_specs[0] = ANY
        heads_in, tables, qkv_w, hidden, mlp_back = late
        ins += [*heads_in, *tables, qkv_w, hidden, mlp_back]
        in_specs += [VMEM] * 9 + [ANY] * 2
        length, cols = heads_in[0].shape
        part_shapes.append(part_shapes[0])
        shape, dtype = grad_shapes[0]
        grad_shapes.append(((*shape[:3], 3 * cols), dtype))
        high = c_size // LOW
        own = [
            pltpu.VMEM(*part_shapes[1]),
            pltpu.VMEM(*grad_shapes[-1]),
            pltpu.VMEM((high, *parts[0].shape[1:]), BF16),
            pltpu.SemaphoreType.DMA((high,)),
            pltpu.VMEM((length, cols), F32),
            pltpu.VMEM((length, cols), F32),
            pltpu.VMEM((length, cols), F32),
            pltpu.VMEM((length, 3 * cols), BF16),
            pltpu.VMEM((2, length, shape[2]), BF16),
            pltpu.SemaphoreType.DMA((2,)),
            pltpu.VMEM((2, 2, *mlp_back.shape[1:]), F32),
            pltpu.SemaphoreType.DMA((2,)),
        ]
    shapes, scratch = [], []
    for shape, dtype in part_shapes:
        shapes.append(jax.ShapeDtypeStruct(shape[1:], F32))
        scratch += line_fold_scratch(c_size, shape[1:], dtype)
    for shape, dtype in grad_shapes:
        piece = (ratio, *shape[2:])
        shapes.append(jax.ShapeDtypeStruct(piece, dtype))
        scratch += fold_scratch(f_size, piece, dtype)
    specs = [VMEM] * len(part_shapes) + [ANY] * len(grad_shapes)
    if fused:
        shapes.append(jax.ShapeDtypeStruct((1, 3 * cols), F32))
        specs.append(VMEM)
    scratch += [pltpu.SemaphoreType.DMA((len(grad_shapes), ratio))] * 2
    outs = pl.pallas_call(
        functools.partial(
            reduce_kernel, len(part_shapes), len(grad_shapes), fused, f_size, c_size
        ),
        out_shape=tuple(shapes),
        in_specs=in_specs,
        out_specs=tuple(specs),
        scratch_shapes=own + scratch,
        compiler_params=pltpu.CompilerParams(
            collective_id=collective_id,
            has_side_effects=True,
            vmem_limit_bytes=66_000_000 if fused else None,
        ),
        name=f"reduce_{collective_id}",
    )(*ins)
    n_part, n_w = len(part_shapes), len(grad_shapes)
    return outs[:n_part], outs[n_part : n_part + n_w], outs[n_part + n_w :]


def reduce_all(f_size, c_size, parts, grads):
    size = sum(2.25 * part.size * part.dtype.itemsize for part in parts)
    size += sum(2.5 * grad.size * grad.dtype.itemsize for grad in grads)
    if size <= 56 * 2**20:
        return reduce_call(f_size, c_size, parts, grads, 2)[:2]
    half = len(grads) // 2
    (first,), early, _ = reduce_call(f_size, c_size, parts[:1], grads[:half], 2)
    (second,), late, _ = reduce_call(f_size, c_size, parts[1:], grads[half:], 3)
    return (first, second), (*early, *late)


def small_kernel(f_size, c_size, tiles, out, held, send_sem, recv_sem):
    fs, cx = Axis("fsdp", f_size), Axis("ctx", c_size)
    total = f_size * c_size
    me = fs.me * c_size + cx.me
    meet_everyone(fs, cx)

    def copy(step):
        other = lax.rem(me + step, total)
        return pltpu.make_async_remote_copy(
            src_ref=tiles.at[other],
            dst_ref=held.at[step - 1],
            send_sem=send_sem.at[step - 1],
            recv_sem=recv_sem.at[step - 1],
            device_id={fs.name: lax.div(other, c_size), cx.name: lax.rem(other, c_size)},
            device_id_type=pl.DeviceIdType.MESH,
        )

    def start(step, carry):
        copy(step).start()
        return carry

    lax.fori_loop(1, total, start, 0)

    def collect(step, acc):
        arrived(held.at[step - 1], recv_sem.at[step - 1])
        return acc + held[step - 1]

    out[...] = lax.fori_loop(1, total, collect, tiles[me])

    def drain(step, carry):
        copy(step).wait_send()
        return carry

    lax.fori_loop(1, total, drain, 0)


def small_call(f_size, c_size, tiles, collective_id):
    total = f_size * c_size
    return pl.pallas_call(
        functools.partial(small_kernel, f_size, c_size),
        out_shape=jax.ShapeDtypeStruct(tiles.shape[1:], F32),
        in_specs=[VMEM],
        out_specs=VMEM,
        scratch_shapes=[
            pltpu.VMEM((total - 1, *tiles.shape[1:]), F32),
            pltpu.SemaphoreType.DMA((total - 1,)),
            pltpu.SemaphoreType.DMA((total - 1,)),
        ],
        compiler_params=pltpu.CompilerParams(collective_id=collective_id, has_side_effects=True),
        name=f"small_{collective_id}",
    )(tiles)


def normed_of(rows):
    centred = rows - jnp.mean(rows, axis=-1, keepdims=True)
    inv_std = lax.rsqrt(jnp.mean(centred * centred, axis=-1, keepdims=True) + NORM_EPS)
    return centred * inv_std, inv_std


def gelu_both(values):
    tangent = jnp.tanh(GELU_COEF * (values + 0.044715 * values * values * values))
    act = 0.5 * values * (1.0 + tangent)
    slope = 0.5 * (1.0 + tangent) + 0.5 * values * (1.0 - tangent * tangent) * GELU_COEF * (
        1.0 + 3.0 * 0.044715 * values * values
    )
    return act, slope


def rope_tables(count, rot_dim):
    positions = jnp.arange(count, dtype=F32)
    half_dim = rot_dim // 2
    inverse = 10000.0 ** (-(jnp.arange(half_dim, dtype=F32) * 2.0) / rot_dim)
    angles = positions[:, None] * inverse[None, :]
    return (jnp.cos(angles)[:, None, :], jnp.sin(angles)[:, None, :])


def rotate_pairs(values, cosine, sine, rot_dim, sign):
    half_dim = rot_dim // 2
    first_half = values[..., :half_dim]
    second_half = values[..., half_dim:rot_dim]
    return jnp.concatenate(
        [
            first_half * cosine - sign * second_half * sine,
            second_half * cosine + sign * first_half * sine,
            values[..., rot_dim:],
        ],
        axis=-1,
    )


def lane_tables(count):
    half_dim = ROT_DIM // 2
    inverse = np.float32(10000.0) ** (-(np.arange(half_dim, dtype=np.float32) * 2.0) / ROT_DIM)
    angles = np.arange(count, dtype=np.float32)[:, None] * inverse.astype(np.float32)[None, :]
    cosine, sine = np.cos(angles.astype(np.float64)), np.sin(angles.astype(np.float64))
    rest = np.zeros((count, HEAD_DIM - ROT_DIM))
    straight = np.concatenate([cosine, cosine, rest + 1.0] * (128 // HEAD_DIM), axis=1)
    swing = np.concatenate([-sine, sine, rest] * (128 // HEAD_DIM), axis=1)
    return [jnp.asarray(table.astype(np.float32)) for table in (straight, swing)]


def turn(values, straight, swing, sign):
    half_dim = ROT_DIM // 2
    lane = lax.broadcasted_iota(jnp.int32, values.shape, 1)
    first = lax.rem(lane, HEAD_DIM) < half_dim
    other = jnp.where(
        first, pltpu.roll(values, 128 - half_dim, 1), pltpu.roll(values, half_dim, 1)
    )
    return values * straight + sign * other * swing


def backward_head(head, query, key, value, context, context_grad, lse, dq, dk, dv):
    length = query.shape[0]
    block = math.gcd(length, 256)
    scale = HEAD_DIM ** (-0.5)
    last_two = (((1,), (1,)), ((), ()))
    first_two = (((0,), (0,)), ((), ()))

    def dot(left, right, dims):
        return lax.dot_general(left, right, dims, preferred_element_type=F32)

    lanes = slice(head * HEAD_DIM, (head + 1) * HEAD_DIM)
    for first in reversed(range(0, length, block)):
        last = first + block
        q, g = query[first:last, lanes], context_grad[first:last, lanes]
        k, v = key[:last, lanes], value[:last, lanes]
        delta = jnp.sum(
            g.astype(F32) * context[first:last, lanes].astype(F32), axis=-1, keepdims=True
        )
        scores = dot(q, k, last_two) * scale
        row = lax.broadcasted_iota(jnp.int32, (block, last), 0) + first
        col = lax.broadcasted_iota(jnp.int32, (block, last), 1)
        probs = jnp.where(col <= row, jnp.exp(scores - lse[first:last, head : head + 1]), 0.0)
        score_grad = (probs * (dot(g, v, last_two) - delta)).astype(BF16)
        value_grad = dot(probs.astype(BF16), g, first_two)
        key_grad = dot(score_grad, q, first_two) * scale
        dq[first:last, lanes] = dot(score_grad, k, (((1,), (0,)), ((), ()))) * scale
        if last == length:
            dv[:, lanes] = value_grad
            dk[:, lanes] = key_grad
        else:
            dv[:last, lanes] += value_grad
            dk[:last, lanes] += key_grad


def backward_turn(straight, swing, dq, dk, dv, out, sums):
    length, cols = dq.shape
    block = math.gcd(length, 256)
    for part, grad in enumerate((dq, dk, dv)):
        for lane in range(0, cols, 128):
            at = part * cols + lane

            def step(i, total, grad=grad, lane=lane, at=at, part=part):
                rows = pl.ds(pl.multiple_of(i * block, block), block)
                values = grad[rows, lane : lane + 128]
                if part < 2:
                    values = turn(values, straight[rows, :], swing[rows, :], -1.0)
                out[rows, at : at + 128] = values.astype(BF16)
                return total + jnp.sum(values, axis=0, keepdims=True)

            sums[:, at : at + 128] = lax.fori_loop(
                0, length // block, step, jnp.zeros((1, 128), F32)
            )


def attention_forward(query, key, value, scale):
    length = query.shape[0]
    block = math.gcd(length, 256)
    contexts, lses = [], []
    for first in range(0, length, block):
        last = first + block
        scores = (
            jnp.einsum("qhd,khd->hqk", query[first:last], key[:last], preferred_element_type=F32)
            * scale
        )
        allowed = jnp.arange(last)[None, :] <= (first + jnp.arange(block))[:, None]
        scores = jnp.where(allowed, scores, MASKED)
        top = jnp.max(scores, axis=-1)
        weights = jnp.where(allowed, jnp.exp(scores - top[..., None]), 0.0)
        total = jnp.sum(weights, axis=-1)
        context = jnp.einsum(
            "hqk,khd->qhd", weights.astype(BF16), value[:last], preferred_element_type=F32
        )
        contexts.append(context / jnp.transpose(total)[..., None])
        lses.append(top + jnp.log(total))
    return jnp.concatenate(contexts, axis=0), jnp.concatenate(lses, axis=1)


def attention_backward(query, key, value, context_grad, delta, lse, scale):
    length, heads, dim = query.shape
    block = math.gcd(length, 256)
    query_grads = []
    key_grad = jnp.zeros((length, heads, dim), F32)
    value_grad = jnp.zeros((length, heads, dim), F32)
    for first in range(0, length, block):
        last = first + block
        q, g = query[first:last], context_grad[first:last]
        scores = jnp.einsum("qhd,khd->hqk", q, key[:last], preferred_element_type=F32) * scale
        allowed = jnp.arange(last)[None, :] <= (first + jnp.arange(block))[:, None]
        probs = jnp.where(allowed, jnp.exp(scores - lse[:, first:last, None]), 0.0)
        value_grad = value_grad.at[:last].add(
            jnp.einsum("hqk,qhd->khd", probs.astype(BF16), g, preferred_element_type=F32)
        )
        prob_grad = jnp.einsum("qhd,khd->hqk", g, value[:last], preferred_element_type=F32)
        score_grad = (probs * (prob_grad - delta[:, first:last, None])).astype(BF16)
        query_grads.append(
            jnp.einsum("hqk,khd->qhd", score_grad, key[:last], preferred_element_type=F32) * scale
        )
        key_grad = key_grad.at[:last].add(
            jnp.einsum("hqk,qhd->khd", score_grad, q, preferred_element_type=F32) * scale
        )
    return jnp.concatenate(query_grads, axis=0), key_grad, value_grad


def body(
    tokens,
    norm_gain,
    norm_bias,
    qkv_weight,
    qkv_bias,
    out_weight,
    out_bias,
    fc1_weight,
    fc1_bias,
    fc2_weight,
    fc2_bias,
    cotangent,
):
    f_size, c_size = lax.axis_size("fsdp"), lax.axis_size("ctx")
    ratio = c_size // f_size
    devices = f_size * c_size
    own_seqs, tok_count, width = tokens.shape
    own_rows = own_seqs * tok_count
    length = tok_count * c_size
    rows = own_seqs * length
    head_dim = HEAD_DIM
    scale = head_dim ** (-0.5)
    row_block = qkv_weight.shape[0]
    cols = qkv_weight.shape[2] // ratio
    hidden_cols = fc1_weight.shape[1] // ratio
    heads = cols // head_dim
    c_index = lax.axis_index("ctx")

    vec = norm_gain.shape[0]
    vec1 = fc1_bias.shape[0]
    me = lax.axis_index("fsdp") * c_size + c_index
    per = max(128 // vec, 1)
    lane_piece = jnp.arange(128) // vec == me % per

    def placed(vector):
        return jnp.where(lane_piece, jnp.tile(vector.reshape(-1, vec), (1, per)), 0).astype(BF16)

    def lanes(array):
        array = array.reshape(-1, min(array.shape[-1], 128))
        return jnp.pad(array, ((0, 0), (0, 128 - array.shape[1])))

    small = jnp.concatenate(
        [placed(v) for v in (norm_gain, norm_bias, out_bias, fc2_bias, qkv_bias)]
        + [lanes(fc1_bias)]
    )
    small = jnp.pad(small, ((0, -small.shape[0] % 16), (0, 0)))

    qkv_src = (
        jnp.transpose(qkv_weight.reshape(row_block, 3, ratio, cols), (2, 0, 1, 3))
        .reshape(ratio, row_block, 3 * cols)
    )
    fc1_src = jnp.transpose(fc1_weight.reshape(row_block, ratio, hidden_cols), (1, 0, 2))
    out_src = jnp.transpose(out_weight.reshape(ratio, cols, row_block), (0, 2, 1))
    fc2_src = jnp.transpose(fc2_weight.reshape(ratio, hidden_cols, row_block), (0, 2, 1))

    fused = cols % 128 == 0 and row_block % 128 == 0 and own_seqs == 1
    tables = lane_tables(length) if fused else None
    gathered = gather_call(
        f_size,
        c_size,
        [tokens.reshape(own_rows, width), cotangent.reshape(own_rows, width)],
        small,
        [qkv_src, fc1_src, fc2_src, out_src],
        tables,
        0,
    )
    first_all, cot_all, small_all, qkv_all, fc1_all, fc2_all, out_all = gathered[:7]

    def rows_of(gathered):
        return jnp.swapaxes(gathered.reshape(c_size, own_seqs, tok_count, width), 0, 1).reshape(
            rows, width
        )

    def blocks_of(array):
        return jnp.swapaxes(array.reshape(own_seqs, c_size, tok_count, width), 0, 1).reshape(
            c_size, own_rows, width
        )

    grad_rows = rows_of(cot_all)
    qkv_w = qkv_all.reshape(width, 3 * cols)
    fc1_w = fc1_all.reshape(width, hidden_cols)
    out_t = out_all.reshape(width, cols)
    fc2_t = fc2_all.reshape(width, hidden_cols)

    vectors = small_all.reshape(devices, -1, 128)
    joined = jnp.sum(vectors[:, :7].astype(F32).reshape(devices // per, per, 7, 128), axis=1)
    joined = jnp.swapaxes(joined, 0, 1).reshape(7, width)
    gain_full, shift_full, out_bias_full, fc2_bias_full = (joined[i] for i in range(4))
    lane = min(vec1, 128)
    fc1_bias_full = vectors[:, 7 : 7 + vec1 // lane, :lane].reshape(-1)
    fc1_b = lax.dynamic_slice_in_dim(fc1_bias_full, c_index * hidden_cols, hidden_cols, 0).astype(
        F32
    )

    def heads_of(array):
        return array.reshape(own_seqs, length, heads, head_dim)

    if fused:
        hidden_in = rows_of(first_all)
        context_rows = gathered[10]
    else:
        cosine, sine = rope_tables(length, ROT_DIM)
        qkv_b = lax.dynamic_slice_in_dim(joined[4:7], c_index * cols, cols, 1).reshape(-1)
        normed, _ = normed_of(rows_of(first_all).astype(F32))
        hidden_in = (normed * gain_full + shift_full).astype(BF16)
        mixed = jnp.dot(hidden_in, qkv_w, preferred_element_type=F32) + qkv_b
        query, key = (
            rotate_pairs(heads_of(part), cosine, sine, ROT_DIM, 1.0).astype(BF16)
            for part in (mixed[:, :cols], mixed[:, cols : 2 * cols])
        )
        value = heads_of(mixed[:, 2 * cols :].astype(BF16))
        forward = [attention_forward(query[s], key[s], value[s], scale) for s in range(own_seqs)]
        context_b = jnp.stack([pair[0] for pair in forward]).astype(BF16)
        lse = jnp.stack([pair[1] for pair in forward])
        context_rows = context_b.reshape(rows, cols)
    pre = jnp.dot(hidden_in, fc1_w, preferred_element_type=F32) + fc1_b
    act, slope = gelu_both(pre)
    act_b = act.astype(BF16)
    contract_last = (((1,), (1,)), ((), ()))
    partial_out = lax.dot_general(
        context_rows, out_t, contract_last, preferred_element_type=F32
    ) + lax.dot_general(act_b, fc2_t, contract_last, preferred_element_type=F32)

    pre_grad = jnp.dot(grad_rows, fc2_t, preferred_element_type=F32) * slope
    pre_grad_b = pre_grad.astype(BF16)
    contract_first = (((0,), (0,)), ((), ()))

    def weight_grad(left, right):
        product = lax.dot_general(left, right, contract_first, preferred_element_type=F32)
        return product.astype(BF16).reshape(ratio, f_size, row_block, right.shape[1])

    fc2_grad = weight_grad(grad_rows, act_b)
    fc1_grad = weight_grad(hidden_in, pre_grad_b)
    out_grad = weight_grad(grad_rows, context_rows)
    fc1_b_grad = jnp.sum(pre_grad, axis=0)
    mlp_back = lax.dot_general(pre_grad_b, fc1_w, contract_last, preferred_element_type=F32)
    context_grad = jnp.dot(grad_rows, out_t, preferred_element_type=F32).astype(BF16)
    out_blocks = blocks_of(partial_out.astype(BF16))
    if fused:
        (branch, normed_grad), (fc2_shard, fc1_shard, out_shard, qkv_shard), (sums_qkv,) = (
            reduce_call(
                f_size,
                c_size,
                [out_blocks],
                [fc2_grad, fc1_grad, out_grad],
                2,
                (
                    [*gathered[7:11], context_grad, gathered[11]],
                    tables,
                    qkv_w,
                    hidden_in,
                    blocks_of(mlp_back),
                ),
            )
        )
        qkv_b_grad = sums_qkv.reshape(3, cols)
    else:
        context_grad = heads_of(context_grad)
        delta = jnp.swapaxes(
            jnp.sum(context_grad.astype(F32) * context_b.astype(F32), axis=-1), 1, 2
        )
        grads = [
            attention_backward(
                query[s], key[s], value[s], context_grad[s], delta[s], lse[s], scale
            )
            for s in range(own_seqs)
        ]
        query_grad, key_grad, value_grad = [jnp.stack(parts) for parts in zip(*grads)]
        mixed_grad = jnp.concatenate(
            [
                rotate_pairs(query_grad, cosine, sine, ROT_DIM, -1.0).reshape(rows, cols),
                rotate_pairs(key_grad, cosine, sine, ROT_DIM, -1.0).reshape(rows, cols),
                value_grad.reshape(rows, cols),
            ],
            axis=1,
        )
        mixed_grad_b = mixed_grad.astype(BF16)
        qkv_b_grad = jnp.sum(mixed_grad, axis=0).reshape(3, cols)
        qkv_grad = weight_grad(hidden_in, mixed_grad_b)
        normed_part = (
            lax.dot_general(mixed_grad_b, qkv_w, contract_last, preferred_element_type=F32) + mlp_back
        )
        (branch, normed_grad), (fc2_shard, fc1_shard, out_shard, qkv_shard) = reduce_all(
            f_size,
            c_size,
            [out_blocks, blocks_of(normed_part.astype(BF16))],
            [fc2_grad, fc1_grad, out_grad, qkv_grad],
        )

    x_own = tokens.reshape(own_rows, width).astype(F32)
    cot_own = cotangent.reshape(own_rows, width).astype(F32)
    output = (x_own + branch + out_bias_full + fc2_bias_full).astype(BF16)
    normed_own, inv_std_own = normed_of(x_own)
    hat_grad = normed_grad * gain_full
    back_rows = inv_std_own * (
        hat_grad
        - jnp.mean(hat_grad, axis=-1, keepdims=True)
        - normed_own * jnp.mean(hat_grad * normed_own, axis=-1, keepdims=True)
    )
    input_grad = (back_rows + cot_own).astype(BF16)

    def whole(block, full, axis):
        return lax.dynamic_update_slice_in_dim(
            jnp.zeros(full, F32), block, c_index * block.shape[axis], axis
        )

    grad_gain = jnp.sum(normed_grad * normed_own, axis=0).reshape(devices, vec)
    grad_shift = jnp.sum(normed_grad, axis=0).reshape(devices, vec)
    grad_cot = jnp.sum(cot_own, axis=0).reshape(devices, vec)
    q_parts = jnp.swapaxes(whole(qkv_b_grad, (3, width), 1).reshape(3, devices, vec), 0, 1)
    f_parts = whole(fc1_b_grad, (vec1 * devices,), 0).reshape(devices, vec1)
    tiles = jnp.concatenate(
        [grad_gain, grad_shift, grad_cot, q_parts.reshape(devices, 3 * vec), f_parts], axis=1
    )
    used = tiles.shape[1]
    tiles = jnp.pad(tiles, ((0, 0), (0, -used % 1024))).reshape(devices, -1, 128)
    sums = small_call(f_size, c_size, tiles, 4).reshape(-1)

    qkv_out = jnp.transpose(
        qkv_shard.reshape(ratio, row_block, 3, cols), (1, 2, 0, 3)
    ).reshape(row_block, 3, ratio * cols)
    fc1_out = jnp.swapaxes(fc1_shard, 0, 1).reshape(row_block, ratio * hidden_cols)
    out_out = jnp.swapaxes(out_shard, 1, 2).reshape(ratio * cols, row_block)
    fc2_out = jnp.swapaxes(fc2_shard, 1, 2).reshape(ratio * hidden_cols, row_block)
    return (
        output.reshape(own_seqs, tok_count, width),
        input_grad.reshape(own_seqs, tok_count, width),
        sums[:vec],
        sums[vec : 2 * vec],
        qkv_out.astype(F32),
        sums[3 * vec : 6 * vec].reshape(3, vec),
        out_out.astype(F32),
        sums[2 * vec : 3 * vec],
        fc1_out.astype(F32),
        sums[6 * vec : 6 * vec + vec1],
        fc2_out.astype(F32),
        sums[2 * vec : 3 * vec],
    )


def solution(mesh):
    row = P("fsdp", "ctx", None)
    vector = P(("fsdp", "ctx"))
    return jax.shard_map(
        body,
        mesh=mesh,
        in_specs=(
            row,
            vector,
            vector,
            P("ctx", None, "fsdp"),
            P(None, ("fsdp", "ctx")),
            P("fsdp", "ctx"),
            vector,
            P("ctx", "fsdp"),
            vector,
            P("fsdp", "ctx"),
            vector,
            row,
        ),
        out_specs=(
            row,
            row,
            vector,
            vector,
            P("ctx", None, "fsdp"),
            P(None, ("fsdp", "ctx")),
            P("fsdp", "ctx"),
            vector,
            P("ctx", "fsdp"),
            vector,
            P("fsdp", "ctx"),
            vector,
        ),
        check_vma=False,
    )
```

```python
import functools
import math

import jax
import jax.numpy as jnp
import numpy as np
from jax import lax
from jax.experimental import pallas as pl
from jax.experimental.pallas import tpu as pltpu
from jax.sharding import PartitionSpec as P

HEAD_DIM = 64
ROT_DIM = 32
NORM_EPS = 1e-05
GELU_COEF = math.sqrt(2.0 / math.pi)
MASKED = -1e30
LOW = 2
F32 = jnp.float32
BF16 = jnp.bfloat16
ANY = pl.BlockSpec(memory_space=pl.ANY)
VMEM = pl.BlockSpec(memory_space=pltpu.VMEM)


class Axis:
    def __init__(self, name, size):
        self.name = name
        self.size = size
        self.low = LOW
        self.high = size // LOW
        self.me = lax.axis_index(name)
        self.hi = lax.div(self.me, LOW)
        self.lo = lax.rem(self.me, LOW)
        self.partner = self.hi * LOW + (1 - self.lo)

    def at(self, hi, lo):
        return hi * LOW + lo

    def ahead(self, steps):
        return self.at(lax.rem(self.hi + steps, self.high), self.lo)

    def behind(self, steps):
        return self.at(lax.rem(self.hi + self.high - steps, self.high), self.lo)

    def behind_other(self, steps):
        return self.at(lax.rem(self.hi + self.high - steps, self.high), 1 - self.lo)


def remote(src, dst, send_sem, recv_sem, axis, index):
    return pltpu.make_async_remote_copy(
        src_ref=src,
        dst_ref=dst,
        send_sem=send_sem,
        recv_sem=recv_sem,
        device_id={axis.name: index},
        device_id_type=pl.DeviceIdType.MESH,
    )


def arrived(dst, sem):
    pltpu.make_async_copy(dst, dst, sem).wait()


class Spread:
    def __init__(self, axis, slot, source, send_hi, recv_hi, send_lo, recv_lo):
        self.axis, self.slot, self.source = axis, slot, source
        self.send_hi, self.recv_hi, self.send_lo, self.recv_lo = send_hi, recv_hi, send_lo, recv_lo

    def copy_hi(self, step):
        ax = self.axis
        return remote(
            self.source,
            self.slot(ax.me),
            self.send_hi.at[step - 1],
            self.recv_hi.at[step - 1],
            ax,
            ax.ahead(step),
        )

    def copy_lo(self, step):
        ax = self.axis
        held = ax.behind(step)
        src = self.source if step == 0 else self.slot(held)
        return remote(
            src, self.slot(held), self.send_lo.at[step], self.recv_lo.at[step], ax, ax.partner
        )

    def start(self):
        for step in range(1, self.axis.high):
            self.copy_hi(step).start()
        self.copy_lo(0).start()

    def forward(self, step):
        arrived(self.slot(self.axis.behind(step)), self.recv_hi.at[step - 1])
        self.copy_lo(step).start()

    def finish(self):
        for step in range(self.axis.high):
            arrived(self.slot(self.axis.behind_other(step)), self.recv_lo.at[step])
        for step in range(1, self.axis.high):
            self.copy_hi(step).wait_send()
        for step in range(self.axis.high):
            self.copy_lo(step).wait_send()


def spread_sems(axis_size):
    high = axis_size // LOW
    return [
        pltpu.SemaphoreType.DMA((max(high - 1, 1),)),
        pltpu.SemaphoreType.DMA((max(high - 1, 1),)),
        pltpu.SemaphoreType.DMA((high,)),
        pltpu.SemaphoreType.DMA((high,)),
    ]


class Line:
    def __init__(self, axis, slot, source, *sems):
        self.axis, self.slot, self.source = axis, slot, source
        self.send_up, self.recv_up, self.send_down, self.recv_down, self.send_lo, self.recv_lo = (
            sems
        )

    def copy(self, hi, sends, recvs, target):
        ax = self.axis
        block = ax.at(hi, ax.lo)
        src = self.source if hi is ax.hi else self.slot(block)
        return remote(src, self.slot(block), sends.at[hi], recvs.at[hi], ax, target)

    def up(self, hi):
        return self.copy(hi, self.send_up, self.recv_up, self.axis.me + LOW)

    def down(self, hi):
        return self.copy(hi, self.send_down, self.recv_down, self.axis.me - LOW)

    def across(self, hi):
        return self.copy(hi, self.send_lo, self.recv_lo, self.axis.partner)

    def start(self):
        ax = self.axis

        @pl.when(ax.hi < ax.high - 1)
        def _():
            self.up(ax.hi).start()

        @pl.when(ax.hi > 0)
        def _():
            self.down(ax.hi).start()

        self.across(ax.hi).start()

    def forward(self, step):
        ax = self.axis

        @pl.when(ax.hi >= step)
        def _():
            held = ax.hi - step
            arrived(self.slot(ax.at(held, ax.lo)), self.recv_up.at[held])

            @pl.when(ax.hi < ax.high - 1)
            def _():
                self.up(held).start()

            self.across(held).start()

        @pl.when(ax.hi + step < ax.high)
        def _():
            held = ax.hi + step
            arrived(self.slot(ax.at(held, ax.lo)), self.recv_down.at[held])

            @pl.when(ax.hi > 0)
            def _():
                self.down(held).start()

            self.across(held).start()

    def finish(self):
        ax = self.axis
        for hi in range(ax.high):
            arrived(self.slot(ax.at(hi, 1 - ax.lo)), self.recv_lo.at[hi])
        for step in range(ax.high):

            @pl.when(jnp.logical_and(ax.hi >= step, ax.hi < ax.high - 1))
            def _(step=step):
                self.up(ax.hi if step == 0 else ax.hi - step).wait_send()

            @pl.when(jnp.logical_and(ax.hi + step < ax.high, ax.hi > 0))
            def _(step=step):
                self.down(ax.hi if step == 0 else ax.hi + step).wait_send()

            @pl.when(ax.hi >= step)
            def _(step=step):
                self.across(ax.hi if step == 0 else ax.hi - step).wait_send()

            if step > 0:

                @pl.when(ax.hi + step < ax.high)
                def _(step=step):
                    self.across(ax.hi + step).wait_send()


def line_sems(axis_size):
    return [pltpu.SemaphoreType.DMA((axis_size // LOW,))] * 6


def meet_everyone(fs, cx):
    barrier = pltpu.get_barrier_semaphore()
    total = fs.size * cx.size
    me = fs.me * cx.size + cx.me

    def signal(step, carry):
        other = lax.rem(me + step, total)
        pl.semaphore_signal(
            barrier,
            inc=1,
            device_id={fs.name: lax.div(other, cx.size), cx.name: lax.rem(other, cx.size)},
            device_id_type=pl.DeviceIdType.MESH,
        )
        return carry

    lax.fori_loop(1, total, signal, 0)
    pl.semaphore_wait(barrier, total - 1)


def shift_of(f_index, f_size):
    return lax.rem(f_index, LOW) * (f_size // LOW) + lax.div(f_index, LOW)


def unshift(shift, f_size):
    return lax.rem(shift, f_size // LOW) * LOW + lax.div(shift, f_size // LOW)


def low_slot(fs, column, device):
    return lax.rem(device + fs.size - shift_of(column, fs.size), fs.size)


def gather_kernel(n_act, n_w, fused, f_size, c_size, *refs):
    fs, cx = Axis("fsdp", f_size), Axis("ctx", c_size)
    ratio = c_size // f_size
    total = f_size * c_size
    me = fs.me * c_size + cx.me
    n_extra = 2 if fused else 0
    n_in = n_act + 1 + n_w + n_extra
    ins, refs = refs[:n_in], refs[n_in:]
    acts, small_own, w_srcs = ins[:n_act], ins[n_act], ins[n_act + 1 : n_act + 1 + n_w]
    n_out = n_act + 1 + n_w + (5 if fused else 0)
    outs, rest = refs[:n_out], list(refs[n_out:])
    act_outs, small_out, w_outs = outs[:n_act], outs[n_act], outs[n_act + 1 : n_act + 1 + n_w]
    if fused:
        tables = ins[n_act + 1 + n_w :]
        query, key, value, context, lse = outs[n_act + 1 + n_w :]
    small_send, small_recv = rest[:2]
    rest = rest[2:]
    own_sem = rest.pop(0)
    lines = []
    for index in range(n_act):
        out = act_outs[index]
        slot = lambda c, out=out: out.at[c]
        source = slot(cx.me) if fused and index == 0 else acts[index]
        lines.append(Line(cx, slot, source, *rest[:6]))
        rest = rest[6:]
    mids, rest = rest[:n_w], rest[n_w:]
    mid_send, mid_recv, w_send, w_recv = rest[:4]
    rest = rest[4:]
    column = lax.div(cx.me, ratio)
    spreads = []
    for index in range(n_w):
        out = w_outs[index]
        slot = lambda f, out=out: out.at[:, low_slot(fs, column, f)]
        spreads.append(Spread(fs, slot, slot(fs.me), *rest[:4]))
        rest = rest[4:]
    pass_to = lax.rem(cx.me + shift_of(fs.me, f_size), f_size)
    pass_from = unshift(lax.rem(fs.me + f_size - lax.rem(cx.me, f_size), f_size), f_size)
    stays = pass_to == fs.me
    row_hi, row_lo = lax.div(cx.me, f_size), lax.rem(cx.me, f_size)

    def move(index):
        src, dst = w_srcs[index], mids[index]
        away = lambda: remote(src, dst, mid_send.at[index], mid_recv.at[index], fs, pass_to)
        here = lambda: pltpu.make_async_copy(src, dst, mid_recv.at[index])
        return away, here

    def scatter(index, i):
        to_c = pass_from * ratio + i
        src, dst = mids[index].at[i], w_outs[index].at[row_hi, row_lo]
        sem = w_recv.at[index, row_hi]
        away = lambda: remote(src, dst, w_send.at[index, i], sem, cx, to_c)
        here = lambda: pltpu.make_async_copy(src, dst, sem)
        return to_c == cx.me, away, here

    def either(is_self, away, here):
        @pl.when(is_self)
        def _():
            here().start()

        @pl.when(jnp.logical_not(is_self))
        def _():
            away().start()

    def start_moves():
        for index in range(n_w):
            either(stays, *move(index))

    def start_scatter(index):
        arrived(mids[index], mid_recv.at[index])
        for i in range(ratio):
            either(*scatter(index, i))

    def start_spread(index):
        for hi in range(ratio):
            arrived(w_outs[index].at[hi, low_slot(fs, column, fs.me)], w_recv.at[index, hi])
        spreads[index].start()

    def forward_spread(index):
        for step in range(1, fs.high):
            spreads[index].forward(step)

    def small_copy(step):
        other = lax.rem(me + step, total)
        return pltpu.make_async_remote_copy(
            src_ref=small_own,
            dst_ref=small_out.at[me],
            send_sem=small_send.at[step - 1],
            recv_sem=small_recv.at[me],
            device_id={fs.name: lax.div(other, c_size), cx.name: lax.rem(other, c_size)},
            device_id_type=pl.DeviceIdType.MESH,
        )

    def small_start(step, carry):
        small_copy(step).start()
        return carry

    def small_wait(step, carry):
        other = lax.rem(me + step, total)
        arrived(small_out.at[other], small_recv.at[other])
        return carry

    def small_drain(step, carry):
        small_copy(step).wait_send()
        return carry

    def vector(row, first, chunks, per):
        parts = []
        for chunk in range(chunks):
            part = small_out[first + chunk * per, row : row + 1, :].astype(F32)
            for more in range(1, per):
                part = part + small_out[first + chunk * per + more, row : row + 1, :].astype(F32)
            parts.append(part)
        return jnp.concatenate(parts, axis=1)

    def normalise():
        width = acts[0].shape[1]
        chunks = width // 128
        gain = vector(0, 0, chunks, total // chunks)
        shift = vector(1, 0, chunks, total // chunks)

        def step(i, carry):
            rows = pl.ds(pl.multiple_of(i * 32, 32), 32)
            x = acts[0][rows, :].astype(F32)
            centred = x - jnp.mean(x, axis=-1, keepdims=True)
            inv_std = lax.rsqrt(jnp.mean(centred * centred, axis=-1, keepdims=True) + NORM_EPS)
            act_outs[0][cx.me, rows, :] = (centred * inv_std * gain + shift).astype(BF16)
            return carry

        lax.fori_loop(0, acts[0].shape[0] // 32, step, 0)

    def project():
        rows, width = acts[0].shape
        cols = query.shape[1]
        per = total * cols // width
        first = cx.me * per
        bias = [vector(4 + part, first, cols // 128, per * 128 // cols) for part in range(3)]

        def step(i, carry):
            x = act_outs[0][pl.ds(2 * i, 2)].reshape(2 * rows, width)
            span = pl.ds(pl.multiple_of(i * 2 * rows, 2 * rows), 2 * rows)
            straight, swing = [table[span, :] for table in tables]
            for part, out in enumerate((query, key, value)):
                w = w_outs[0][:, :, :, part * cols : (part + 1) * cols].reshape(width, cols)
                y = jnp.dot(x, w, preferred_element_type=F32) + bias[part]
                for lane in range(0, cols, 128):
                    half = y[:, lane : lane + 128]
                    if part < 2:
                        half = turn(half, straight, swing, 1.0)
                    out[span, lane : lane + 128] = half.astype(BF16)
            return carry

        lax.fori_loop(0, c_size // 2, step, 0)

    def attend(head):
        length = query.shape[0]
        block = math.gcd(length, 256)
        lanes = slice(head * HEAD_DIM, (head + 1) * HEAD_DIM)
        last_two = (((1,), (1,)), ((), ()))
        for first in range(0, length, block):
            last = first + block
            scores = (
                lax.dot_general(
                    query[first:last, lanes],
                    key[:last, lanes],
                    last_two,
                    preferred_element_type=F32,
                )
                * HEAD_DIM ** (-0.5)
            )
            row = lax.broadcasted_iota(jnp.int32, (block, last), 0) + first
            col = lax.broadcasted_iota(jnp.int32, (block, last), 1)
            scores = jnp.where(col <= row, scores, MASKED)
            top = jnp.max(scores, axis=-1, keepdims=True)
            weights = jnp.exp(scores - top)
            summed = jnp.sum(weights, axis=-1, keepdims=True)
            mixed = jnp.dot(weights.astype(BF16), value[:last, lanes], preferred_element_type=F32)
            context[first:last, lanes] = (mixed / summed).astype(BF16)
            lse[first:last, head : head + 1] = top + jnp.log(summed)

    meet_everyone(fs, cx)
    lax.fori_loop(1, total, small_start, 0)
    start_moves()
    own = {}
    small_own_copy = pltpu.make_async_copy(small_own, small_out.at[me], own_sem.at[n_act])
    small_own_copy.start()
    for index in range(n_act):
        if not (fused and index == 0):
            own[index] = pltpu.make_async_copy(
                acts[index], lines[index].slot(cx.me), own_sem.at[index]
            )
            own[index].start()
            lines[index].start()
    small_own_copy.wait()
    lax.fori_loop(1, total, small_wait, 0)
    if fused:
        normalise()
        lines[0].start()

    scatters = [functools.partial(start_scatter, index) for index in range(n_w)]
    starts = [functools.partial(start_spread, index) for index in range(n_w)]
    lasts = [functools.partial(forward_spread, index) for index in range(n_w)]
    rows = [
        [functools.partial(lines[index].forward, step) for step in range(1, cx.high)]
        for index in range(n_act)
    ]
    comm = [scatters.pop(0)] + [more[0] for more in rows[1:]] + [scatters.pop(0), rows[0][0]]
    comm += scatters
    comm += rows[0][1:2] + [starts[0]] + [more[1] for more in rows[1:] if len(more) > 1]
    comm += [starts[1], lasts[0]] + rows[0][2:]
    for work in comm:
        work()
    comm = []
    for index in range(2, n_w):
        comm += [starts[index], lasts[index - 1]]
    comm = comm[:2] + [work for more in rows[1:] for work in more[2:]] + comm[2:] + [lasts[-1]]
    while len(comm) > 4:
        comm.pop(0)()
    lines[0].finish()
    spreads[0].finish()
    if fused:
        compute = [project]
        compute += [functools.partial(attend, head) for head in range(lse.shape[1])]
        for work in compute:
            if comm:
                comm.pop(0)()
            if comm and work is project:
                comm.pop(0)()
            work()
    for work in comm:
        work()
    for index in own:
        own[index].wait()
    for index in range(1, n_act):
        lines[index].finish()
    for index in range(n_w):
        if index > 0:
            spreads[index].finish()

        @pl.when(jnp.logical_not(stays))
        def _(index=index):
            move(index)[0]().wait_send()

        for i in range(ratio):
            is_self, away, here = scatter(index, i)

            @pl.when(jnp.logical_not(is_self))
            def _(away=away):
                away().wait_send()

    lax.fori_loop(1, total, small_drain, 0)


def gather_call(f_size, c_size, acts, small, w_srcs, tables, collective_id):
    ratio = c_size // f_size
    total = f_size * c_size
    fused = tables is not None
    ins = [*acts, small, *w_srcs] + (list(tables) if fused else [])
    shapes = [jax.ShapeDtypeStruct((c_size, *a.shape), a.dtype) for a in acts]
    shapes.append(jax.ShapeDtypeStruct((total, *small.shape), small.dtype))
    for w in w_srcs:
        shapes.append(jax.ShapeDtypeStruct((ratio, f_size, *w.shape[1:]), w.dtype))
    specs = [ANY] * len(shapes)
    specs[len(acts)] = VMEM
    if fused:
        specs[0] = specs[len(acts) + 1] = VMEM
        length, cols = c_size * acts[0].shape[0], w_srcs[0].shape[2] // 3
        shapes += [jax.ShapeDtypeStruct((length, cols), BF16)] * 4
        shapes.append(jax.ShapeDtypeStruct((length, cols // HEAD_DIM), F32))
        specs += [VMEM] * 5
    scratch = [pltpu.SemaphoreType.DMA((total - 1,)), pltpu.SemaphoreType.DMA((total,))]
    scratch.append(pltpu.SemaphoreType.DMA((len(acts) + 1,)))
    for _ in acts:
        scratch += line_sems(c_size)
    scratch += [pltpu.VMEM(w.shape, w.dtype) for w in w_srcs]
    scratch += [pltpu.SemaphoreType.DMA((len(w_srcs),))] * 2
    scratch += [pltpu.SemaphoreType.DMA((len(w_srcs), ratio))] * 2
    for _ in w_srcs:
        scratch += spread_sems(f_size)
    return pl.pallas_call(
        functools.partial(gather_kernel, len(acts), len(w_srcs), fused, f_size, c_size),
        out_shape=tuple(shapes),
        in_specs=[VMEM] * len(ins),
        out_specs=tuple(specs),
        scratch_shapes=scratch,
        compiler_params=pltpu.CompilerParams(collective_id=collective_id, has_side_effects=True),
        name=f"gather_{collective_id}",
    )(*ins)


def add_into(dst, terms):
    rows = dst.shape[-2]
    lead = dst.shape[:-2]
    chunk = math.gcd(rows, 32)

    def at(ref, index, start):
        return (*index, pl.ds(start, chunk), slice(None))

    for index in [()] if not lead else [(i,) for i in range(lead[0])]:

        def step(i, carry, index=index):
            start = pl.multiple_of(i * chunk, chunk)
            total = terms[0][at(terms[0], index, start)].astype(F32)
            for term in terms[1:]:
                total = total + term[at(term, index, start)].astype(F32)
            dst[at(dst, index, start)] = total.astype(dst.dtype)
            return carry

        lax.fori_loop(0, rows // chunk, step, 0)


class Fold:
    def __init__(self, axis, block, from_lo, from_hi, *sems):
        self.axis, self.block, self.result = axis, block, from_lo.at[0]
        self.from_lo, self.from_hi = from_lo, from_hi
        self.send_lo, self.recv_lo, self.send_hi, self.recv_hi = sems

    def copy_lo(self, step):
        ax = self.axis
        hi = lax.rem(ax.hi + step, ax.high)
        return remote(
            self.block(ax.at(hi, 1 - ax.lo)),
            self.from_lo.at[step],
            self.send_lo.at[step],
            self.recv_lo.at[step],
            ax,
            ax.partner,
        )

    def copy_hi(self, step):
        ax = self.axis
        return remote(
            self.from_lo.at[step],
            self.from_hi.at[step - 1],
            self.send_hi.at[step - 1],
            self.recv_hi.at[step - 1],
            ax,
            ax.ahead(step),
        )

    def start(self):
        for step in list(range(1, self.axis.high)) + [0]:
            self.copy_lo(step).start()

    def forward(self, step):
        arrived(self.from_lo.at[step], self.recv_lo.at[step])
        add_into(
            self.from_lo.at[step], [self.block(self.axis.ahead(step)), self.from_lo.at[step]]
        )
        self.copy_hi(step).start()

    def finish(self):
        arrived(self.from_lo.at[0], self.recv_lo.at[0])
        terms = [self.block(self.axis.me), self.from_lo.at[0]]
        for step in range(1, self.axis.high):
            arrived(self.from_hi.at[step - 1], self.recv_hi.at[step - 1])
            terms.append(self.from_hi.at[step - 1])
        add_into(self.result, terms)

    def drain(self):
        for step in range(self.axis.high):
            self.copy_lo(step).wait_send()
        for step in range(1, self.axis.high):
            self.copy_hi(step).wait_send()


class LineFold:
    def __init__(self, axis, block, own, result, from_lo, from_z, from_end, *sems):
        self.axis, self.block, self.own, self.result = axis, block, own, result
        self.from_lo, self.from_z, self.from_end = from_lo, from_z, from_end
        self.send_lo, self.recv_lo, self.send_z, self.recv_z, self.recv_end = sems
        low_end, high_end = jnp.int32(0), jnp.int32(axis.high - 1)
        self.order = []
        for _ in range(axis.high):
            take_low = axis.hi - low_end >= high_end - axis.hi
            self.order.append(jnp.where(take_low, low_end, high_end))
            low_end = jnp.where(take_low, low_end + 1, low_end)
            high_end = jnp.where(take_low, high_end, high_end - 1)

    def across(self, hi):
        ax = self.axis
        return remote(
            self.block(ax.at(hi, 1 - ax.lo)),
            self.from_lo.at[hi],
            self.send_lo.at[hi],
            self.recv_lo.at[hi],
            ax,
            ax.partner,
        )

    def onward(self, hi, up, last):
        ax = self.axis
        side = 0 if up else 1
        dst, sem = (
            (self.from_end.at[side], self.recv_end.at[side])
            if last
            else (self.from_z.at[hi], self.recv_z.at[hi])
        )
        target = ax.me + LOW if up else ax.me - LOW
        return remote(self.from_lo.at[hi], dst, self.send_z.at[hi], sem, ax, target)

    def start(self):
        for hi in self.order:
            self.across(hi).start()

    def pass_on(self, hi, up):
        ax = self.axis
        first = ax.hi == (0 if up else ax.high - 1)
        own = self.own(hi)

        @pl.when(first)
        def _():
            add_into(self.from_lo.at[hi], [own, self.from_lo.at[hi]])

        @pl.when(jnp.logical_not(first))
        def _():
            arrived(self.from_z.at[hi], self.recv_z.at[hi])
            add_into(self.from_lo.at[hi], [own, self.from_lo.at[hi], self.from_z.at[hi]])

        near = ax.hi == (hi - 1 if up else hi + 1)

        @pl.when(near)
        def _():
            self.onward(hi, up, True).start()

        @pl.when(jnp.logical_not(near))
        def _():
            self.onward(hi, up, False).start()

    def forward(self, hi):
        ax = self.axis
        arrived(self.from_lo.at[hi], self.recv_lo.at[hi])

        @pl.when(ax.hi < hi)
        def _():
            self.pass_on(hi, True)

        @pl.when(ax.hi > hi)
        def _():
            self.pass_on(hi, False)

    def finish(self):
        ax = self.axis
        own = [self.own(ax.hi), self.from_lo.at[ax.hi]]
        if ax.high == 1:
            add_into(self.result, own)
            return
        low_end, high_end = ax.hi == 0, ax.hi == ax.high - 1

        @pl.when(jnp.logical_not(low_end))
        def _():
            arrived(self.from_end.at[0], self.recv_end.at[0])

        @pl.when(jnp.logical_not(high_end))
        def _():
            arrived(self.from_end.at[1], self.recv_end.at[1])

        @pl.when(low_end)
        def _():
            add_into(self.result, own + [self.from_end.at[1]])

        @pl.when(high_end)
        def _():
            add_into(self.result, own + [self.from_end.at[0]])

        @pl.when(jnp.logical_not(jnp.logical_or(low_end, high_end)))
        def _():
            add_into(self.result, own + [self.from_end.at[0], self.from_end.at[1]])

    def drain(self):
        ax = self.axis
        for hi in range(ax.high):
            self.across(hi).wait_send()

            @pl.when(ax.hi != hi)
            def _(hi=hi):
                self.onward(hi, True, False).wait_send()


def line_fold_scratch(axis_size, shape, dtype):
    high = axis_size // LOW
    return [
        pltpu.VMEM((high, *shape), dtype),
        pltpu.VMEM((high, *shape), dtype),
        pltpu.VMEM((2, *shape), dtype),
        pltpu.SemaphoreType.DMA((high,)),
        pltpu.SemaphoreType.DMA((high,)),
        pltpu.SemaphoreType.DMA((high,)),
        pltpu.SemaphoreType.DMA((high,)),
        pltpu.SemaphoreType.DMA((2,)),
    ]


def fold_scratch(axis_size, shape, dtype):
    high = axis_size // LOW
    more = max(high - 1, 1)
    return [
        pltpu.VMEM((high, *shape), dtype),
        pltpu.VMEM((more, *shape), dtype),
        pltpu.SemaphoreType.DMA((high,)),
        pltpu.SemaphoreType.DMA((high,)),
        pltpu.SemaphoreType.DMA((more,)),
        pltpu.SemaphoreType.DMA((more,)),
    ]


def reduce_kernel(n_part, n_w, fused, f_size, c_size, *refs):
    fs, cx = Axis("fsdp", f_size), Axis("ctx", c_size)
    ratio = c_size // f_size
    n_late = 1 if fused else 0
    parts, refs = refs[: n_part - n_late], refs[n_part - n_late :]
    grads, refs = refs[: n_w - n_late], refs[n_w - n_late :]
    if fused:
        heads_in, refs = refs[:6], refs[6:]
        straight, swing, qkv_w, hidden, mlp_back = refs[:5]
        refs = refs[5:]
    rows_outs, refs = refs[:n_part], refs[n_part:]
    grad_outs, scratch = refs[:n_w], list(refs[n_w:])
    if fused:
        sums = scratch.pop(0)
        late_part, late_grad, own_rows, own_sem = scratch[:4]
        dq, dk, dv, mixed_grad, tall, tall_sem, wide, wide_sem = scratch[4:12]
        scratch = scratch[12:]
        parts, grads = (*parts, late_part), (*grads, late_grad)
    row_folds = []
    for index in range(n_part):
        block = lambda c, part=parts[index]: part.at[c]
        own = lambda hi, block=block: block(cx.at(hi, cx.lo))
        if fused and index == 0:
            own = lambda hi: own_rows.at[hi]
        row_folds.append(LineFold(cx, block, own, rows_outs[index], *scratch[:8]))
        scratch = scratch[8:]
    column = lax.div(cx.me, ratio)
    folds, totals = [], []
    for index in range(n_w):
        block = lambda f, grad=grads[index]: grad.at[:, low_slot(fs, column, f)]
        totals.append(scratch[0].at[0])
        folds.append(Fold(fs, block, *scratch[:6]))
        scratch = scratch[6:]
    g_send, g_recv = scratch

    meet_everyone(fs, cx)
    for fold in row_folds[: n_part - n_late]:
        fold.start()
    for fold in folds[: n_w - n_late]:
        fold.start()
    own_copies = []
    if fused:
        for hi in range(cx.high):
            own_copies.append(
                pltpu.make_async_copy(
                    parts[0].at[cx.at(hi, cx.lo)], own_rows.at[hi], own_sem.at[hi]
                )
            )
            own_copies[-1].start()

    slot = lax.rem(cx.me, ratio)
    row_lo = low_slot(fs, column, fs.me)

    def deliver(index, hi):
        to_c = hi * f_size + row_lo
        is_self = jnp.logical_and(column == fs.me, to_c == cx.me)
        src = totals[index].at[hi]
        dst = grad_outs[index].at[slot]
        away = lambda: pltpu.make_async_remote_copy(
            src_ref=src,
            dst_ref=dst,
            send_sem=g_send.at[index, hi],
            recv_sem=g_recv.at[index, slot],
            device_id={fs.name: column, cx.name: to_c},
            device_id_type=pl.DeviceIdType.MESH,
        )
        here = lambda: pltpu.make_async_copy(src, dst, g_recv.at[index, slot])
        return is_self, away, here

    def deliver_all(index):
        folds[index].finish()
        for hi in range(ratio):
            is_self, away, here = deliver(index, hi)

            @pl.when(is_self)
            def _(here=here):
                here().start()

            @pl.when(jnp.logical_not(is_self))
            def _(away=away):
                away().start()

    def pass_halves(index):
        for step in range(1, fs.high):
            folds[index].forward(step)

    def row_work(fold):
        return [functools.partial(fold.forward, hi) for hi in fold.order]

    halves = [functools.partial(pass_halves, index) for index in range(n_w)]
    delivers = [functools.partial(deliver_all, index) for index in range(n_w)]

    def column_grads():
        wide_rows = late_grad.shape[2]

        def copy(i):
            at = pl.ds(pl.multiple_of(i * wide_rows, wide_rows), wide_rows)
            slot = lax.rem(i, 2)
            return pltpu.make_async_copy(hidden.at[:, at], tall.at[slot], tall_sem.at[slot])

        copy(0).start()

        def step(i, carry):
            @pl.when(i + 1 < c_size)
            def _():
                copy(i + 1).start()

            copy(i).wait()
            late_grad[lax.div(i, f_size), lax.rem(i, f_size)] = lax.dot_general(
                tall[lax.rem(i, 2)],
                mixed_grad[...],
                (((0,), (0,)), ((), ())),
                preferred_element_type=F32,
            ).astype(BF16)
            return carry

        lax.fori_loop(0, c_size, step, 0)

    def row_grads():
        rows = late_part.shape[1]

        def copy(i):
            slot = lax.rem(i, 2)
            return pltpu.make_async_copy(
                mlp_back.at[pl.ds(2 * i, 2)], wide.at[slot], wide_sem.at[slot]
            )

        copy(0).start()

        def step(i, carry):
            @pl.when(i + 1 < c_size // 2)
            def _():
                copy(i + 1).start()

            copy(i).wait()
            span = pl.ds(pl.multiple_of(2 * i * rows, 2 * rows), 2 * rows)
            total = lax.dot_general(
                mixed_grad[span, :],
                qkv_w[...],
                (((1,), (1,)), ((), ())),
                preferred_element_type=F32,
            )
            total = total.reshape(2, rows, total.shape[1]) + wide[lax.rem(i, 2)]
            late_part[pl.ds(2 * i, 2)] = total.astype(BF16)
            return carry

        lax.fori_loop(0, c_size // 2, step, 0)

    if fused:
        heads = dq.shape[1] // HEAD_DIM
        early = row_work(row_folds[0])
        comm = [early.pop(0), early.pop(0), delivers.pop(0)]
        for work in early:
            comm.append(work)
            if len(delivers) > 1:
                comm.append(delivers.pop(0))
        for work in halves[:-1]:
            work()
        for copy in own_copies:
            copy.wait()
        for head in range(heads):
            backward_head(head, *heads_in, dq, dk, dv)
            if comm:
                comm.pop(0)()
        backward_turn(straight, swing, dq, dk, dv, mixed_grad, sums)
        row_grads()
        row_folds[1].start()
        if comm:
            comm.pop(0)()
        column_grads()
        folds[-1].start()
        for work in comm:
            work()
        halves[-1]()
        for count, work in enumerate(row_work(row_folds[1])):
            work()
            if count >= 1 and delivers:
                delivers.pop(0)()
    else:
        for count, work in enumerate([work for fold in row_folds for work in row_work(fold)]):
            for more in halves[:2]:
                more()
            halves = halves[2:]
            work()
            if count >= 1 and delivers and not halves:
                delivers.pop(0)()
        for work in halves:
            work()
    for work in delivers:
        work()
    for fold in row_folds:
        fold.finish()
    for index in range(n_w):
        for i in range(ratio):
            arrived(grad_outs[index].at[i], g_recv.at[index, i])
    for fold in row_folds:
        fold.drain()
    for index in range(n_w):
        folds[index].drain()
        for hi in range(ratio):
            is_self, away, here = deliver(index, hi)

            @pl.when(jnp.logical_not(is_self))
            def _(away=away):
                away().wait_send()


def reduce_call(f_size, c_size, parts, grads, collective_id, late=None):
    ratio = c_size // f_size
    fused = late is not None
    ins, in_specs = [*parts, *grads], [VMEM] * (len(parts) + len(grads))
    part_shapes = [(part.shape, part.dtype) for part in parts]
    grad_shapes = [(grad.shape, grad.dtype) for grad in grads]
    own = []
    if fused:
        in_specs[0] = ANY
        heads_in, tables, qkv_w, hidden, mlp_back = late
        ins += [*heads_in, *tables, qkv_w, hidden, mlp_back]
        in_specs += [VMEM] * 9 + [ANY] * 2
        length, cols = heads_in[0].shape
        part_shapes.append(part_shapes[0])
        shape, dtype = grad_shapes[0]
        grad_shapes.append(((*shape[:3], 3 * cols), dtype))
        high = c_size // LOW
        own = [
            pltpu.VMEM(*part_shapes[1]),
            pltpu.VMEM(*grad_shapes[-1]),
            pltpu.VMEM((high, *parts[0].shape[1:]), BF16),
            pltpu.SemaphoreType.DMA((high,)),
            pltpu.VMEM((length, cols), F32),
            pltpu.VMEM((length, cols), F32),
            pltpu.VMEM((length, cols), F32),
            pltpu.VMEM((length, 3 * cols), BF16),
            pltpu.VMEM((2, length, shape[2]), BF16),
            pltpu.SemaphoreType.DMA((2,)),
            pltpu.VMEM((2, 2, *mlp_back.shape[1:]), F32),
            pltpu.SemaphoreType.DMA((2,)),
        ]
    shapes, scratch = [], []
    for shape, dtype in part_shapes:
        shapes.append(jax.ShapeDtypeStruct(shape[1:], F32))
        scratch += line_fold_scratch(c_size, shape[1:], dtype)
    for shape, dtype in grad_shapes:
        piece = (ratio, *shape[2:])
        shapes.append(jax.ShapeDtypeStruct(piece, dtype))
        scratch += fold_scratch(f_size, piece, dtype)
    specs = [VMEM] * len(part_shapes) + [ANY] * len(grad_shapes)
    if fused:
        shapes.append(jax.ShapeDtypeStruct((1, 3 * cols), F32))
        specs.append(VMEM)
    scratch += [pltpu.SemaphoreType.DMA((len(grad_shapes), ratio))] * 2
    outs = pl.pallas_call(
        functools.partial(
            reduce_kernel, len(part_shapes), len(grad_shapes), fused, f_size, c_size
        ),
        out_shape=tuple(shapes),
        in_specs=in_specs,
        out_specs=tuple(specs),
        scratch_shapes=own + scratch,
        compiler_params=pltpu.CompilerParams(
            collective_id=collective_id,
            has_side_effects=True,
            vmem_limit_bytes=66_000_000 if fused else None,
        ),
        name=f"reduce_{collective_id}",
    )(*ins)
    n_part, n_w = len(part_shapes), len(grad_shapes)
    return outs[:n_part], outs[n_part : n_part + n_w], outs[n_part + n_w :]


def reduce_all(f_size, c_size, parts, grads):
    size = sum(2.25 * part.size * part.dtype.itemsize for part in parts)
    size += sum(2.5 * grad.size * grad.dtype.itemsize for grad in grads)
    if size <= 56 * 2**20:
        return reduce_call(f_size, c_size, parts, grads, 2)[:2]
    half = len(grads) // 2
    (first,), early, _ = reduce_call(f_size, c_size, parts[:1], grads[:half], 2)
    (second,), late, _ = reduce_call(f_size, c_size, parts[1:], grads[half:], 3)
    return (first, second), (*early, *late)


def small_kernel(f_size, c_size, tiles, out, held, send_sem, recv_sem):
    fs, cx = Axis("fsdp", f_size), Axis("ctx", c_size)
    total = f_size * c_size
    me = fs.me * c_size + cx.me
    meet_everyone(fs, cx)

    def copy(step):
        other = lax.rem(me + step, total)
        return pltpu.make_async_remote_copy(
            src_ref=tiles.at[other],
            dst_ref=held.at[step - 1],
            send_sem=send_sem.at[step - 1],
            recv_sem=recv_sem.at[step - 1],
            device_id={fs.name: lax.div(other, c_size), cx.name: lax.rem(other, c_size)},
            device_id_type=pl.DeviceIdType.MESH,
        )

    def start(step, carry):
        copy(step).start()
        return carry

    lax.fori_loop(1, total, start, 0)

    def collect(step, acc):
        arrived(held.at[step - 1], recv_sem.at[step - 1])
        return acc + held[step - 1]

    out[...] = lax.fori_loop(1, total, collect, tiles[me])

    def drain(step, carry):
        copy(step).wait_send()
        return carry

    lax.fori_loop(1, total, drain, 0)


def small_call(f_size, c_size, tiles, collective_id):
    total = f_size * c_size
    return pl.pallas_call(
        functools.partial(small_kernel, f_size, c_size),
        out_shape=jax.ShapeDtypeStruct(tiles.shape[1:], F32),
        in_specs=[VMEM],
        out_specs=VMEM,
        scratch_shapes=[
            pltpu.VMEM((total - 1, *tiles.shape[1:]), F32),
            pltpu.SemaphoreType.DMA((total - 1,)),
            pltpu.SemaphoreType.DMA((total - 1,)),
        ],
        compiler_params=pltpu.CompilerParams(collective_id=collective_id, has_side_effects=True),
        name=f"small_{collective_id}",
    )(tiles)


def normed_of(rows):
    centred = rows - jnp.mean(rows, axis=-1, keepdims=True)
    inv_std = lax.rsqrt(jnp.mean(centred * centred, axis=-1, keepdims=True) + NORM_EPS)
    return centred * inv_std, inv_std


def gelu_both(values):
    tangent = jnp.tanh(GELU_COEF * (values + 0.044715 * values * values * values))
    act = 0.5 * values * (1.0 + tangent)
    slope = 0.5 * (1.0 + tangent) + 0.5 * values * (1.0 - tangent * tangent) * GELU_COEF * (
        1.0 + 3.0 * 0.044715 * values * values
    )
    return act, slope


def rope_tables(count, rot_dim):
    positions = jnp.arange(count, dtype=F32)
    half_dim = rot_dim // 2
    inverse = 10000.0 ** (-(jnp.arange(half_dim, dtype=F32) * 2.0) / rot_dim)
    angles = positions[:, None] * inverse[None, :]
    return (jnp.cos(angles)[:, None, :], jnp.sin(angles)[:, None, :])


def rotate_pairs(values, cosine, sine, rot_dim, sign):
    half_dim = rot_dim // 2
    first_half = values[..., :half_dim]
    second_half = values[..., half_dim:rot_dim]
    return jnp.concatenate(
        [
            first_half * cosine - sign * second_half * sine,
            second_half * cosine + sign * first_half * sine,
            values[..., rot_dim:],
        ],
        axis=-1,
    )


def lane_tables(count):
    half_dim = ROT_DIM // 2
    inverse = np.float32(10000.0) ** (-(np.arange(half_dim, dtype=np.float32) * 2.0) / ROT_DIM)
    angles = np.arange(count, dtype=np.float32)[:, None] * inverse.astype(np.float32)[None, :]
    cosine, sine = np.cos(angles.astype(np.float64)), np.sin(angles.astype(np.float64))
    rest = np.zeros((count, HEAD_DIM - ROT_DIM))
    straight = np.concatenate([cosine, cosine, rest + 1.0] * (128 // HEAD_DIM), axis=1)
    swing = np.concatenate([-sine, sine, rest] * (128 // HEAD_DIM), axis=1)
    return [jnp.asarray(table.astype(np.float32)) for table in (straight, swing)]


def turn(values, straight, swing, sign):
    half_dim = ROT_DIM // 2
    lane = lax.broadcasted_iota(jnp.int32, values.shape, 1)
    first = lax.rem(lane, HEAD_DIM) < half_dim
    other = jnp.where(
        first, pltpu.roll(values, 128 - half_dim, 1), pltpu.roll(values, half_dim, 1)
    )
    return values * straight + sign * other * swing


def backward_head(head, query, key, value, context, context_grad, lse, dq, dk, dv):
    length = query.shape[0]
    block = math.gcd(length, 256)
    scale = HEAD_DIM ** (-0.5)
    last_two = (((1,), (1,)), ((), ()))
    first_two = (((0,), (0,)), ((), ()))

    def dot(left, right, dims):
        return lax.dot_general(left, right, dims, preferred_element_type=F32)

    lanes = slice(head * HEAD_DIM, (head + 1) * HEAD_DIM)
    for first in reversed(range(0, length, block)):
        last = first + block
        q, g = query[first:last, lanes], context_grad[first:last, lanes]
        k, v = key[:last, lanes], value[:last, lanes]
        delta = jnp.sum(
            g.astype(F32) * context[first:last, lanes].astype(F32), axis=-1, keepdims=True
        )
        scores = dot(q, k, last_two) * scale
        row = lax.broadcasted_iota(jnp.int32, (block, last), 0) + first
        col = lax.broadcasted_iota(jnp.int32, (block, last), 1)
        probs = jnp.where(col <= row, jnp.exp(scores - lse[first:last, head : head + 1]), 0.0)
        score_grad = (probs * (dot(g, v, last_two) - delta)).astype(BF16)
        value_grad = dot(probs.astype(BF16), g, first_two)
        key_grad = dot(score_grad, q, first_two) * scale
        dq[first:last, lanes] = dot(score_grad, k, (((1,), (0,)), ((), ()))) * scale
        if last == length:
            dv[:, lanes] = value_grad
            dk[:, lanes] = key_grad
        else:
            dv[:last, lanes] += value_grad
            dk[:last, lanes] += key_grad


def backward_turn(straight, swing, dq, dk, dv, out, sums):
    length, cols = dq.shape
    block = math.gcd(length, 256)
    for part, grad in enumerate((dq, dk, dv)):
        for lane in range(0, cols, 128):
            at = part * cols + lane

            def step(i, total, grad=grad, lane=lane, at=at, part=part):
                rows = pl.ds(pl.multiple_of(i * block, block), block)
                values = grad[rows, lane : lane + 128]
                if part < 2:
                    values = turn(values, straight[rows, :], swing[rows, :], -1.0)
                out[rows, at : at + 128] = values.astype(BF16)
                return total + jnp.sum(values, axis=0, keepdims=True)

            sums[:, at : at + 128] = lax.fori_loop(
                0, length // block, step, jnp.zeros((1, 128), F32)
            )


def attention_forward(query, key, value, scale):
    length = query.shape[0]
    block = math.gcd(length, 256)
    contexts, lses = [], []
    for first in range(0, length, block):
        last = first + block
        scores = (
            jnp.einsum("qhd,khd->hqk", query[first:last], key[:last], preferred_element_type=F32)
            * scale
        )
        allowed = jnp.arange(last)[None, :] <= (first + jnp.arange(block))[:, None]
        scores = jnp.where(allowed, scores, MASKED)
        top = jnp.max(scores, axis=-1)
        weights = jnp.where(allowed, jnp.exp(scores - top[..., None]), 0.0)
        total = jnp.sum(weights, axis=-1)
        context = jnp.einsum(
            "hqk,khd->qhd", weights.astype(BF16), value[:last], preferred_element_type=F32
        )
        contexts.append(context / jnp.transpose(total)[..., None])
        lses.append(top + jnp.log(total))
    return jnp.concatenate(contexts, axis=0), jnp.concatenate(lses, axis=1)


def attention_backward(query, key, value, context_grad, delta, lse, scale):
    length, heads, dim = query.shape
    block = math.gcd(length, 256)
    query_grads = []
    key_grad = jnp.zeros((length, heads, dim), F32)
    value_grad = jnp.zeros((length, heads, dim), F32)
    for first in range(0, length, block):
        last = first + block
        q, g = query[first:last], context_grad[first:last]
        scores = jnp.einsum("qhd,khd->hqk", q, key[:last], preferred_element_type=F32) * scale
        allowed = jnp.arange(last)[None, :] <= (first + jnp.arange(block))[:, None]
        probs = jnp.where(allowed, jnp.exp(scores - lse[:, first:last, None]), 0.0)
        value_grad = value_grad.at[:last].add(
            jnp.einsum("hqk,qhd->khd", probs.astype(BF16), g, preferred_element_type=F32)
        )
        prob_grad = jnp.einsum("qhd,khd->hqk", g, value[:last], preferred_element_type=F32)
        score_grad = (probs * (prob_grad - delta[:, first:last, None])).astype(BF16)
        query_grads.append(
            jnp.einsum("hqk,khd->qhd", score_grad, key[:last], preferred_element_type=F32) * scale
        )
        key_grad = key_grad.at[:last].add(
            jnp.einsum("hqk,qhd->khd", score_grad, q, preferred_element_type=F32) * scale
        )
    return jnp.concatenate(query_grads, axis=0), key_grad, value_grad


def body(
    tokens,
    norm_gain,
    norm_bias,
    qkv_weight,
    qkv_bias,
    out_weight,
    out_bias,
    fc1_weight,
    fc1_bias,
    fc2_weight,
    fc2_bias,
    cotangent,
):
    f_size, c_size = lax.axis_size("fsdp"), lax.axis_size("ctx")
    ratio = c_size // f_size
    devices = f_size * c_size
    own_seqs, tok_count, width = tokens.shape
    own_rows = own_seqs * tok_count
    length = tok_count * c_size
    rows = own_seqs * length
    head_dim = HEAD_DIM
    scale = head_dim ** (-0.5)
    row_block = qkv_weight.shape[0]
    cols = qkv_weight.shape[2] // ratio
    hidden_cols = fc1_weight.shape[1] // ratio
    heads = cols // head_dim
    c_index = lax.axis_index("ctx")

    vec = norm_gain.shape[0]
    vec1 = fc1_bias.shape[0]
    me = lax.axis_index("fsdp") * c_size + c_index
    per = max(128 // vec, 1)
    lane_piece = jnp.arange(128) // vec == me % per

    def placed(vector):
        return jnp.where(lane_piece, jnp.tile(vector.reshape(-1, vec), (1, per)), 0).astype(BF16)

    def lanes(array):
        array = array.reshape(-1, min(array.shape[-1], 128))
        return jnp.pad(array, ((0, 0), (0, 128 - array.shape[1])))

    small = jnp.concatenate(
        [placed(v) for v in (norm_gain, norm_bias, out_bias, fc2_bias, qkv_bias)]
        + [lanes(fc1_bias)]
    )
    small = jnp.pad(small, ((0, -small.shape[0] % 16), (0, 0)))

    qkv_src = (
        jnp.transpose(qkv_weight.reshape(row_block, 3, ratio, cols), (2, 0, 1, 3))
        .reshape(ratio, row_block, 3 * cols)
    )
    fc1_src = jnp.transpose(fc1_weight.reshape(row_block, ratio, hidden_cols), (1, 0, 2))
    out_src = jnp.transpose(out_weight.reshape(ratio, cols, row_block), (0, 2, 1))
    fc2_src = jnp.transpose(fc2_weight.reshape(ratio, hidden_cols, row_block), (0, 2, 1))

    fused = cols % 128 == 0 and row_block % 128 == 0 and own_seqs == 1
    tables = lane_tables(length) if fused else None
    gathered = gather_call(
        f_size,
        c_size,
        [tokens.reshape(own_rows, width), cotangent.reshape(own_rows, width)],
        small,
        [qkv_src, fc1_src, fc2_src, out_src],
        tables,
        0,
    )
    first_all, cot_all, small_all, qkv_all, fc1_all, fc2_all, out_all = gathered[:7]

    def rows_of(gathered):
        return jnp.swapaxes(gathered.reshape(c_size, own_seqs, tok_count, width), 0, 1).reshape(
            rows, width
        )

    def blocks_of(array):
        return jnp.swapaxes(array.reshape(own_seqs, c_size, tok_count, width), 0, 1).reshape(
            c_size, own_rows, width
        )

    grad_rows = rows_of(cot_all)
    qkv_w = qkv_all.reshape(width, 3 * cols)
    fc1_w = fc1_all.reshape(width, hidden_cols)
    out_t = out_all.reshape(width, cols)
    fc2_t = fc2_all.reshape(width, hidden_cols)

    vectors = small_all.reshape(devices, -1, 128)
    joined = jnp.sum(vectors[:, :7].astype(F32).reshape(devices // per, per, 7, 128), axis=1)
    joined = jnp.swapaxes(joined, 0, 1).reshape(7, width)
    gain_full, shift_full, out_bias_full, fc2_bias_full = (joined[i] for i in range(4))
    lane = min(vec1, 128)
    fc1_bias_full = vectors[:, 7 : 7 + vec1 // lane, :lane].reshape(-1)
    fc1_b = lax.dynamic_slice_in_dim(fc1_bias_full, c_index * hidden_cols, hidden_cols, 0).astype(
        F32
    )

    def heads_of(array):
        return array.reshape(own_seqs, length, heads, head_dim)

    if fused:
        hidden_in = rows_of(first_all)
        context_rows = gathered[10]
    else:
        cosine, sine = rope_tables(length, ROT_DIM)
        qkv_b = lax.dynamic_slice_in_dim(joined[4:7], c_index * cols, cols, 1).reshape(-1)
        normed, _ = normed_of(rows_of(first_all).astype(F32))
        hidden_in = (normed * gain_full + shift_full).astype(BF16)
        mixed = jnp.dot(hidden_in, qkv_w, preferred_element_type=F32) + qkv_b
        query, key = (
            rotate_pairs(heads_of(part), cosine, sine, ROT_DIM, 1.0).astype(BF16)
            for part in (mixed[:, :cols], mixed[:, cols : 2 * cols])
        )
        value = heads_of(mixed[:, 2 * cols :].astype(BF16))
        forward = [attention_forward(query[s], key[s], value[s], scale) for s in range(own_seqs)]
        context_b = jnp.stack([pair[0] for pair in forward]).astype(BF16)
        lse = jnp.stack([pair[1] for pair in forward])
        context_rows = context_b.reshape(rows, cols)
    pre = jnp.dot(hidden_in, fc1_w, preferred_element_type=F32) + fc1_b
    act, slope = gelu_both(pre)
    act_b = act.astype(BF16)
    contract_last = (((1,), (1,)), ((), ()))
    partial_out = lax.dot_general(
        context_rows, out_t, contract_last, preferred_element_type=F32
    ) + lax.dot_general(act_b, fc2_t, contract_last, preferred_element_type=F32)

    pre_grad = jnp.dot(grad_rows, fc2_t, preferred_element_type=F32) * slope
    pre_grad_b = pre_grad.astype(BF16)
    contract_first = (((0,), (0,)), ((), ()))

    def weight_grad(left, right):
        product = lax.dot_general(left, right, contract_first, preferred_element_type=F32)
        return product.astype(BF16).reshape(ratio, f_size, row_block, right.shape[1])

    fc2_grad = weight_grad(grad_rows, act_b)
    fc1_grad = weight_grad(hidden_in, pre_grad_b)
    out_grad = weight_grad(grad_rows, context_rows)
    fc1_b_grad = jnp.sum(pre_grad, axis=0)
    mlp_back = lax.dot_general(pre_grad_b, fc1_w, contract_last, preferred_element_type=F32)
    context_grad = jnp.dot(grad_rows, out_t, preferred_element_type=F32).astype(BF16)
    out_blocks = blocks_of(partial_out.astype(BF16))
    if fused:
        (branch, normed_grad), (fc2_shard, fc1_shard, out_shard, qkv_shard), (sums_qkv,) = (
            reduce_call(
                f_size,
                c_size,
                [out_blocks],
                [fc2_grad, fc1_grad, out_grad],
                2,
                (
                    [*gathered[7:11], context_grad, gathered[11]],
                    tables,
                    qkv_w,
                    hidden_in,
                    blocks_of(mlp_back),
                ),
            )
        )
        qkv_b_grad = sums_qkv.reshape(3, cols)
    else:
        context_grad = heads_of(context_grad)
        delta = jnp.swapaxes(
            jnp.sum(context_grad.astype(F32) * context_b.astype(F32), axis=-1), 1, 2
        )
        grads = [
            attention_backward(
                query[s], key[s], value[s], context_grad[s], delta[s], lse[s], scale
            )
            for s in range(own_seqs)
        ]
        query_grad, key_grad, value_grad = [jnp.stack(parts) for parts in zip(*grads)]
        mixed_grad = jnp.concatenate(
            [
                rotate_pairs(query_grad, cosine, sine, ROT_DIM, -1.0).reshape(rows, cols),
                rotate_pairs(key_grad, cosine, sine, ROT_DIM, -1.0).reshape(rows, cols),
                value_grad.reshape(rows, cols),
            ],
            axis=1,
        )
        mixed_grad_b = mixed_grad.astype(BF16)
        qkv_b_grad = jnp.sum(mixed_grad, axis=0).reshape(3, cols)
        qkv_grad = weight_grad(hidden_in, mixed_grad_b)
        normed_part = (
            lax.dot_general(mixed_grad_b, qkv_w, contract_last, preferred_element_type=F32) + mlp_back
        )
        (branch, normed_grad), (fc2_shard, fc1_shard, out_shard, qkv_shard) = reduce_all(
            f_size,
            c_size,
            [out_blocks, blocks_of(normed_part.astype(BF16))],
            [fc2_grad, fc1_grad, out_grad, qkv_grad],
        )

    x_own = tokens.reshape(own_rows, width).astype(F32)
    cot_own = cotangent.reshape(own_rows, width).astype(F32)
    output = (x_own + branch + out_bias_full + fc2_bias_full).astype(BF16)
    normed_own, inv_std_own = normed_of(x_own)
    hat_grad = normed_grad * gain_full
    back_rows = inv_std_own * (
        hat_grad
        - jnp.mean(hat_grad, axis=-1, keepdims=True)
        - normed_own * jnp.mean(hat_grad * normed_own, axis=-1, keepdims=True)
    )
    input_grad = (back_rows + cot_own).astype(BF16)

    def whole(block, full, axis):
        return lax.dynamic_update_slice_in_dim(
            jnp.zeros(full, F32), block, c_index * block.shape[axis], axis
        )

    grad_gain = jnp.sum(normed_grad * normed_own, axis=0).reshape(devices, vec)
    grad_shift = jnp.sum(normed_grad, axis=0).reshape(devices, vec)
    grad_cot = jnp.sum(cot_own, axis=0).reshape(devices, vec)
    q_parts = jnp.swapaxes(whole(qkv_b_grad, (3, width), 1).reshape(3, devices, vec), 0, 1)
    f_parts = whole(fc1_b_grad, (vec1 * devices,), 0).reshape(devices, vec1)
    tiles = jnp.concatenate(
        [grad_gain, grad_shift, grad_cot, q_parts.reshape(devices, 3 * vec), f_parts], axis=1
    )
    used = tiles.shape[1]
    tiles = jnp.pad(tiles, ((0, 0), (0, -used % 1024))).reshape(devices, -1, 128)
    sums = small_call(f_size, c_size, tiles, 4).reshape(-1)

    qkv_out = jnp.transpose(
        qkv_shard.reshape(ratio, row_block, 3, cols), (1, 2, 0, 3)
    ).reshape(row_block, 3, ratio * cols)
    fc1_out = jnp.swapaxes(fc1_shard, 0, 1).reshape(row_block, ratio * hidden_cols)
    out_out = jnp.swapaxes(out_shard, 1, 2).reshape(ratio * cols, row_block)
    fc2_out = jnp.swapaxes(fc2_shard, 1, 2).reshape(ratio * hidden_cols, row_block)
    return (
        output.reshape(own_seqs, tok_count, width),
        input_grad.reshape(own_seqs, tok_count, width),
        sums[:vec],
        sums[vec : 2 * vec],
        qkv_out.astype(F32),
        sums[3 * vec : 6 * vec].reshape(3, vec),
        out_out.astype(F32),
        sums[2 * vec : 3 * vec],
        fc1_out.astype(F32),
        sums[6 * vec : 6 * vec + vec1],
        fc2_out.astype(F32),
        sums[2 * vec : 3 * vec],
    )


def solution(mesh):
    row = P("fsdp", "ctx", None)
    vector = P(("fsdp", "ctx"))
    return jax.shard_map(
        body,
        mesh=mesh,
        in_specs=(
            row,
            vector,
            vector,
            P("ctx", None, "fsdp"),
            P(None, ("fsdp", "ctx")),
            P("fsdp", "ctx"),
            vector,
            P("ctx", "fsdp"),
            vector,
            P("fsdp", "ctx"),
            vector,
            row,
        ),
        out_specs=(
            row,
            row,
            vector,
            vector,
            P("ctx", None, "fsdp"),
            P(None, ("fsdp", "ctx")),
            P("fsdp", "ctx"),
            vector,
            P("ctx", "fsdp"),
            vector,
            P("fsdp", "ctx"),
            vector,
        ),
        check_vma=False,
    )
```
